32 devices in a mesh: dp: 2 (over x), tx: 4 (over z), ty: 4 (over y, core).
Axes of the slice: x: 2, y: 2, z: 4, core: 2. Of those that a mesh axis runs over, the one named last changes fastest.
Arguments:
- x_act: bfloat16 [24, 768, 1024], P('dp', None, 'tx'), parts along dimension 0
- cot_out: bfloat16 [24, 768, 1024], P('dp', None, 'tx'), parts along dimension 0
- ln1_gain: bfloat16 [1024], P('tx')
- ln1_bias: bfloat16 [1024], P('tx')
- ln2_gain: bfloat16 [1024], P('tx')
- ln2_bias: bfloat16 [1024], P('tx')
- w_qkv: bfloat16 [1024, 16, 192], P('tx', 'ty')
- b_qkv: bfloat16 [16, 192], P('ty')
- w_dense: bfloat16 [1024, 1024], P('ty', 'tx')
- b_dense: bfloat16 [1024], P('tx')
- w_up: bfloat16 [1024, 4096], P('tx', 'ty')
- b_up: bfloat16 [4096], P('ty')
- w_down: bfloat16 [4096, 1024], P('ty', 'tx')
- b_down: bfloat16 [1024], P('tx')
Outputs:
- output 1: bfloat16 [24, 768, 1024], P('dp', None, 'tx'), parts along dimension 0
- output 2: bfloat16 [24, 768, 1024], P('dp', None, 'tx'), parts along dimension 0
- output 3: float32 [2048], P(('dp', 'tx')), parts along dimension 0
- output 4: float32 [2048], P(('dp', 'tx')), parts along dimension 0
- output 5: float32 [2048], P(('dp', 'tx')), parts along dimension 0
- output 6: float32 [2048], P(('dp', 'tx')), parts along dimension 0
- output 7: float32 [2048, 16, 192], P(('dp', 'tx'), 'ty'), parts along dimension 0
- output 8: float32 [32, 192], P(('dp', 'ty')), parts along dimension 0
- output 9: float32 [2048, 1024], P(('dp', 'ty'), 'tx'), parts along dimension 0
- output 10: float32 [2048], P(('dp', 'tx')), parts along dimension 0
- output 11: float32 [2048, 4096], P(('dp', 'tx'), 'ty'), parts along dimension 0
- output 12: float32 [8192], P(('dp', 'ty')), parts along dimension 0
- output 13: float32 [8192, 1024], P(('dp', 'ty'), 'tx'), parts along dimension 0
- output 14: float32 [2048], P(('dp', 'tx')), parts along dimension 0
There are 2 independent parts. The reference program is written for one: setup_inputs(seed, part) draws one part's arguments, and reference() takes and returns one part's arrays. A program takes and returns all parts, laid end to end along the dimension named above; an argument that names none is the same for every part.
All inputs are finite; a program needn't handle non-finite values.
Results may differ from the reference program's by a relative error of at most 0.02.
Values are sent between devices in bfloat16 or wider.
A program may use at most 1 GiB of HBM per device.

```python
import jax
import jax.numpy as jnp
from jax import lax

BATCH = 12
SEQ_LEN = 768
D_MODEL = 1024
N_HEADS = 16
HEAD_DIM = 64
ROT_DIM = HEAD_DIM // 4
FF_DIM = 4 * D_MODEL
LN_EPS = 1e-5
ROPE_BASE = 10000.0


def setup_inputs(seed: int = 0, part: int = 0) -> dict:
    base_key = jax.random.key(seed)
    act_keys = jax.random.split(jax.random.fold_in(base_key, part), 4)
    param_keys = jax.random.split(jax.random.key(seed + 1), 12)
    shape = (BATCH, SEQ_LEN, D_MODEL)
    col_pos = (jnp.arange(D_MODEL, dtype=jnp.float32) + 0.5) / D_MODEL
    noise = jax.random.normal(act_keys[0], shape, jnp.float32)
    slopes = 1.5 * jax.random.normal(act_keys[1], (BATCH, SEQ_LEN, 1), jnp.float32)
    offsets = 0.5 * jax.random.normal(act_keys[2], (BATCH, SEQ_LEN, 1), jnp.float32)
    x_act = noise * (0.5 + 1.5 * col_pos) + slopes * (2.0 * col_pos - 1.0) + offsets
    cot_out = jax.random.normal(act_keys[3], shape, jnp.float32)

    def normal_param(index, dims, spread, center):
        draw = jax.random.normal(param_keys[index], dims, jnp.float32)
        return (center + spread * draw).astype(jnp.bfloat16)

    return {
        'x_act': x_act.astype(jnp.bfloat16),
        'cot_out': cot_out.astype(jnp.bfloat16),
        'ln1_gain': normal_param(0, (D_MODEL,), 0.3, 1.0),
        'ln1_bias': normal_param(1, (D_MODEL,), 0.3, 0.0),
        'ln2_gain': normal_param(2, (D_MODEL,), 0.3, 1.0),
        'ln2_bias': normal_param(3, (D_MODEL,), 0.3, 0.0),
        'w_qkv': normal_param(4, (D_MODEL, N_HEADS, 3 * HEAD_DIM), D_MODEL ** -0.5, 0.0),
        'b_qkv': normal_param(5, (N_HEADS, 3 * HEAD_DIM), 0.3, 0.0),
        'w_dense': normal_param(6, (D_MODEL, D_MODEL), D_MODEL ** -0.5, 0.0),
        'b_dense': normal_param(7, (D_MODEL,), 0.3, 0.0),
        'w_up': normal_param(8, (D_MODEL, FF_DIM), D_MODEL ** -0.5, 0.0),
        'b_up': normal_param(9, (FF_DIM,), 0.3, 0.0),
        'w_down': normal_param(10, (FF_DIM, D_MODEL), FF_DIM ** -0.5, 0.0),
        'b_down': normal_param(11, (D_MODEL,), 0.3, 0.0),
    }


def rotary_tables(positions):
    inv_freq = ROPE_BASE ** (-jnp.arange(0, ROT_DIM, 2, dtype=jnp.float32) / ROT_DIM)
    angles = positions[:, None] * inv_freq[None, :]
    angles = jnp.concatenate([angles, angles], axis=-1)
    return jnp.cos(angles), jnp.sin(angles)


def apply_rotary(tensor, cos_tab, sin_tab):
    half_rot = ROT_DIM // 2
    rot_part = tensor[..., :ROT_DIM]
    turned = jnp.concatenate([-rot_part[..., half_rot:], rot_part[..., :half_rot]], axis=-1)
    mixed = rot_part * cos_tab[:, None, :] + turned * sin_tab[:, None, :]
    return jnp.concatenate([mixed, tensor[..., ROT_DIM:]], axis=-1)


def head_attention(operands):
    q_head, k_head, v_head = operands
    scores = jnp.einsum('bqe,bke->bqk', q_head.astype(jnp.float32), k_head.astype(jnp.float32)) * HEAD_DIM ** -0.5
    seq_index = jnp.arange(SEQ_LEN)
    causal = seq_index[:, None] >= seq_index[None, :]
    scores = jnp.where(causal[None], scores, -1e30)
    probs = jax.nn.softmax(scores, axis=-1).astype(jnp.bfloat16)
    context = jnp.einsum('bqk,bke->bqe', probs.astype(jnp.float32), v_head.astype(jnp.float32))
    return context.astype(jnp.bfloat16)


def layer_forward(x_act, ln1_gain, ln1_bias, ln2_gain, ln2_bias, w_qkv, b_qkv, w_dense, b_dense, w_up, b_up, w_down, b_down):
    tokens = BATCH * SEQ_LEN
    x_float = x_act.astype(jnp.float32)
    mean = jnp.mean(x_float, axis=-1, keepdims=True)
    variance = jnp.mean(x_float * x_float, axis=-1, keepdims=True) - mean * mean
    x_hat = (x_float - mean) * lax.rsqrt(variance + LN_EPS)
    h_attn = (x_hat * ln1_gain.astype(jnp.float32) + ln1_bias.astype(jnp.float32)).astype(jnp.bfloat16)
    h_mlp = (x_hat * ln2_gain.astype(jnp.float32) + ln2_bias.astype(jnp.float32)).astype(jnp.bfloat16)
    qkv_act = jnp.dot(h_attn.reshape(tokens, D_MODEL), w_qkv.reshape(D_MODEL, 3 * D_MODEL), preferred_element_type=jnp.float32)
    qkv_act = (qkv_act.reshape(BATCH, SEQ_LEN, N_HEADS, 3 * HEAD_DIM) + b_qkv.astype(jnp.float32)).astype(jnp.bfloat16)
    cos_tab, sin_tab = rotary_tables(jnp.arange(SEQ_LEN, dtype=jnp.float32))
    q_rot = apply_rotary(qkv_act[..., :HEAD_DIM].astype(jnp.float32), cos_tab, sin_tab).astype(jnp.bfloat16)
    k_rot = apply_rotary(qkv_act[..., HEAD_DIM:2 * HEAD_DIM].astype(jnp.float32), cos_tab, sin_tab).astype(jnp.bfloat16)
    values = qkv_act[..., 2 * HEAD_DIM:]
    per_head = (jnp.moveaxis(q_rot, 2, 0), jnp.moveaxis(k_rot, 2, 0), jnp.moveaxis(values, 2, 0))
    context = lax.map(jax.checkpoint(head_attention), per_head)
    context = jnp.moveaxis(context, 0, 2).reshape(tokens, D_MODEL)
    attn_out = jnp.dot(context, w_dense, preferred_element_type=jnp.float32) + b_dense.astype(jnp.float32)
    pre_act = jnp.dot(h_mlp.reshape(tokens, D_MODEL), w_up, preferred_element_type=jnp.float32) + b_up.astype(jnp.float32)
    pre_act = pre_act.astype(jnp.bfloat16)
    gelu_out = jax.nn.gelu(pre_act.astype(jnp.float32), approximate=False).astype(jnp.bfloat16)
    mlp_out = jnp.dot(gelu_out, w_down, preferred_element_type=jnp.float32) + b_down.astype(jnp.float32)
    y_float = x_float + (attn_out + mlp_out).reshape(BATCH, SEQ_LEN, D_MODEL)
    return y_float.astype(jnp.bfloat16)


def reference(x_act, cot_out, ln1_gain, ln1_bias, ln2_gain, ln2_bias, w_qkv, b_qkv, w_dense, b_dense, w_up, b_up, w_down, b_down):
    y_out, pullback = jax.vjp(layer_forward, x_act, ln1_gain, ln1_bias, ln2_gain, ln2_bias, w_qkv, b_qkv, w_dense, b_dense, w_up, b_up, w_down, b_down)
    grad_list = pullback(cot_out)
    return (y_out, grad_list[0], grad_list[1].astype(jnp.float32), grad_list[2].astype(jnp.float32), grad_list[3].astype(jnp.float32), grad_list[4].astype(jnp.float32), grad_list[5].astype(jnp.float32), grad_list[6].astype(jnp.float32), grad_list[7].astype(jnp.float32), grad_list[8].astype(jnp.float32), grad_list[9].astype(jnp.float32), grad_list[10].astype(jnp.float32), grad_list[11].astype(jnp.float32), grad_list[12].astype(jnp.float32))
```

```python
import functools
import jax
import jax.numpy as jnp
from jax import lax
from jax.experimental import pallas as pl
from jax.experimental.pallas import tpu as pltpu
from jax.sharding import PartitionSpec as P

LN_EPS = 1e-5
ROPE_BASE = 10000.0
HEAD = 64
ROT = 16
F32 = jnp.float32
BF16 = jnp.bfloat16


def rope_tables(seq_len, width):
    inv_freq = ROPE_BASE ** (-jnp.arange(0, ROT, 2, dtype=F32) / ROT)
    angles = jnp.arange(seq_len, dtype=F32)[:, None] * inv_freq[None, :]
    angles = jnp.concatenate([angles, angles], axis=-1)
    pad = ((0, 0), (0, HEAD - ROT))
    cos_head = jnp.pad(jnp.cos(angles), pad, constant_values=1.0)
    sin_head = jnp.pad(jnp.sin(angles), pad)
    return jnp.tile(cos_head, (1, width // HEAD)), jnp.tile(sin_head, (1, width // HEAD))


def rope_turn(width):
    row = lax.broadcasted_iota(jnp.int32, (width, width), 0)
    col = lax.broadcasted_iota(jnp.int32, (width, width), 1)
    lane = col % HEAD
    minus = (row == col + ROT // 2) & (lane < ROT // 2)
    plus = (row == col - ROT // 2) & (lane >= ROT // 2) & (lane < ROT)
    return (plus.astype(F32) - minus.astype(F32)).astype(BF16)


def dot_nn(a, b):
    return lax.dot_general(a, b, (((1,), (0,)), ((), ())), preferred_element_type=F32)


def dot_nt(a, b):
    return lax.dot_general(a, b, (((1,), (1,)), ((), ())), preferred_element_type=F32)


def dot_tn(a, b):
    return lax.dot_general(a, b, (((0,), (0,)), ((), ())), preferred_element_type=F32)


def attn_kernel(qkv_ref, dctx_ref, cos_ref, sin_ref, turn_ref, ctx_ref, dqkv_ref, dbias_ref, q_s, k_s, dq_s, *, blk):
    seq, width = dctx_ref.shape[1], dctx_ref.shape[2]
    heads, steps = width // HEAD, seq // blk
    turn = turn_ref[...]

    def rotate(t):
        return (t.astype(F32) * cos_ref[...] + dot_nn(t, turn) * sin_ref[...]).astype(BF16)

    def rotate_back(t):
        return (t.astype(F32) * cos_ref[...] - dot_nn(t, turn) * sin_ref[...]).astype(BF16)

    q_s[...] = rotate(qkv_ref[0, :, 0:width]) * BF16(HEAD ** -0.5)
    k_s[...] = rotate(qkv_ref[0, :, width:2 * width])
    row = lax.broadcasted_iota(jnp.int32, (blk, blk), 0)
    col = lax.broadcasted_iota(jnp.int32, (blk, blk), 1)
    causal = row >= col
    dk_heads, dv_heads = [], []
    for h in range(heads):
        hs = slice(h * HEAD, (h + 1) * HEAD)
        k_h = k_s[:, hs]
        v_h = qkv_ref[0, :, 2 * width + h * HEAD:2 * width + (h + 1) * HEAD]
        dk = [None] * steps
        dv = [None] * steps
        for i in range(steps):
            rows = slice(i * blk, (i + 1) * blk)
            n = (i + 1) * blk
            q_i = q_s[rows, hs]
            do_i = dctx_ref[0, rows, hs]
            s = dot_nt(q_i, k_h[:n])
            s_diag = jnp.where(causal, s[:, n - blk:], -1e30)
            s = s_diag if i == 0 else jnp.concatenate([s[:, :n - blk], s_diag], axis=1)
            p = jnp.exp(s - jnp.max(s, axis=1, keepdims=True))
            p = p * (1.0 / jnp.sum(p, axis=1, keepdims=True))
            p_b = p.astype(BF16)
            ctx_ref[0, rows, hs] = dot_nn(p_b, v_h[:n]).astype(BF16)
            dp = dot_nt(do_i, v_h[:n]).astype(BF16).astype(F32)
            ds = (p * (dp - jnp.sum(p * dp, axis=1, keepdims=True))).astype(BF16)
            dq_s[rows, hs] = (dot_nn(ds, k_h[:n]) * HEAD ** -0.5).astype(BF16)
            dk_i = dot_tn(ds, q_i)
            dv_i = dot_tn(p_b, do_i)
            for j in range(i + 1):
                part_k, part_v = dk_i[j * blk:(j + 1) * blk], dv_i[j * blk:(j + 1) * blk]
                dk[j] = part_k if dk[j] is None else dk[j] + part_k
                dv[j] = part_v if dv[j] is None else dv[j] + part_v
        dk_heads.append(jnp.concatenate(dk, axis=0).astype(BF16))
        dv_heads.append(jnp.concatenate(dv, axis=0).astype(BF16))
    d_q = rotate_back(dq_s[...])
    d_k = rotate_back(jnp.concatenate(dk_heads, axis=1))
    d_v = jnp.concatenate(dv_heads, axis=1)
    for pos, piece in enumerate((d_q, d_k, d_v)):
        cols = slice(pos * width, (pos + 1) * width)
        dqkv_ref[0, :, cols] = piece
        dbias_ref[0, :, cols] = jnp.broadcast_to(piece.astype(F32).sum(0, keepdims=True), (8, width))


def attention(qkv, d_ctx, batch, seq):
    width = d_ctx.shape[-1]
    blk = min(256, seq)
    cos_tab, sin_tab = rope_tables(seq, width)
    whole = lambda *shape: pl.BlockSpec(shape, lambda b: (0,) * len(shape))
    per_seq = lambda rows, cols: pl.BlockSpec((1, rows, cols), lambda b: (b, 0, 0))
    flops = batch * (width // HEAD) * seq * seq * HEAD * 12
    return pl.pallas_call(
        functools.partial(attn_kernel, blk=blk),
        grid=(batch,),
        in_specs=[per_seq(seq, 3 * width), per_seq(seq, width), whole(seq, width), whole(seq, width), whole(width, width)],
        out_specs=[per_seq(seq, width), per_seq(seq, 3 * width), per_seq(8, 3 * width)],
        out_shape=[
            jax.ShapeDtypeStruct((batch, seq, width), BF16),
            jax.ShapeDtypeStruct((batch, seq, 3 * width), BF16),
            jax.ShapeDtypeStruct((batch, 8, 3 * width), F32),
        ],
        scratch_shapes=[pltpu.VMEM((seq, width), BF16)] * 3,
        compiler_params=pltpu.CompilerParams(dimension_semantics=("arbitrary",), vmem_limit_bytes=48 << 20),
        cost_estimate=pl.CostEstimate(flops=4 * flops, bytes_accessed=batch * seq * width * 16, transcendentals=batch * (width // HEAD) * seq * seq // 2),
        name="attention",
    )(qkv.reshape(batch, seq, 3 * width), d_ctx.reshape(batch, seq, width), cos_tab, sin_tab, rope_turn(width))


def gelu_bf16(pre_act):
    return jax.nn.gelu(pre_act.astype(F32), approximate=False).astype(BF16)


def solution(mesh):
    n_tx, n_ty = mesh.shape['tx'], mesh.shape['ty']
    act_spec = P('dp', None, 'tx')
    width_spec = P('tx')
    in_specs = (act_spec, act_spec, width_spec, width_spec, width_spec, width_spec, P('tx', 'ty', None), P('ty', None), P('ty', 'tx'), width_spec, P('tx', 'ty'), P('ty'), P('ty', 'tx'), width_spec)
    width_out = P(('dp', 'tx'))
    out_specs = (act_spec, act_spec, width_out, width_out, width_out, width_out, P(('dp', 'tx'), 'ty', None), P(('dp', 'ty'), None), P(('dp', 'ty'), 'tx'), width_out, P(('dp', 'tx'), 'ty'), P(('dp', 'ty')), P(('dp', 'ty'), 'tx'), width_out)
    core_pairs = [(0, 1), (1, 0), (2, 3), (3, 2)]
    y_pairs = [(0, 2), (2, 0), (1, 3), (3, 1)]

    def over_core(a):
        return lax.ppermute(a, 'ty', core_pairs)

    def over_y(a):
        return lax.ppermute(a, 'ty', y_pairs)

    def over_z(a, k):
        return lax.ppermute(a, 'tx', [(i, (i + k) % n_tx) for i in range(n_tx)])

    def body(x_act, cot_out, ln1_gain, ln1_bias, ln2_gain, ln2_bias, w_qkv, b_qkv, w_dense, b_dense, w_up, b_up, w_down, b_down):
        batch, seq, d_loc = x_act.shape
        d_model = d_loc * n_tx
        heads = w_qkv.shape[1]
        hw = heads * HEAD
        n_b = batch // n_tx
        tok = n_b * seq
        chunk = tok // n_ty
        z, t, g = lax.axis_index('tx'), lax.axis_index('ty'), lax.axis_index('dp')
        core, y = t % 2, t // 2

        half = d_loc // 2

        def gather_rows(w):
            mine = lax.dynamic_slice_in_dim(w, g * half, half, 0)
            return lax.all_gather(mine, ('tx', 'dp'), axis=0, tiled=True)

        wq_loc = w_qkv.reshape(d_loc, heads, 3, HEAD).transpose(0, 2, 1, 3).reshape(d_loc, 3 * hw)
        w_a = gather_rows(jnp.concatenate([wq_loc, w_dense.T], axis=1))
        w_u = gather_rows(w_up)
        w_dt = gather_rows(w_down.T)
        w_q, w_o = w_a[:, :3 * hw], w_a[:, 3 * hw:]

        def gather_tokens(a, extra=None):
            a4 = a.reshape(n_tx, n_ty, chunk, d_loc)
            buf = jnp.zeros((n_ty, chunk, d_model), a.dtype)
            own = lax.dynamic_index_in_dim(a4, z, 0, keepdims=False)
            buf = lax.dynamic_update_slice(buf, own, (0, 0, z * d_loc))
            extras = []
            for k in (2, 1, 3):
                piece = lax.dynamic_slice(a4, ((z + k) % n_tx, t, 0, 0), (1, 1, chunk, d_loc)).reshape(chunk, d_loc)
                if extra is not None:
                    piece = jnp.concatenate([piece, extra], axis=0)
                got = over_z(piece, k)
                src = (z - k) % n_tx
                if extra is not None:
                    extras.append((src, got[chunk:]))
                    got = got[:chunk]
                got = got[None]
                two = jnp.concatenate([got, over_y(got)], axis=0)
                four = jnp.concatenate([two, over_core(two)], axis=0)
                for j, flip in enumerate((0, 2, 1, 3)):
                    buf = lax.dynamic_update_slice(buf, four[j:j + 1], (t ^ flip, 0, src * d_loc))
            return buf.reshape(tok, d_model), extras

        vec_loc = jnp.stack([ln1_gain, ln1_bias, ln2_gain, ln2_bias, b_dense, b_down], axis=0)
        vec_loc = jnp.pad(vec_loc, ((0, 10), (0, 0)))
        x, extras = gather_tokens(x_act, vec_loc)
        vecs = lax.dynamic_update_slice(jnp.zeros((16, d_model), BF16), vec_loc, (0, z * d_loc))
        for src, rows in extras:
            vecs = lax.dynamic_update_slice(vecs, rows, (0, src * d_loc))
        cot, _ = gather_tokens(cot_out)
        g1, be1, g2, be2, b_o, b_d = [vecs[i].astype(F32) for i in range(6)]

        x_f = x.astype(F32)
        mean = x_f.mean(-1, keepdims=True)
        inv_std = lax.rsqrt((x_f * x_f).mean(-1, keepdims=True) - mean * mean + LN_EPS)
        x_hat = (x_f - mean) * inv_std
        h1 = (x_hat * g1 + be1).astype(BF16)
        h2 = (x_hat * g2 + be2).astype(BF16)

        pre = (dot_nn(h2, w_u) + b_up.astype(F32)).astype(BF16)
        d_gelu = dot_nn(cot, w_dt).astype(BF16)
        u, gelu_pullback = jax.vjp(gelu_bf16, pre)
        (d_pre,) = gelu_pullback(d_gelu)

        def scatter_grad(part):
            return lax.psum_scatter(part, 'tx', scatter_dimension=0, tiled=True)

        part_down, part_up = dot_tn(cot, u).astype(BF16), dot_tn(h2, d_pre).astype(BF16)
        sum_down, sum_up = scatter_grad(part_down), scatter_grad(part_up)
        d_w_down, d_w_up = sum_down.astype(F32).T, sum_up.astype(F32)
        d_b_up = d_pre.astype(F32).sum(0)

        bq = b_qkv.astype(F32).reshape(heads, 3, HEAD).transpose(1, 0, 2).reshape(3 * hw)
        qkv = (dot_nn(h1, w_q) + bq).astype(BF16)
        cot_late, _, _ = lax.optimization_barrier((cot, part_down, part_up))
        d_ctx = dot_nn(cot_late, w_o).astype(BF16)
        ctx, d_qkv, d_bq = attention(qkv, d_ctx, n_b, seq)
        ctx, d_qkv = ctx.reshape(tok, hw), d_qkv.reshape(tok, 3 * hw)
        d_bq = d_bq[:, 0].sum(0)
        part_a = jnp.concatenate([dot_tn(h1, d_qkv).astype(BF16), dot_tn(cot, ctx).astype(BF16)], axis=1)
        part_a, _, _ = lax.optimization_barrier((part_a, sum_down, sum_up))
        d_w_a = scatter_grad(part_a).astype(F32)
        d_w_qkv = d_w_a[:, :3 * hw].reshape(d_loc, 3, heads, HEAD).transpose(0, 2, 1, 3).reshape(d_loc, heads, 3 * HEAD)
        d_w_dense = d_w_a[:, 3 * hw:].T

        def reduce_chunk(part):
            part = part.reshape(2, 2, chunk, d_model)
            keep = lax.dynamic_index_in_dim(part, core, 1, keepdims=False)
            give = lax.dynamic_index_in_dim(part, 1 - core, 1, keepdims=False)
            got = over_core(give)
            keep_y = lax.dynamic_index_in_dim(keep, y, 0, keepdims=False).astype(F32) + lax.dynamic_index_in_dim(got, y, 0, keepdims=False).astype(F32)
            give_y = lax.dynamic_index_in_dim(keep, 1 - y, 0, keepdims=False).astype(F32) + lax.dynamic_index_in_dim(got, 1 - y, 0, keepdims=False).astype(F32)
            return keep_y + over_y(give_y.astype(BF16)).astype(F32)

        def spread_chunk(mine):
            out = jnp.zeros((n_tx, n_ty, chunk, d_loc), BF16)
            for k in (2, 1, 3, 0):
                piece = lax.dynamic_slice(mine, (0, ((z + k) % n_tx) * d_loc), (chunk, d_loc))
                got = (over_z(piece, k) if k else piece)[None]
                src = (z - k) % n_tx
                two = jnp.concatenate([got, over_y(got)], axis=0)
                four = jnp.concatenate([two, over_core(two)], axis=0)
                for j, flip in enumerate((0, 2, 1, 3)):
                    out = lax.dynamic_update_slice(out, four[None, j:j + 1], (src, t ^ flip, 0, 0))
            return out.reshape(batch, seq, d_loc)

        def my_chunk(a):
            return lax.dynamic_slice_in_dim(a, t * chunk, chunk, 0)

        y_part = (dot_nt(u, w_dt) + dot_nt(ctx, w_o)).astype(BF16)
        y_mine = my_chunk(x).astype(F32) + reduce_chunk(y_part) + (b_o + b_d)
        y_out = spread_chunk(y_mine.astype(BF16))

        d_h1 = dot_nt(d_qkv, w_q).astype(BF16).astype(F32)
        d_h2 = dot_nt(d_pre, w_u).astype(BF16).astype(F32)
        a6_part = (d_h1 * g1 + d_h2 * g2).astype(BF16)
        ln_vec = jnp.stack([(d_h1 * x_hat).sum(0), d_h1.sum(0), (d_h2 * x_hat).sum(0), d_h2.sum(0)], axis=0)
        a6 = reduce_chunk(a6_part)
        xh = my_chunk(x_hat)
        d_x = my_chunk(inv_std) * (a6 - a6.mean(-1, keepdims=True) - xh * (a6 * xh).mean(-1, keepdims=True))
        dx_act = spread_chunk((my_chunk(cot).astype(F32) + d_x).astype(BF16))

        ln_vec = ln_vec + over_core(ln_vec)
        ln_vec = ln_vec + over_y(ln_vec)
        small = jnp.concatenate([ln_vec.reshape(-1), d_b_up, d_bq])
        total = small
        for k in range(1, n_tx):
            total = total + over_z(small, k)
        ln_sum = lax.dynamic_slice(total[:4 * d_model].reshape(4, d_model), (0, z * d_loc), (4, d_loc))
        d_b_up = total[4 * d_model:4 * d_model + d_b_up.shape[0]]
        d_b_qkv = total[4 * d_model + d_b_up.shape[0]:].reshape(3, heads, HEAD).transpose(1, 0, 2).reshape(heads, 3 * HEAD)
        d_b_out = cot_out.astype(F32).sum((0, 1))
        return (y_out, dx_act, ln_sum[0], ln_sum[1], ln_sum[2], ln_sum[3], d_w_qkv, d_b_qkv, d_w_dense, d_b_out, d_w_up, d_b_up, d_w_down, d_b_out)

    return jax.shard_map(body, mesh=mesh, in_specs=in_specs, out_specs=out_specs, check_vma=False)
```

```python
import functools
import jax
import jax.numpy as jnp
from jax import lax
from jax.experimental import pallas as pl
from jax.experimental.pallas import tpu as pltpu
from jax.sharding import PartitionSpec as P

LN_EPS = 1e-5
ROPE_BASE = 10000.0
HEAD = 64
ROT = 16
F32 = jnp.float32
BF16 = jnp.bfloat16

def rope_tables(seq_len, width):
    inv_freq = ROPE_BASE ** (-jnp.arange(0, ROT, 2, dtype=F32) / ROT)
    angles = jnp.arange(seq_len, dtype=F32)[:, None] * inv_freq[None, :]
    angles = jnp.concatenate([angles, angles], axis=-1)
    pad = ((0, 0), (0, HEAD - ROT))
    cos_head = jnp.pad(jnp.cos(angles), pad, constant_values=1.0)
    sin_head = jnp.pad(jnp.sin(angles), pad)
    return jnp.tile(cos_head, (1, width // HEAD)), jnp.tile(sin_head, (1, width // HEAD))


def rope_turn(width):
    row = lax.broadcasted_iota(jnp.int32, (width, width), 0)
    col = lax.broadcasted_iota(jnp.int32, (width, width), 1)
    lane = col % HEAD
    minus = (row == col + ROT // 2) & (lane < ROT // 2)
    plus = (row == col - ROT // 2) & (lane >= ROT // 2) & (lane < ROT)
    return (plus.astype(F32) - minus.astype(F32)).astype(BF16)


def dot_nn(a, b):
    return lax.dot_general(a, b, (((1,), (0,)), ((), ())), preferred_element_type=F32)


def dot_nt(a, b):
    return lax.dot_general(a, b, (((1,), (1,)), ((), ())), preferred_element_type=F32)


def dot_tn(a, b):
    return lax.dot_general(a, b, (((0,), (0,)), ((), ())), preferred_element_type=F32)


def attn_kernel(qkv_ref, dctx_ref, cos_ref, sin_ref, turn_ref, ctx_ref, dqkv_ref, dbias_ref, q_s, k_s, dq_s, *, blk):
    seq, width = dctx_ref.shape[1], dctx_ref.shape[2]
    heads, steps = width // HEAD, seq // blk
    turn = turn_ref[...]

    def rotate(t):
        return (t.astype(F32) * cos_ref[...] + dot_nn(t, turn) * sin_ref[...]).astype(BF16)

    def rotate_back(t):
        return (t.astype(F32) * cos_ref[...] - dot_nn(t, turn) * sin_ref[...]).astype(BF16)

    q_s[...] = rotate(qkv_ref[0, :, 0:width]) * BF16(HEAD ** -0.5)
    k_s[...] = rotate(qkv_ref[0, :, width:2 * width])
    row = lax.broadcasted_iota(jnp.int32, (blk, blk), 0)
    col = lax.broadcasted_iota(jnp.int32, (blk, blk), 1)
    causal = row >= col
    dk_heads, dv_heads = [], []
    for h in range(heads):
        hs = slice(h * HEAD, (h + 1) * HEAD)
        k_h = k_s[:, hs]
        v_h = qkv_ref[0, :, 2 * width + h * HEAD:2 * width + (h + 1) * HEAD]
        dk = [None] * steps
        dv = [None] * steps
        for i in range(steps):
            rows = slice(i * blk, (i + 1) * blk)
            n = (i + 1) * blk
            q_i = q_s[rows, hs]
            do_i = dctx_ref[0, rows, hs]
            s = dot_nt(q_i, k_h[:n])
            s_diag = jnp.where(causal, s[:, n - blk:], -1e30)
            s = s_diag if i == 0 else jnp.concatenate([s[:, :n - blk], s_diag], axis=1)
            p = jnp.exp(s - jnp.max(s, axis=1, keepdims=True))
            p = p * (1.0 / jnp.sum(p, axis=1, keepdims=True))
            p_b = p.astype(BF16)
            ctx_ref[0, rows, hs] = dot_nn(p_b, v_h[:n]).astype(BF16)
            dp = dot_nt(do_i, v_h[:n]).astype(BF16).astype(F32)
            ds = (p * (dp - jnp.sum(p * dp, axis=1, keepdims=True))).astype(BF16)
            dq_s[rows, hs] = (dot_nn(ds, k_h[:n]) * HEAD ** -0.5).astype(BF16)
            dk_i = dot_tn(ds, q_i)
            dv_i = dot_tn(p_b, do_i)
            for j in range(i + 1):
                part_k, part_v = dk_i[j * blk:(j + 1) * blk], dv_i[j * blk:(j + 1) * blk]
                dk[j] = part_k if dk[j] is None else dk[j] + part_k
                dv[j] = part_v if dv[j] is None else dv[j] + part_v
        dk_heads.append(jnp.concatenate(dk, axis=0).astype(BF16))
        dv_heads.append(jnp.concatenate(dv, axis=0).astype(BF16))
    d_q = rotate_back(dq_s[...])
    d_k = rotate_back(jnp.concatenate(dk_heads, axis=1))
    d_v = jnp.concatenate(dv_heads, axis=1)
    for pos, piece in enumerate((d_q, d_k, d_v)):
        cols = slice(pos * width, (pos + 1) * width)
        dqkv_ref[0, :, cols] = piece
        dbias_ref[0, :, cols] = jnp.broadcast_to(piece.astype(F32).sum(0, keepdims=True), (8, width))


def attention(qkv, d_ctx, batch, seq):
    width = d_ctx.shape[-1]
    blk = min(256, seq)
    cos_tab, sin_tab = rope_tables(seq, width)
    whole = lambda *shape: pl.BlockSpec(shape, lambda b: (0,) * len(shape))
    per_seq = lambda rows, cols: pl.BlockSpec((1, rows, cols), lambda b: (b, 0, 0))
    flops = batch * (width // HEAD) * seq * seq * HEAD * 12
    return pl.pallas_call(
        functools.partial(attn_kernel, blk=blk),
        grid=(batch,),
        in_specs=[per_seq(seq, 3 * width), per_seq(seq, width), whole(seq, width), whole(seq, width), whole(width, width)],
        out_specs=[per_seq(seq, width), per_seq(seq, 3 * width), per_seq(8, 3 * width)],
        out_shape=[
            jax.ShapeDtypeStruct((batch, seq, width), BF16),
            jax.ShapeDtypeStruct((batch, seq, 3 * width), BF16),
            jax.ShapeDtypeStruct((batch, 8, 3 * width), F32),
        ],
        scratch_shapes=[pltpu.VMEM((seq, width), BF16)] * 3,
        compiler_params=pltpu.CompilerParams(dimension_semantics=("arbitrary",), vmem_limit_bytes=48 << 20),
        cost_estimate=pl.CostEstimate(flops=4 * flops, bytes_accessed=batch * seq * width * 16, transcendentals=batch * (width // HEAD) * seq * seq // 2),
        name="attention",
    )(qkv.reshape(batch, seq, 3 * width), d_ctx.reshape(batch, seq, width), cos_tab, sin_tab, rope_turn(width))


def gelu_bf16(pre_act):
    return jax.nn.gelu(pre_act.astype(F32), approximate=False).astype(BF16)


MESH = pl.DeviceIdType.MESH
SUBS = 3


class Links:
    def __init__(self, send_sems, recv_sems):
        self.send_sems, self.recv_sems, self.count, self.sent = send_sems, recv_sems, 0, []

    def slot(self):
        self.count += 1
        return self.count - 1

    def make(self, slot, src, dst, dev):
        return pltpu.make_async_remote_copy(src_ref=src, dst_ref=dst, send_sem=self.send_sems.at[slot], recv_sem=self.recv_sems.at[slot], device_id=dev, device_id_type=MESH)

    def send(self, slot, src, dst, dev, cond=None):
        def go():
            self.make(slot, src, dst, dev).start()
        go() if cond is None else pl.when(cond)(go)
        self.sent.append((slot, src, dst, dev, cond))

    def arrive(self, slot, dst, dev, cond=None):
        def go():
            self.make(slot, dst, dst, dev).wait_recv()
        go() if cond is None else pl.when(cond)(go)

    def drain(self):
        for slot, src, dst, dev, cond in self.sent:
            def go():
                self.make(slot, src, dst, dev).wait_send()
            go() if cond is None else pl.when(cond)(go)


def neighbours():
    g, z, t = lax.axis_index('dp'), lax.axis_index('tx'), lax.axis_index('ty')
    core, y = t % 2, t // 2
    t_core, t_y, t_diag = y * 2 + 1 - core, (1 - y) * 2 + core, (1 - y) * 2 + 1 - core
    return g, z, t, core, y, t_core, t_y, t_diag


def enter(devices):
    barrier = pltpu.get_barrier_semaphore()
    for dev in devices:
        pl.semaphore_signal(barrier, inc=1, device_id=dev, device_id_type=MESH)
    pl.semaphore_wait(barrier, len(devices))


def gather_kernel(x_in, c_in, wu_in, wd_in, v_in, x_out, c_out, wu_out, wd_out, v_out, x_tmp, c_tmp, w_tmp, v_tmp, send_sems, recv_sems, local_sems, *, n_tx):
    g, z, t, core, y, t_core, t_y, t_diag = neighbours()
    core_dev, y_dev, x_dev = (g, z, t_core), (g, z, t_y), (1 - g, z, t)
    z_dev = [(g, (z + k) % n_tx, t) for k in range(n_tx)]
    left, right = (g, z - 1, t), (g, z + 1, t)
    d_loc = x_in.shape[-1]
    half = d_loc // 2
    links = Links(send_sems, recv_sems)

    def cols(s):
        return pl.ds(pl.multiple_of(s * d_loc, d_loc), d_loc)

    def w_rows(s, group):
        return pl.ds(pl.multiple_of(s * d_loc + group * half, half), half)

    own_in = [
        pltpu.make_async_copy(x_in.at[z], x_tmp, local_sems.at[0]),
        pltpu.make_async_copy(c_in.at[z], c_tmp, local_sems.at[1]),
        pltpu.make_async_copy(wu_in, w_tmp.at[0], local_sems.at[2]),
        pltpu.make_async_copy(wd_in, w_tmp.at[1], local_sems.at[3]),
        pltpu.make_async_copy(v_in, v_tmp, local_sems.at[4]),
    ]
    for copy in own_in:
        copy.start()
    enter([core_dev, y_dev, x_dev] + z_dev[1:])

    weights = ((wu_in, wu_out), (wd_in, wd_out))
    w_slot = [[links.slot() for _ in range(2 * n_tx)] for _ in weights]
    x_slot = [[links.slot() for _ in range(n_tx)] for _ in weights]

    def w_send(w, hops, src):
        s_left, s_right = z - hops, z + hops
        links.send(w_slot[w][hops + 1], src(s_left), weights[w][1].at[w_rows(s_left, g)], right, (s_left >= 0) & (z < n_tx - 1))
        links.send(w_slot[w][n_tx + hops + 1], src(s_right), weights[w][1].at[w_rows(s_right, g)], left, (s_right < n_tx) & (z > 0))

    def w_start(w):
        mine = weights[w][0].at[pl.ds(pl.multiple_of(g * half, half), half)]
        w_send(w, 0, lambda s: mine)

    def w_pass(w, hops):
        out = weights[w][1]
        for slot, s, ok in ((hops, z - hops, z - hops >= 0), (n_tx + hops, z + hops, z + hops < n_tx)):
            place = out.at[w_rows(s, g)]
            links.arrive(w_slot[w][slot], place, right, ok)
            links.send(x_slot[w][slot % n_tx if slot < n_tx else n_tx - hops], place, place, x_dev, ok)
        if hops < n_tx - 1:
            w_send(w, hops, lambda s: out.at[w_rows(s, g)])

    def w_finish(w):
        for hops in range(1, n_tx):
            for slot, s, ok in ((hops, z - hops, z - hops >= 0), (n_tx - hops, z + hops, z + hops < n_tx)):
                links.arrive(x_slot[w][slot], weights[w][1].at[w_rows(s, 1 - g)], x_dev, ok)

    arrays = ((x_in, x_out), (c_in, c_out))
    z_slot = [[links.slot() for _ in range(n_tx)] for _ in arrays]
    y_slot = [[links.slot() for _ in range(n_tx)] for _ in arrays]
    c_slot = [[[links.slot() for _ in range(2)] for _ in range(n_tx)] for _ in arrays]

    def t_start(a):
        for k in (2, 1, 3):
            links.send(z_slot[a][k], arrays[a][0].at[(z + k) % n_tx, t], arrays[a][1].at[t, :, cols(z)], z_dev[k])

    def t_pass(a, k):
        place = arrays[a][1].at[t, :, cols((z + n_tx - k) % n_tx)]
        links.arrive(z_slot[a][k], place, y_dev)
        links.send(y_slot[a][k], place, place, y_dev)
        links.send(c_slot[a][k][0], place, place, core_dev)

    def t_pass_y(a, k):
        place = arrays[a][1].at[t_y, :, cols((z + n_tx - k) % n_tx)]
        links.arrive(y_slot[a][k], place, y_dev)
        links.send(c_slot[a][k][1], place, place, core_dev)

    def t_finish(a):
        for k in range(1, n_tx):
            for j, chunk in enumerate((t_core, t_diag)):
                links.arrive(c_slot[a][k][j], arrays[a][1].at[chunk, :, cols((z + n_tx - k) % n_tx)], core_dev)

    v_slot = [links.slot() for _ in range(n_tx)]
    order = (1, 3, 2)
    w_start(0)
    w_start(1)
    for k in range(1, n_tx):
        links.send(v_slot[k], v_in, v_out.at[:, cols(z)], z_dev[k])
    t_start(0)
    places = [x_out.at[:, :, cols(z)], c_out.at[:, :, cols(z)], wu_out.at[pl.ds(pl.multiple_of(z * d_loc, d_loc), d_loc)], wd_out.at[pl.ds(pl.multiple_of(z * d_loc, d_loc), d_loc)], v_out.at[:, cols(z)]]
    own_out = []
    for i, (copy, src, dst) in enumerate(zip(own_in, (x_tmp, c_tmp, w_tmp.at[0], w_tmp.at[1], v_tmp), places)):
        copy.wait()
        own_out.append(pltpu.make_async_copy(src, dst, local_sems.at[i]))
        own_out[-1].start()
    w_pass(0, 1)
    w_pass(1, 1)
    t_start(1)
    w_pass(0, 2)
    w_pass(1, 2)
    for k in order:
        t_pass(0, k)
    w_pass(0, 3)
    w_pass(1, 3)
    for k in order:
        t_pass_y(0, k)
    for k in order:
        t_pass(1, k)
    for k in order:
        t_pass_y(1, k)
    w_finish(0)
    w_finish(1)
    t_finish(0)
    t_finish(1)
    for k in range(1, n_tx):
        links.arrive(v_slot[k], v_out.at[:, cols((z + n_tx - k) % n_tx)], y_dev)
    links.drain()
    for copy in own_out:
        copy.wait()


def gather_inputs(x_act, cot_out, w_up, w_dt, vecs, n_tx, n_ty):
    batch, seq, d_loc = x_act.shape
    chunk = batch * seq // (n_tx * n_ty)
    d_model, ff = d_loc * n_tx, w_up.shape[1]
    any_spec = pl.BlockSpec(memory_space=pl.ANY)
    tokens = jax.ShapeDtypeStruct((n_ty, chunk, d_model), BF16)
    weight = jax.ShapeDtypeStruct((d_model, ff), BF16)
    slots = 2 * (2 * n_tx + n_tx) + 2 * (n_tx + n_tx + 2 * n_tx) + n_tx
    return pl.pallas_call(
        functools.partial(gather_kernel, n_tx=n_tx),
        in_specs=[any_spec] * 5,
        out_specs=[any_spec] * 5,
        out_shape=[tokens, tokens, weight, weight, jax.ShapeDtypeStruct((vecs.shape[0], d_model), BF16)],
        scratch_shapes=[
            pltpu.VMEM((n_ty, chunk, d_loc), BF16),
            pltpu.VMEM((n_ty, chunk, d_loc), BF16),
            pltpu.VMEM((2, d_loc, ff), BF16),
            pltpu.VMEM((vecs.shape[0], d_loc), BF16),
            pltpu.SemaphoreType.DMA((slots,)),
            pltpu.SemaphoreType.DMA((slots,)),
            pltpu.SemaphoreType.DMA((5,)),
        ],
        compiler_params=pltpu.CompilerParams(collective_id=0, has_side_effects=True),
        cost_estimate=pl.CostEstimate(flops=40_000_000_000, bytes_accessed=40_000_000, transcendentals=0),
        name="gather_inputs",
    )(x_act.reshape(n_tx, n_ty, chunk, d_loc), cot_out.reshape(n_tx, n_ty, chunk, d_loc), w_up, w_dt, vecs)


def output_kernel(y_part, a_part, x_in, c_in, bias, small, y_out, dx_out, small_out, x_s, c_s, rc, sy, ry, fin, sm_buf, send_sems, recv_sems, local_sems, *, n_tx):
    g, z, t, core, y, t_core, t_y, t_diag = neighbours()
    core_dev, y_dev = (g, z, t_core), (g, z, t_y)
    z_dev = [(g, (z + k) % n_tx, t) for k in range(n_tx)]
    chunk, d_model = x_s.shape
    d_loc = d_model // n_tx
    sub = chunk // SUBS
    links = Links(send_sems, recv_sems)
    parts, outs = (y_part, a_part), (y_out, dx_out)
    own_in = [pltpu.make_async_copy(x_in.at[t], x_s, local_sems.at[0]), pltpu.make_async_copy(c_in.at[t], c_s, local_sems.at[1])]
    for copy in own_in:
        copy.start()
    enter([core_dev, y_dev] + z_dev[1:])
    items = [(a, i) for a in range(2) for i in range(SUBS)]

    def cols(s):
        return pl.ds(pl.multiple_of(s * d_loc, d_loc), d_loc)

    def rows(i):
        return pl.ds(i * sub, sub)

    core_slot = {(item, j): links.slot() for item in items for j in range(2)}
    y_slot = {item: links.slot() for item in items}
    z_slot = {(item, k): links.slot() for item in items for k in range(n_tx)}
    ag_y = {(item, k): links.slot() for item in items for k in range(n_tx)}
    ag_c = {(item, k, j): links.slot() for item in items for k in range(n_tx) for j in range(2)}

    sm_slot = [links.slot() for _ in range(5)]
    links.send(sm_slot[0], small, sm_buf.at[0], core_dev)
    for item in items:
        a, i = item
        for j, yy in enumerate((1 - y, y)):
            links.send(core_slot[item, j], parts[a].at[yy, 1 - core, rows(i)], rc.at[a, yy, rows(i)], core_dev)

    step = 32

    def give(item):
        a, i = item
        links.arrive(core_slot[item, 0], rc.at[a, 1 - y, rows(i)], core_dev)

        def body(r, carry):
            at = pl.ds(i * sub + r * step, step)
            total = parts[a][1 - y, core, at, :].astype(F32) + rc[a, 1 - y, at, :].astype(F32)
            sy[a, at, :] = total.astype(BF16)
            return carry
        lax.fori_loop(0, sub // step, body, 0)
        links.send(y_slot[item], sy.at[a, rows(i)], ry.at[a, rows(i)], y_dev)

    def finish(item):
        a, i = item
        links.arrive(core_slot[item, 1], rc.at[a, y, rows(i)], core_dev)
        links.arrive(y_slot[item], ry.at[a, rows(i)], y_dev)

        def body(r, carry):
            at = pl.ds(i * sub + r * step, step)
            total = parts[a][y, core, at, :].astype(F32) + rc[a, y, at, :].astype(F32) + ry[a, at, :].astype(F32)
            x = x_s[at, :].astype(F32)
            if a == 0:
                out = x + total + bias[0:1, :]
            else:
                mean = jnp.mean(x, axis=-1, keepdims=True)
                inv = lax.rsqrt(jnp.mean(x * x, axis=-1, keepdims=True) - mean * mean + LN_EPS)
                xh = (x - mean) * inv
                m1 = jnp.mean(total, axis=-1, keepdims=True)
                m2 = jnp.mean(total * xh, axis=-1, keepdims=True)
                out = c_s[at, :].astype(F32) + inv * (total - m1 - xh * m2)
            fin[a, at, :] = out.astype(BF16)
            return carry
        lax.fori_loop(0, sub // step, body, 0)
        for k in (2, 1, 3):
            links.send(z_slot[item, k], fin.at[a, rows(i), cols((z + k) % n_tx)], outs[a].at[z, t, rows(i)], z_dev[k])
        mine = fin.at[a, rows(i), cols(z)]
        place = outs[a].at[z, t, rows(i)]
        own = pltpu.make_async_copy(mine, place, local_sems.at[2 + a * SUBS + i])
        own.start()
        links.send(ag_y[item, 0], mine, place, y_dev)
        links.send(ag_c[item, 0, 0], mine, place, core_dev)
        return own

    def src(k):
        return (z + n_tx - k) % n_tx

    def forward(item):
        a, i = item
        for k in (1, 3, 2):
            place = outs[a].at[src(k), t, rows(i)]
            links.arrive(z_slot[item, k], place, y_dev)
            links.send(ag_y[item, k], place, place, y_dev)
            links.send(ag_c[item, k, 0], place, place, core_dev)

    def forward_y(item):
        a, i = item
        for k in (0, 1, 3, 2):
            place = outs[a].at[src(k), t_y, rows(i)]
            links.arrive(ag_y[item, k], place, y_dev)
            links.send(ag_c[item, k, 1], place, place, core_dev)

    for item in items:
        give(item)
    for copy in own_in:
        copy.wait()
    links.arrive(sm_slot[0], sm_buf.at[0], core_dev)
    row = lax.broadcasted_iota(jnp.int32, small.shape, 0)
    sm_buf[1] = small[...] + jnp.where(row < 4, sm_buf[0], 0.0)
    links.send(sm_slot[1], sm_buf.at[1], sm_buf.at[2], y_dev)
    owns = []
    n = len(items)
    for i in range(n + 2):
        if i < n:
            owns.append(finish(items[i]))
        if i == 1:
            links.arrive(sm_slot[1], sm_buf.at[2], y_dev)
            sm_buf[3] = sm_buf[1] + jnp.where(row < 4, sm_buf[2], 0.0)
            for k in range(1, n_tx):
                links.send(sm_slot[1 + k], sm_buf.at[3], sm_buf.at[3 + k], z_dev[k])
        if 0 <= i - 1 < n:
            forward(items[i - 1])
        if 0 <= i - 2 < n:
            forward_y(items[i - 2])
    for k in range(1, n_tx):
        links.arrive(sm_slot[1 + k], sm_buf.at[3 + k], y_dev)
    small_out[...] = sm_buf[3] + sm_buf[4] + sm_buf[5] + sm_buf[6]
    for item in items:
        a, i = item
        for k in range(n_tx):
            for j, who in enumerate((t_core, t_diag)):
                links.arrive(ag_c[item, k, j], outs[a].at[src(k), who, rows(i)], core_dev)
    links.drain()
    for own in owns:
        own.wait()


def send_outputs(y_part, a_part, x, cot, bias, small, n_tx, n_ty):
    chunk, d_model = x.shape[1:]
    d_loc = d_model // n_tx
    any_spec, vmem = pl.BlockSpec(memory_space=pl.ANY), pl.BlockSpec(memory_space=pltpu.VMEM)
    out = jax.ShapeDtypeStruct((n_tx, n_ty, chunk, d_loc), BF16)
    slots = 2 * SUBS * (3 + 4 * n_tx) + 5
    return pl.pallas_call(
        functools.partial(output_kernel, n_tx=n_tx),
        in_specs=[vmem, vmem, any_spec, any_spec, vmem, vmem],
        out_specs=[any_spec, any_spec, vmem],
        out_shape=[out, out, jax.ShapeDtypeStruct(small.shape, F32)],
        scratch_shapes=[
            pltpu.VMEM((chunk, d_model), BF16),
            pltpu.VMEM((chunk, d_model), BF16),
            pltpu.VMEM((2, 2, chunk, d_model), BF16),
            pltpu.VMEM((2, chunk, d_model), BF16),
            pltpu.VMEM((2, chunk, d_model), BF16),
            pltpu.VMEM((2, chunk, d_model), BF16),
            pltpu.VMEM((7,) + small.shape, F32),
            pltpu.SemaphoreType.DMA((slots,)),
            pltpu.SemaphoreType.DMA((slots,)),
            pltpu.SemaphoreType.DMA((2 + 2 * SUBS,)),
        ],
        compiler_params=pltpu.CompilerParams(collective_id=1, has_side_effects=True, vmem_limit_bytes=56 << 20),
        cost_estimate=pl.CostEstimate(flops=40_000_000_000, bytes_accessed=40_000_000, transcendentals=0),
        name="send_outputs",
    )(y_part.reshape(2, 2, chunk, d_model), a_part.reshape(2, 2, chunk, d_model), x, cot, bias, small)


def solution(mesh):
    n_tx, n_ty = mesh.shape['tx'], mesh.shape['ty']
    act_spec = P('dp', None, 'tx')
    width_spec = P('tx')
    in_specs = (act_spec, act_spec, width_spec, width_spec, width_spec, width_spec, P('tx', 'ty', None), P('ty', None), P('ty', 'tx'), width_spec, P('tx', 'ty'), P('ty'), P('ty', 'tx'), width_spec)
    width_out = P(('dp', 'tx'))
    out_specs = (act_spec, act_spec, width_out, width_out, width_out, width_out, P(('dp', 'tx'), 'ty', None), P(('dp', 'ty'), None), P(('dp', 'ty'), 'tx'), width_out, P(('dp', 'tx'), 'ty'), P(('dp', 'ty')), P(('dp', 'ty'), 'tx'), width_out)
    def body(x_act, cot_out, ln1_gain, ln1_bias, ln2_gain, ln2_bias, w_qkv, b_qkv, w_dense, b_dense, w_up, b_up, w_down, b_down):
        batch, seq, d_loc = x_act.shape
        d_model = d_loc * n_tx
        heads = w_qkv.shape[1]
        hw = heads * HEAD
        n_b = batch // n_tx
        tok = n_b * seq
        z, g = lax.axis_index('tx'), lax.axis_index('dp')

        half = d_loc // 2

        def gather_rows(w):
            mine = lax.dynamic_slice_in_dim(w, g * half, half, 0)
            return lax.all_gather(mine, ('tx', 'dp'), axis=0, tiled=True)

        wq_loc = w_qkv.reshape(d_loc, heads, 3, HEAD).transpose(0, 2, 1, 3).reshape(d_loc, 3 * hw)
        w_a = gather_rows(jnp.concatenate([wq_loc, w_dense.T], axis=1))
        w_q, w_o = w_a[:, :3 * hw], w_a[:, 3 * hw:]
        vec_loc = jnp.stack([ln1_gain, ln1_bias, ln2_gain, ln2_bias, b_dense, b_down], axis=0)
        vec_loc = jnp.pad(vec_loc, ((0, 10), (0, 0)))
        x_chunks, cot_chunks, w_u, w_dt, vecs = gather_inputs(x_act, cot_out, w_up, w_down.T, vec_loc, n_tx, n_ty)
        x, cot = x_chunks.reshape(tok, d_model), cot_chunks.reshape(tok, d_model)
        g1, be1, g2, be2, b_o, b_d = [vecs[i].astype(F32) for i in range(6)]

        x_f = x.astype(F32)
        mean = x_f.mean(-1, keepdims=True)
        inv_std = lax.rsqrt((x_f * x_f).mean(-1, keepdims=True) - mean * mean + LN_EPS)
        x_hat = (x_f - mean) * inv_std
        h1 = (x_hat * g1 + be1).astype(BF16)
        h2 = (x_hat * g2 + be2).astype(BF16)

        pre = (dot_nn(h2, w_u) + b_up.astype(F32)).astype(BF16)
        d_gelu = dot_nn(cot, w_dt).astype(BF16)
        u, gelu_pullback = jax.vjp(gelu_bf16, pre)
        (d_pre,) = gelu_pullback(d_gelu)

        def scatter_grad(part):
            return lax.psum_scatter(part, 'tx', scatter_dimension=0, tiled=True)

        part_down, part_up = dot_tn(cot, u).astype(BF16), dot_tn(h2, d_pre).astype(BF16)
        sum_down, sum_up = scatter_grad(part_down), scatter_grad(part_up)
        d_w_down, d_w_up = sum_down.astype(F32).T, sum_up.astype(F32)
        d_b_up = d_pre.astype(F32).sum(0)

        bq = b_qkv.astype(F32).reshape(heads, 3, HEAD).transpose(1, 0, 2).reshape(3 * hw)
        qkv = (dot_nn(h1, w_q) + bq).astype(BF16)
        cot_late, _, _ = lax.optimization_barrier((cot, part_down, part_up))
        d_ctx = dot_nn(cot_late, w_o).astype(BF16)
        ctx, d_qkv, d_bq = attention(qkv, d_ctx, n_b, seq)
        ctx, d_qkv = ctx.reshape(tok, hw), d_qkv.reshape(tok, 3 * hw)
        d_bq = d_bq[:, 0].sum(0)
        part_a = jnp.concatenate([dot_tn(h1, d_qkv).astype(BF16), dot_tn(cot, ctx).astype(BF16)], axis=1)
        part_a, _, _ = lax.optimization_barrier((part_a, sum_down, sum_up))
        d_w_a = scatter_grad(part_a).astype(F32)
        d_w_qkv = d_w_a[:, :3 * hw].reshape(d_loc, 3, heads, HEAD).transpose(0, 2, 1, 3).reshape(d_loc, heads, 3 * HEAD)
        d_w_dense = d_w_a[:, 3 * hw:].T

        y_part = (dot_nt(u, w_dt) + dot_nt(ctx, w_o)).astype(BF16)

        d_h1 = dot_nt(d_qkv, w_q).astype(BF16).astype(F32)
        d_h2 = dot_nt(d_pre, w_u).astype(BF16).astype(F32)
        a6_part = (d_h1 * g1 + d_h2 * g2).astype(BF16)
        small = jnp.stack([(d_h1 * x_hat).sum(0), d_h1.sum(0), (d_h2 * x_hat).sum(0), d_h2.sum(0), jnp.pad(d_b_up, (0, d_model - d_b_up.shape[0])), jnp.pad(d_bq, (0, d_model - 3 * hw))], axis=0)
        small = jnp.pad(small, ((0, 2), (0, 0)))
        bias = jnp.broadcast_to((b_o + b_d)[None], (8, d_model))
        y_out, dx_act, total = send_outputs(y_part, a6_part, x_chunks, cot_chunks, bias, small, n_tx, n_ty)
        y_out, dx_act = y_out.reshape(batch, seq, d_loc), dx_act.reshape(batch, seq, d_loc)
        ln_sum = lax.dynamic_slice(total, (0, z * d_loc), (4, d_loc))
        d_b_up = total[4, :d_b_up.shape[0]]
        d_b_qkv = total[5, :3 * hw].reshape(3, heads, HEAD).transpose(1, 0, 2).reshape(heads, 3 * HEAD)
        d_b_out = cot_out.astype(F32).sum((0, 1))
        return (y_out, dx_act, ln_sum[0], ln_sum[1], ln_sum[2], ln_sum[3], d_w_qkv, d_b_qkv, d_w_dense, d_b_out, d_w_up, d_b_up, d_w_down, d_b_out)

    return jax.shard_map(body, mesh=mesh, in_specs=in_specs, out_specs=out_specs, check_vma=False)
```

```python
import functools
import jax
import jax.numpy as jnp
from jax import lax
from jax.experimental import pallas as pl
from jax.experimental.pallas import tpu as pltpu
from jax.sharding import PartitionSpec as P

LN_EPS = 1e-5
ROPE_BASE = 10000.0
HEAD = 64
ROT = 16
F32 = jnp.float32
BF16 = jnp.bfloat16

def rope_tables(seq_len, width):
    inv_freq = ROPE_BASE ** (-jnp.arange(0, ROT, 2, dtype=F32) / ROT)
    angles = jnp.arange(seq_len, dtype=F32)[:, None] * inv_freq[None, :]
    angles = jnp.concatenate([angles, angles], axis=-1)
    pad = ((0, 0), (0, HEAD - ROT))
    cos_head = jnp.pad(jnp.cos(angles), pad, constant_values=1.0)
    sin_head = jnp.pad(jnp.sin(angles), pad)
    return jnp.tile(cos_head, (1, width // HEAD)), jnp.tile(sin_head, (1, width // HEAD))


def rope_turn(width):
    row = lax.broadcasted_iota(jnp.int32, (width, width), 0)
    col = lax.broadcasted_iota(jnp.int32, (width, width), 1)
    lane = col % HEAD
    minus = (row == col + ROT // 2) & (lane < ROT // 2)
    plus = (row == col - ROT // 2) & (lane >= ROT // 2) & (lane < ROT)
    return (plus.astype(F32) - minus.astype(F32)).astype(BF16)


def dot_nn(a, b):
    return lax.dot_general(a, b, (((1,), (0,)), ((), ())), preferred_element_type=F32)


def dot_nt(a, b):
    return lax.dot_general(a, b, (((1,), (1,)), ((), ())), preferred_element_type=F32)


def dot_tn(a, b):
    return lax.dot_general(a, b, (((0,), (0,)), ((), ())), preferred_element_type=F32)


def gelu_bf16(pre_act):
    return jax.nn.gelu(pre_act.astype(F32), approximate=False).astype(BF16)


MESH = pl.DeviceIdType.MESH


class Links:
    def __init__(self, send_sems, recv_sems):
        self.send_sems, self.recv_sems, self.count, self.sent = send_sems, recv_sems, 0, []

    def slot(self, count=1):
        self.count += count
        return self.count - count

    def make(self, slot, src, dst, dev):
        return pltpu.make_async_remote_copy(src_ref=src, dst_ref=dst, send_sem=self.send_sems.at[slot], recv_sem=self.recv_sems.at[slot], device_id=dev, device_id_type=MESH)

    def send(self, slot, src, dst, dev, cond=None):
        def go():
            self.make(slot, src, dst, dev).start()
        go() if cond is None else pl.when(cond)(go)
        self.sent.append((slot, src, dst, dev, cond))

    def arrive(self, slot, dst, dev, cond=None):
        def go():
            self.make(slot, dst, dst, dev).wait_recv()
        go() if cond is None else pl.when(cond)(go)

    def drain(self):
        for slot, src, dst, dev, cond in self.sent:
            def go():
                self.make(slot, src, dst, dev).wait_send()
            go() if cond is None else pl.when(cond)(go)


def neighbours():
    g, z, t = lax.axis_index('dp'), lax.axis_index('tx'), lax.axis_index('ty')
    core, y = t % 2, t // 2
    t_core, t_y, t_diag = y * 2 + 1 - core, (1 - y) * 2 + core, (1 - y) * 2 + 1 - core
    return g, z, t, core, y, t_core, t_y, t_diag


def enter(devices):
    barrier = pltpu.get_barrier_semaphore()
    for dev in devices:
        pl.semaphore_signal(barrier, inc=1, device_id=dev, device_id_type=MESH)
    pl.semaphore_wait(barrier, len(devices))


def gather_kernel(x_in, c_in, wu_in, wd_in, v_in, x_out, c_out, wu_out, wd_out, v_out, x_tmp, c_tmp, w_tmp, v_tmp, send_sems, recv_sems, local_sems, *, n_tx):
    g, z, t, core, y, t_core, t_y, t_diag = neighbours()
    core_dev, y_dev, x_dev = (g, z, t_core), (g, z, t_y), (1 - g, z, t)
    z_dev = [(g, (z + k) % n_tx, t) for k in range(n_tx)]
    left, right = (g, z - 1, t), (g, z + 1, t)
    d_loc = x_in.shape[-1]
    half = d_loc // 2
    links = Links(send_sems, recv_sems)

    def cols(s):
        return pl.ds(pl.multiple_of(s * d_loc, d_loc), d_loc)

    def w_rows(s, group):
        return pl.ds(pl.multiple_of(s * d_loc + group * half, half), half)

    own_in = [
        pltpu.make_async_copy(x_in.at[z], x_tmp, local_sems.at[0]),
        pltpu.make_async_copy(c_in.at[z], c_tmp, local_sems.at[1]),
        pltpu.make_async_copy(wu_in, w_tmp.at[0], local_sems.at[2]),
        pltpu.make_async_copy(wd_in, w_tmp.at[1], local_sems.at[3]),
        pltpu.make_async_copy(v_in, v_tmp, local_sems.at[4]),
    ]
    for copy in own_in:
        copy.start()
    enter([core_dev, y_dev, x_dev] + z_dev[1:])

    weights = ((wu_in, wu_out), (wd_in, wd_out))
    w_slot = [[links.slot() for _ in range(2 * n_tx)] for _ in weights]
    x_slot = [[links.slot() for _ in range(n_tx)] for _ in weights]

    def w_send(w, hops, src):
        s_left, s_right = z - hops, z + hops
        links.send(w_slot[w][hops + 1], src(s_left), weights[w][1].at[w_rows(s_left, g)], right, (s_left >= 0) & (z < n_tx - 1))
        links.send(w_slot[w][n_tx + hops + 1], src(s_right), weights[w][1].at[w_rows(s_right, g)], left, (s_right < n_tx) & (z > 0))

    def w_start(w):
        mine = weights[w][0].at[pl.ds(pl.multiple_of(g * half, half), half)]
        w_send(w, 0, lambda s: mine)

    def w_pass(w, hops):
        out = weights[w][1]
        for slot, s, ok in ((hops, z - hops, z - hops >= 0), (n_tx + hops, z + hops, z + hops < n_tx)):
            place = out.at[w_rows(s, g)]
            links.arrive(w_slot[w][slot], place, right, ok)
            links.send(x_slot[w][slot % n_tx if slot < n_tx else n_tx - hops], place, place, x_dev, ok)
        if hops < n_tx - 1:
            w_send(w, hops, lambda s: out.at[w_rows(s, g)])

    def w_finish(w):
        for hops in range(1, n_tx):
            for slot, s, ok in ((hops, z - hops, z - hops >= 0), (n_tx - hops, z + hops, z + hops < n_tx)):
                links.arrive(x_slot[w][slot], weights[w][1].at[w_rows(s, 1 - g)], x_dev, ok)

    arrays = ((x_in, x_out), (c_in, c_out))
    z_slot = [[links.slot() for _ in range(n_tx)] for _ in arrays]
    y_slot = [[links.slot() for _ in range(n_tx)] for _ in arrays]
    c_slot = [[[links.slot() for _ in range(2)] for _ in range(n_tx)] for _ in arrays]

    def t_start(a):
        for k in (2, 1, 3):
            links.send(z_slot[a][k], arrays[a][0].at[(z + k) % n_tx, t], arrays[a][1].at[t, :, cols(z)], z_dev[k])

    def t_pass(a, k):
        place = arrays[a][1].at[t, :, cols((z + n_tx - k) % n_tx)]
        links.arrive(z_slot[a][k], place, y_dev)
        links.send(y_slot[a][k], place, place, y_dev)
        links.send(c_slot[a][k][0], place, place, core_dev)

    def t_pass_y(a, k):
        place = arrays[a][1].at[t_y, :, cols((z + n_tx - k) % n_tx)]
        links.arrive(y_slot[a][k], place, y_dev)
        links.send(c_slot[a][k][1], place, place, core_dev)

    def t_finish(a):
        for k in range(1, n_tx):
            for j, chunk in enumerate((t_core, t_diag)):
                links.arrive(c_slot[a][k][j], arrays[a][1].at[chunk, :, cols((z + n_tx - k) % n_tx)], core_dev)

    v_slot = [links.slot() for _ in range(n_tx)]
    order = (1, 3, 2)
    w_start(0)
    w_start(1)
    for k in range(1, n_tx):
        links.send(v_slot[k], v_in, v_out.at[:, cols(z)], z_dev[k])
    t_start(0)
    places = [x_out.at[:, :, cols(z)], c_out.at[:, :, cols(z)], wu_out.at[pl.ds(pl.multiple_of(z * d_loc, d_loc), d_loc)], wd_out.at[pl.ds(pl.multiple_of(z * d_loc, d_loc), d_loc)], v_out.at[:, cols(z)]]
    own_out = []
    for i, (copy, src, dst) in enumerate(zip(own_in, (x_tmp, c_tmp, w_tmp.at[0], w_tmp.at[1], v_tmp), places)):
        copy.wait()
        own_out.append(pltpu.make_async_copy(src, dst, local_sems.at[i]))
        own_out[-1].start()
    w_pass(0, 1)
    w_pass(1, 1)
    t_start(1)
    w_pass(0, 2)
    w_pass(1, 2)
    for k in order:
        t_pass(0, k)
    w_pass(0, 3)
    w_pass(1, 3)
    for k in order:
        t_pass_y(0, k)
    for k in order:
        t_pass(1, k)
    for k in order:
        t_pass_y(1, k)
    w_finish(0)
    w_finish(1)
    t_finish(0)
    t_finish(1)
    for k in range(1, n_tx):
        links.arrive(v_slot[k], v_out.at[:, cols((z + n_tx - k) % n_tx)], y_dev)
    links.drain()
    for copy in own_out:
        copy.wait()


def gather_inputs(x_act, cot_out, w_up, w_dt, vecs, n_tx, n_ty):
    batch, seq, d_loc = x_act.shape
    chunk = batch * seq // (n_tx * n_ty)
    d_model, ff = d_loc * n_tx, w_up.shape[1]
    any_spec = pl.BlockSpec(memory_space=pl.ANY)
    tokens = jax.ShapeDtypeStruct((n_ty, chunk, d_model), BF16)
    weight = jax.ShapeDtypeStruct((d_model, ff), BF16)
    slots = 2 * (2 * n_tx + n_tx) + 2 * (n_tx + n_tx + 2 * n_tx) + n_tx
    return pl.pallas_call(
        functools.partial(gather_kernel, n_tx=n_tx),
        in_specs=[any_spec] * 5,
        out_specs=[any_spec] * 5,
        out_shape=[tokens, tokens, weight, weight, jax.ShapeDtypeStruct((vecs.shape[0], d_model), BF16)],
        scratch_shapes=[
            pltpu.VMEM((n_ty, chunk, d_loc), BF16),
            pltpu.VMEM((n_ty, chunk, d_loc), BF16),
            pltpu.VMEM((2, d_loc, ff), BF16),
            pltpu.VMEM((vecs.shape[0], d_loc), BF16),
            pltpu.SemaphoreType.DMA((slots,)),
            pltpu.SemaphoreType.DMA((slots,)),
            pltpu.SemaphoreType.DMA((5,)),
        ],
        compiler_params=pltpu.CompilerParams(collective_id=0, has_side_effects=True),
        cost_estimate=pl.CostEstimate(flops=40_000_000_000, bytes_accessed=40_000_000, transcendentals=0),
        name="gather_inputs",
    )(x_act.reshape(n_tx, n_ty, chunk, d_loc), cot_out.reshape(n_tx, n_ty, chunk, d_loc), w_up, w_dt, vecs)


def tail_kernel(
    qkv, d_ctx, u, d_pre, h1, x, cot, w_d, w_a, w_u, vecs, small, cos_tab, sin_tab, turn_tab,
    y_out, dx_out, small_out, dw_out,
    qkv_b, dctx_b, u_b, dpre_b, h1_b, x_b, cot_b, q_s, k_s, dq_s, ctx_s, dqkv_s, acc, dbq, ln_acc, pw, dw_buf,
    part, rc, sy, ry, fin, x_own, c_own, sm_buf, send_sems, recv_sems, local_sems, *, n_tx, blk,
):
    g, z, t, core, y, t_core, t_y, t_diag = neighbours()
    core_dev, y_dev = (g, z, t_core), (g, z, t_y)
    z_dev = [(g, (z + k) % n_tx, t) for k in range(n_tx)]
    n_seq, seq, d_model = x.shape
    width = d_ctx.shape[-1]
    d_loc = d_model // n_tx
    heads, steps = width // HEAD, seq // blk
    sub = seq // 4
    links = Links(send_sems, recv_sems)
    outs = (y_out, dx_out)
    late = ((u, u_b), (d_pre, dpre_b), (h1, h1_b), (x, x_b), (cot, cot_b))

    def load_early(s):
        slot = s % 2
        return [
            pltpu.make_async_copy(qkv.at[s], qkv_b.at[slot], local_sems.at[slot]),
            pltpu.make_async_copy(d_ctx.at[s], dctx_b.at[slot], local_sems.at[2 + slot]),
        ]

    def load_late(s):
        return [pltpu.make_async_copy(src.at[s], dst, local_sems.at[4 + i]) for i, (src, dst) in enumerate(late)]

    for copy in load_early(0):
        copy.start()
    acc[...] = jnp.zeros_like(acc)
    dbq[...] = jnp.zeros_like(dbq)
    ln_acc[...] = jnp.zeros_like(ln_acc)
    enter([core_dev, y_dev] + z_dev[1:])

    def cols(s):
        return pl.ds(pl.multiple_of(s * d_loc, d_loc), d_loc)

    def rows(c):
        return pl.ds(pl.multiple_of(c * sub, sub), sub)

    core_slot = [[links.slot(n_seq) for _ in range(2)] for _ in range(2)]
    y_slot = [links.slot(n_seq) for _ in range(2)]
    z_slot = [[links.slot(n_seq) for _ in range(n_tx)] for _ in range(2)]
    ag_y = [[links.slot(n_seq) for _ in range(n_tx)] for _ in range(2)]
    ag_c = [[[links.slot(n_seq) for _ in range(2)] for _ in range(n_tx)] for _ in range(2)]
    sm_slot = [links.slot() for _ in range(5)]
    rs_slot = [links.slot() for _ in range(n_tx)]

    turn = turn_tab[...]

    def rotate(v, sign):
        return (v.astype(F32) * cos_tab[...] + sign * (dot_nn(v, turn) * sin_tab[...])).astype(BF16)

    def attend(s):
        slot = s % 2
        q_s[...] = rotate(qkv_b[slot, :, 0:width], 1.0) * BF16(HEAD ** -0.5)
        k_s[...] = rotate(qkv_b[slot, :, width:2 * width], 1.0)
        row = lax.broadcasted_iota(jnp.int32, (blk, blk), 0)
        col = lax.broadcasted_iota(jnp.int32, (blk, blk), 1)
        causal = row >= col
        dk_heads, dv_heads = [], []
        for h in range(heads):
            hs = slice(h * HEAD, (h + 1) * HEAD)
            k_h = k_s[:, hs]
            v_h = qkv_b[slot, :, 2 * width + h * HEAD:2 * width + (h + 1) * HEAD]
            dk = [None] * steps
            dv = [None] * steps
            for i in range(steps):
                at = slice(i * blk, (i + 1) * blk)
                n = (i + 1) * blk
                q_i = q_s[at, hs]
                do_i = dctx_b[slot, at, hs]
                sc = dot_nt(q_i, k_h[:n])
                s_diag = jnp.where(causal, sc[:, n - blk:], -1e30)
                sc = s_diag if i == 0 else jnp.concatenate([sc[:, :n - blk], s_diag], axis=1)
                p = jnp.exp(sc - jnp.max(sc, axis=1, keepdims=True))
                p = p * (1.0 / jnp.sum(p, axis=1, keepdims=True))
                p_b = p.astype(BF16)
                ctx_s[at, hs] = dot_nn(p_b, v_h[:n]).astype(BF16)
                dp = dot_nt(do_i, v_h[:n]).astype(BF16).astype(F32)
                ds = (p * (dp - jnp.sum(p * dp, axis=1, keepdims=True))).astype(BF16)
                dq_s[at, hs] = (dot_nn(ds, k_h[:n]) * HEAD ** -0.5).astype(BF16)
                dk_i = dot_tn(ds, q_i)
                dv_i = dot_tn(p_b, do_i)
                for j in range(i + 1):
                    part_k, part_v = dk_i[j * blk:(j + 1) * blk], dv_i[j * blk:(j + 1) * blk]
                    dk[j] = part_k if dk[j] is None else dk[j] + part_k
                    dv[j] = part_v if dv[j] is None else dv[j] + part_v
            dk_heads.append(jnp.concatenate(dk, axis=0).astype(BF16))
            dv_heads.append(jnp.concatenate(dv, axis=0).astype(BF16))
        pieces = (rotate(dq_s[...], -1.0), rotate(jnp.concatenate(dk_heads, axis=1), -1.0), jnp.concatenate(dv_heads, axis=1))
        for pos, piece in enumerate(pieces):
            at = slice(pos * width, (pos + 1) * width)
            dqkv_s[:, at] = piece
            dbq[:, at] += piece.astype(F32).reshape(seq // 8, 8, width).sum(0)

    def forward_part(s):
        def body(r, carry):
            at = pl.ds(pl.multiple_of(r * blk, blk), blk)
            total = dot_nt(u_b[at, :], w_d[...]) + dot_nt(ctx_s[at, :], w_a[:, 3 * width:])
            part[0, s, at, :] = total.astype(BF16)
            return carry
        lax.fori_loop(0, steps, body, 0)

    def backward_part(s):
        def body(r, carry):
            at = pl.ds(pl.multiple_of(r * blk, blk), blk)
            d_h1 = dot_nt(dqkv_s[at, :], w_a[:, :3 * width]).astype(BF16).astype(F32)
            d_h2 = dot_nt(dpre_b[at, :], w_u[...]).astype(BF16).astype(F32)
            xf = x_b[at, :].astype(F32)
            mean = jnp.mean(xf, axis=-1, keepdims=True)
            xh = (xf - mean) * lax.rsqrt(jnp.mean(xf * xf, axis=-1, keepdims=True) - mean * mean + LN_EPS)
            part[1, s, at, :] = (d_h1 * vecs[0:1, :] + d_h2 * vecs[1:2, :]).astype(BF16)
            for i, v in enumerate((d_h1 * xh, d_h1, d_h2 * xh, d_h2)):
                ln_acc[i] += v.reshape(blk // 8, 8, d_model).sum(0)
            return carry
        lax.fori_loop(0, steps, body, 0)

    def weight_part():
        def body(r, carry):
            at = pl.ds(pl.multiple_of(r * d_loc, d_loc), d_loc)
            acc[at, :3 * width] += dot_tn(h1_b[:, at], dqkv_s[...])
            acc[at, 3 * width:] += dot_tn(cot_b[:, at], ctx_s[...])
            return carry
        lax.fori_loop(0, n_tx, body, 0)

    def share(a, s):
        for j, yy in enumerate((1 - y, y)):
            links.send(core_slot[a][j] + s, part.at[a, s, rows(yy * 2 + 1 - core)], rc.at[a, s, yy], core_dev)

    step = 32

    def give(s):
        for a in range(2):
            links.arrive(core_slot[a][0] + s, rc.at[a, s, 1 - y], core_dev)

            def body(r, carry):
                at = pl.ds(pl.multiple_of(r * step, step), step)
                mine = part[a, s, pl.ds(pl.multiple_of(t_y * sub + r * step, step), step), :]
                sy[a, s, at, :] = (mine.astype(F32) + rc[a, s, 1 - y, at, :].astype(F32)).astype(BF16)
                return carry
            lax.fori_loop(0, sub // step, body, 0)
            links.send(y_slot[a] + s, sy.at[a, s], ry.at[a, s], y_dev)

    def finish(s):
        for a in range(2):
            links.arrive(core_slot[a][1] + s, rc.at[a, s, y], core_dev)
            links.arrive(y_slot[a] + s, ry.at[a, s], y_dev)

            def body(r, carry):
                at = pl.ds(pl.multiple_of(r * step, step), step)
                whole = pl.ds(pl.multiple_of(t * sub + r * step, step), step)
                total = part[a, s, whole, :].astype(F32) + rc[a, s, y, at, :].astype(F32) + ry[a, s, at, :].astype(F32)
                xf = x_own[s, at, :].astype(F32)
                if a == 0:
                    out = xf + total + vecs[2:3, :]
                else:
                    mean = jnp.mean(xf, axis=-1, keepdims=True)
                    inv = lax.rsqrt(jnp.mean(xf * xf, axis=-1, keepdims=True) - mean * mean + LN_EPS)
                    xh = (xf - mean) * inv
                    m1 = jnp.mean(total, axis=-1, keepdims=True)
                    m2 = jnp.mean(total * xh, axis=-1, keepdims=True)
                    out = c_own[s, at, :].astype(F32) + inv * (total - m1 - xh * m2)
                fin[a, s, at, :] = out.astype(BF16)
                return carry
            lax.fori_loop(0, sub // step, body, 0)
            place = outs[a].at[z * n_seq + s, rows(t)]
            for k in (2, 1, 3):
                links.send(z_slot[a][k] + s, fin.at[a, s, :, cols((z + k) % n_tx)], place, z_dev[k])
            mine = fin.at[a, s, :, cols(z)]
            pltpu.make_async_copy(mine, place, local_sems.at[9 + a * n_seq + s]).start()
            links.send(ag_y[a][0] + s, mine, place, y_dev)
            links.send(ag_c[a][0][0] + s, mine, place, core_dev)

    def src(k):
        return (z + n_tx - k) % n_tx

    def forward(s):
        for a in range(2):
            for k in (1, 3, 2):
                place = outs[a].at[src(k) * n_seq + s, rows(t)]
                links.arrive(z_slot[a][k] + s, place, y_dev)
                links.send(ag_y[a][k] + s, place, place, y_dev)
                links.send(ag_c[a][k][0] + s, place, place, core_dev)

    def forward_y(s):
        for a in range(2):
            for k in (0, 1, 3, 2):
                place = outs[a].at[src(k) * n_seq + s, rows(t_y)]
                links.arrive(ag_y[a][k] + s, place, y_dev)
                links.send(ag_c[a][k][1] + s, place, place, core_dev)

    def settle(s):
        for a in range(2):
            for k in range(n_tx):
                for j, who in enumerate((t_core, t_diag)):
                    links.arrive(ag_c[a][k][j] + s, outs[a].at[src(k) * n_seq + s, rows(who)], core_dev)
            pltpu.make_async_copy(fin.at[a, s, :, cols(z)], outs[a].at[z * n_seq + s, rows(t)], local_sems.at[9 + a * n_seq + s]).wait()
        done(s)

    def done(s):
        for a in range(2):
            for j, yy in enumerate((1 - y, y)):
                links.make(core_slot[a][j] + s, part.at[a, s, rows(yy * 2 + 1 - core)], rc.at[a, s, yy], core_dev).wait_send()
            links.make(y_slot[a] + s, sy.at[a, s], ry.at[a, s], y_dev).wait_send()
            for k in range(n_tx):
                mine = fin.at[a, s, :, cols((z + k) % n_tx)]
                place = outs[a].at[src(k) * n_seq + s, rows(t)]
                if k:
                    links.make(z_slot[a][k] + s, mine, place, z_dev[k]).wait_send()
                links.make(ag_y[a][k] + s, place, place, y_dev).wait_send()
                for j in range(2):
                    links.make(ag_c[a][k][j] + s, place, place, core_dev).wait_send()

    own_in = [
        pltpu.make_async_copy(x.at[:, rows(t), :], x_own, local_sems.at[9 + 2 * n_seq]),
        pltpu.make_async_copy(cot.at[:, rows(t), :], c_own, local_sems.at[10 + 2 * n_seq]),
    ]
    for copy in own_in:
        copy.start()
    for copy in own_in:
        copy.wait()

    def one(s, carry):
        for copy in load_early(s):
            copy.wait()

        @pl.when(s < n_seq - 1)
        def _():
            for copy in load_early(s + 1):
                copy.start()

        for copy in load_late(s):
            copy.start()
        attend(s)

        @pl.when(s > 0)
        def _():
            finish(s - 1)

        for copy in load_late(s):
            copy.wait()
        forward_part(s)
        share(0, s)
        backward_part(s)
        share(1, s)

        @pl.when(s > 0)
        def _():
            forward(s - 1)

        weight_part()
        give(s)

        @pl.when(s > 0)
        def _():
            forward_y(s - 1)

        return carry

    lax.fori_loop(0, n_seq, one, 0)
    last = n_seq - 1
    pw[...] = acc[...].astype(BF16)
    for k in (2, 1, 3):
        links.send(rs_slot[k], pw.at[cols((z + k) % n_tx)], dw_buf.at[k - 1], z_dev[k])
    for i in range(4):
        sm_buf[0, i:i + 1, :] = ln_acc[i].sum(0, keepdims=True)
    sm_buf[0, 4:5, :] = small[4:5, :]
    sm_buf[0, 5:6, 0:3 * width] = dbq[...].sum(0, keepdims=True)
    sm_buf[0, 5:6, 3 * width:] = jnp.zeros((1, d_model - 3 * width), F32)
    sm_buf[0, 6:8, :] = jnp.zeros((2, d_model), F32)
    links.send(sm_slot[0], sm_buf.at[0], sm_buf.at[1], core_dev)
    row = lax.broadcasted_iota(jnp.int32, (8, d_model), 0)
    finish(last)
    links.arrive(sm_slot[0], sm_buf.at[1], core_dev)
    sm_buf[2] = sm_buf[0] + jnp.where(row < 4, sm_buf[1], 0.0)
    links.send(sm_slot[1], sm_buf.at[2], sm_buf.at[3], y_dev)
    forward(last)
    links.arrive(sm_slot[1], sm_buf.at[3], y_dev)
    sm_buf[4] = sm_buf[2] + jnp.where(row < 4, sm_buf[3], 0.0)
    for k in range(1, n_tx):
        links.send(sm_slot[1 + k], sm_buf.at[4], sm_buf.at[4 + k], z_dev[k])
    forward_y(last)
    for k in range(1, n_tx):
        links.arrive(rs_slot[k], dw_buf.at[k - 1], y_dev)
    dw_out[...] = acc[cols(z), :]
    for k in range(1, n_tx):
        dw_out[...] += dw_buf[k - 1].astype(F32)
    for k in range(1, n_tx):
        links.arrive(sm_slot[1 + k], sm_buf.at[4 + k], y_dev)
    small_out[...] = sm_buf[4] + sm_buf[5] + sm_buf[6] + sm_buf[7]
    for s in range(n_seq):
        settle(s)
    for k in range(1, n_tx):
        links.make(rs_slot[k], pw.at[cols((z + k) % n_tx)], dw_buf.at[k - 1], z_dev[k]).wait_send()
        links.make(sm_slot[1 + k], sm_buf.at[4], sm_buf.at[4 + k], z_dev[k]).wait_send()
    links.make(sm_slot[0], sm_buf.at[0], sm_buf.at[1], core_dev).wait_send()
    links.make(sm_slot[1], sm_buf.at[2], sm_buf.at[3], y_dev).wait_send()


def layer_tail(qkv, d_ctx, u, d_pre, h1, x, cot, w_d, w_a, w_u, vecs, small, n_tx, n_ty):
    n_seq, seq, d_model = x.shape
    width, d_loc, blk, sub = d_ctx.shape[-1], d_model // n_tx, 256, seq // n_ty
    any_spec, vmem = pl.BlockSpec(memory_space=pl.ANY), pl.BlockSpec(memory_space=pltpu.VMEM)
    out = jax.ShapeDtypeStruct((n_seq * n_tx, seq, d_loc), BF16)
    cos_tab, sin_tab = rope_tables(seq, width)
    slots = n_seq * 2 * (3 + 4 * n_tx) + 5 + n_tx
    wide = lambda *lead: pltpu.VMEM(lead + (seq, d_model), BF16)
    piece = lambda *lead: pltpu.VMEM(lead + (sub, d_model), BF16)
    return pl.pallas_call(
        functools.partial(tail_kernel, n_tx=n_tx, blk=blk),
        in_specs=[any_spec] * 7 + [vmem] * 8,
        out_specs=[any_spec, any_spec, vmem, vmem],
        out_shape=[out, out, jax.ShapeDtypeStruct((8, d_model), F32), jax.ShapeDtypeStruct((d_loc, d_model), F32)],
        scratch_shapes=[
            pltpu.VMEM((2, seq, 3 * width), BF16),
            pltpu.VMEM((2, seq, width), BF16),
            wide(), wide(), wide(), wide(), wide(),
            pltpu.VMEM((seq, width), BF16),
            pltpu.VMEM((seq, width), BF16),
            pltpu.VMEM((seq, width), BF16),
            pltpu.VMEM((seq, width), BF16),
            pltpu.VMEM((seq, 3 * width), BF16),
            pltpu.VMEM((d_model, d_model), F32),
            pltpu.VMEM((8, 3 * width), F32),
            pltpu.VMEM((4, 8, d_model), F32),
            pltpu.VMEM((d_model, d_model), BF16),
            pltpu.VMEM((n_tx - 1, d_loc, d_model), BF16),
            wide(2, n_seq),
            piece(2, n_seq, 2),
            piece(2, n_seq),
            piece(2, n_seq),
            piece(2, n_seq),
            piece(n_seq),
            piece(n_seq),
            pltpu.VMEM((8, 8, d_model), F32),
            pltpu.SemaphoreType.DMA((slots,)),
            pltpu.SemaphoreType.DMA((slots,)),
            pltpu.SemaphoreType.DMA((11 + 2 * n_seq,)),
        ],
        compiler_params=pltpu.CompilerParams(collective_id=1, has_side_effects=True, vmem_limit_bytes=67_000_000),
        cost_estimate=pl.CostEstimate(flops=60_000_000_000, bytes_accessed=60_000_000, transcendentals=0),
        name="layer_tail",
    )(qkv, d_ctx, u, d_pre, h1, x, cot, w_d, w_a, w_u, vecs, small, cos_tab, sin_tab, rope_turn(width))


def solution(mesh):
    n_tx, n_ty = mesh.shape['tx'], mesh.shape['ty']
    act_spec = P('dp', None, 'tx')
    width_spec = P('tx')
    in_specs = (act_spec, act_spec, width_spec, width_spec, width_spec, width_spec, P('tx', 'ty', None), P('ty', None), P('ty', 'tx'), width_spec, P('tx', 'ty'), P('ty'), P('ty', 'tx'), width_spec)
    width_out = P(('dp', 'tx'))
    out_specs = (act_spec, act_spec, width_out, width_out, width_out, width_out, P(('dp', 'tx'), 'ty', None), P(('dp', 'ty'), None), P(('dp', 'ty'), 'tx'), width_out, P(('dp', 'tx'), 'ty'), P(('dp', 'ty')), P(('dp', 'ty'), 'tx'), width_out)
    def body(x_act, cot_out, ln1_gain, ln1_bias, ln2_gain, ln2_bias, w_qkv, b_qkv, w_dense, b_dense, w_up, b_up, w_down, b_down):
        batch, seq, d_loc = x_act.shape
        d_model = d_loc * n_tx
        heads = w_qkv.shape[1]
        hw = heads * HEAD
        n_b = batch // n_tx
        tok = n_b * seq
        z, g = lax.axis_index('tx'), lax.axis_index('dp')

        half = d_loc // 2

        def gather_rows(w):
            mine = lax.dynamic_slice_in_dim(w, g * half, half, 0)
            return lax.all_gather(mine, ('tx', 'dp'), axis=0, tiled=True)

        wq_loc = w_qkv.reshape(d_loc, heads, 3, HEAD).transpose(0, 2, 1, 3).reshape(d_loc, 3 * hw)
        w_a = gather_rows(jnp.concatenate([wq_loc, w_dense.T], axis=1))
        w_q, w_o = w_a[:, :3 * hw], w_a[:, 3 * hw:]
        vec_loc = jnp.stack([ln1_gain, ln1_bias, ln2_gain, ln2_bias, b_dense, b_down], axis=0)
        vec_loc = jnp.pad(vec_loc, ((0, 10), (0, 0)))
        x_chunks, cot_chunks, w_u, w_dt, vecs = gather_inputs(x_act, cot_out, w_up, w_down.T, vec_loc, n_tx, n_ty)
        x, cot = x_chunks.reshape(tok, d_model), cot_chunks.reshape(tok, d_model)
        g1, be1, g2, be2, b_o, b_d = [vecs[i].astype(F32) for i in range(6)]

        x_f = x.astype(F32)
        mean = x_f.mean(-1, keepdims=True)
        inv_std = lax.rsqrt((x_f * x_f).mean(-1, keepdims=True) - mean * mean + LN_EPS)
        x_hat = (x_f - mean) * inv_std
        h1 = (x_hat * g1 + be1).astype(BF16)
        h2 = (x_hat * g2 + be2).astype(BF16)

        pre = (dot_nn(h2, w_u) + b_up.astype(F32)).astype(BF16)
        d_gelu = dot_nn(cot, w_dt).astype(BF16)
        u, gelu_pullback = jax.vjp(gelu_bf16, pre)
        (d_pre,) = gelu_pullback(d_gelu)

        def scatter_grad(part):
            return lax.psum_scatter(part, 'tx', scatter_dimension=0, tiled=True)

        part_down, part_up = dot_tn(cot, u).astype(BF16), dot_tn(h2, d_pre).astype(BF16)
        sum_down, sum_up = scatter_grad(part_down), scatter_grad(part_up)
        d_w_down, d_w_up = sum_down.astype(F32).T, sum_up.astype(F32)
        d_b_up = d_pre.astype(F32).sum(0)

        bq = b_qkv.astype(F32).reshape(heads, 3, HEAD).transpose(1, 0, 2).reshape(3 * hw)
        qkv = (dot_nn(h1, w_q) + bq).astype(BF16)
        cot_late, _, _ = lax.optimization_barrier((cot, part_down, part_up))
        d_ctx = dot_nn(cot_late, w_o).astype(BF16)
        small = jnp.pad(d_b_up[None], ((4, 3), (0, d_model - d_b_up.shape[0])))
        rows = jnp.pad(jnp.stack([g1, g2, b_o + b_d], axis=0), ((0, 5), (0, 0)))
        by_seq = lambda a: a.reshape(n_b, seq, a.shape[-1])
        y_out, dx_act, total, d_w_a = layer_tail(by_seq(qkv), by_seq(d_ctx), by_seq(u), by_seq(d_pre), by_seq(h1), by_seq(x), by_seq(cot), w_dt, w_a, w_u, rows, small, n_tx, n_ty)
        d_w_qkv = d_w_a[:, :3 * hw].reshape(d_loc, 3, heads, HEAD).transpose(0, 2, 1, 3).reshape(d_loc, heads, 3 * HEAD)
        d_w_dense = d_w_a[:, 3 * hw:].T
        ln_sum = lax.dynamic_slice(total, (0, z * d_loc), (4, d_loc))
        d_b_up = total[4, :d_b_up.shape[0]]
        d_b_qkv = total[5, :3 * hw].reshape(3, heads, HEAD).transpose(1, 0, 2).reshape(heads, 3 * HEAD)
        d_b_out = cot_out.astype(F32).sum((0, 1))
        return (y_out, dx_act, ln_sum[0], ln_sum[1], ln_sum[2], ln_sum[3], d_w_qkv, d_b_qkv, d_w_dense, d_b_out, d_w_up, d_b_up, d_w_down, d_b_out)

    return jax.shard_map(body, mesh=mesh, in_specs=in_specs, out_specs=out_specs, check_vma=False)
```

```python
import functools
import jax
import jax.numpy as jnp
from jax import lax
from jax.experimental import pallas as pl
from jax.experimental.pallas import tpu as pltpu
from jax.sharding import PartitionSpec as P

LN_EPS = 1e-5
ROPE_BASE = 10000.0
HEAD = 64
ROT = 16
F32 = jnp.float32
BF16 = jnp.bfloat16

def rope_tables(seq_len, width):
    inv_freq = ROPE_BASE ** (-jnp.arange(0, ROT, 2, dtype=F32) / ROT)
    angles = jnp.arange(seq_len, dtype=F32)[:, None] * inv_freq[None, :]
    angles = jnp.concatenate([angles, angles], axis=-1)
    pad = ((0, 0), (0, HEAD - ROT))
    cos_head = jnp.pad(jnp.cos(angles), pad, constant_values=1.0)
    sin_head = jnp.pad(jnp.sin(angles), pad)
    return jnp.tile(cos_head, (1, width // HEAD)), jnp.tile(sin_head, (1, width // HEAD))


def rope_turn(width):
    row = lax.broadcasted_iota(jnp.int32, (width, width), 0)
    col = lax.broadcasted_iota(jnp.int32, (width, width), 1)
    lane = col % HEAD
    minus = (row == col + ROT // 2) & (lane < ROT // 2)
    plus = (row == col - ROT // 2) & (lane >= ROT // 2) & (lane < ROT)
    return (plus.astype(F32) - minus.astype(F32)).astype(BF16)


def dot_nn(a, b):
    return lax.dot_general(a, b, (((1,), (0,)), ((), ())), preferred_element_type=F32)


def dot_nt(a, b):
    return lax.dot_general(a, b, (((1,), (1,)), ((), ())), preferred_element_type=F32)


def dot_tn(a, b):
    return lax.dot_general(a, b, (((0,), (0,)), ((), ())), preferred_element_type=F32)


MESH = pl.DeviceIdType.MESH
BOTH = range(2)
OTHERS = (1, 3, 2)


def block(i, size):
    return pl.ds(pl.multiple_of(i * size, size), size)


def row_mean(v):
    return jnp.mean(v, axis=-1, keepdims=True)


def normalise(v):
    mean = row_mean(v)
    inv_std = lax.rsqrt(row_mean(v * v) - mean * mean + LN_EPS)
    return (v - mean) * inv_std, inv_std


def fold(v):
    return v.reshape(v.shape[0] // 8, 8, v.shape[1]).sum(0)


class Links:
    def __init__(self, send_sems, recv_sems):
        self.send_sems, self.recv_sems, self.count = send_sems, recv_sems, 0

    def slot(self, count=1):
        self.count += count
        return self.count - count

    def make(self, slot, src, dst, dev):
        return pltpu.make_async_remote_copy(src_ref=src, dst_ref=dst, send_sem=self.send_sems.at[slot], recv_sem=self.recv_sems.at[slot], device_id=dev, device_id_type=MESH)

    def send(self, slot, src, dst, dev, cond=None):
        def go():
            self.make(slot, src, dst, dev).start()
        go() if cond is None else pl.when(cond)(go)

    def arrive(self, slot, dst, dev, cond=None):
        def go():
            self.make(slot, dst, dst, dev).wait_recv()
        go() if cond is None else pl.when(cond)(go)

    def sent(self, slot, like, cond=None):
        def go():
            self.make(slot, like, like, (0, 0, 0)).wait_send()
        go() if cond is None else pl.when(cond)(go)


def neighbours():
    g, z, t = lax.axis_index('dp'), lax.axis_index('tx'), lax.axis_index('ty')
    core, y = t % 2, t // 2
    t_core, t_y, t_diag = y * 2 + 1 - core, (1 - y) * 2 + core, (1 - y) * 2 + 1 - core
    return g, z, t, core, y, t_core, t_y, t_diag


def enter(devices):
    barrier = pltpu.get_barrier_semaphore()
    for dev in devices:
        pl.semaphore_signal(barrier, inc=1, device_id=dev, device_id_type=MESH)
    pl.semaphore_wait(barrier, len(devices))


def front_kernel(
    x_in, c_in, wu_in, wd_in, wa_in, v_in, b_qkv, b_up,
    x_out, c_out, wu_out, wd_out, wa_out, v_out, h1_out, qkv_out, u_out, dpre_out, dctx_out, dwd_out, dwu_out, dbup_out,
    x_v, c_v, wu_v, wd_v, wa_v, h1_v, h2_v, u_v, gp_v, qkv_v, dpre_v, dctx_v, dw_v,
    send_sems, recv_sems, local_sems, out_sems, *, n_tx, n_ty, blk,
):
    g, z, t, core, y, t_core, t_y, t_diag = neighbours()
    core_dev, y_dev, x_dev = (g, z, t_core), (g, z, t_y), (1 - g, z, t)
    z_dev = [(g, (z + k) % n_tx, t) for k in range(n_tx)]
    left, right = (g, z - 1, t), (g, z + 1, t)
    d_loc = x_in.shape[-1]
    half = d_loc // 2
    tok = x_v.shape[0]
    chunk = tok // n_ty
    width = dctx_v.shape[-1]
    links = Links(send_sems, recv_sems)

    def cols(s):
        return block(s, d_loc)

    def rows(c):
        return block(c, chunk)

    def w_rows(s, group):
        return pl.ds(pl.multiple_of(s * d_loc + group * half, half), half)

    own = [pltpu.make_async_copy(v_in, v_out.at[:, cols(z)], local_sems.at[0])]
    for i, (src, dst) in enumerate(((wu_in, wu_v), (wa_in, wa_v), (wd_in, wd_v))):
        own.append(pltpu.make_async_copy(src, dst.at[cols(z), :], local_sems.at[1 + i]))
    for i, (src, dst) in enumerate(((x_in, x_v), (c_in, c_v))):
        for c in range(n_ty):
            own.append(pltpu.make_async_copy(src.at[z, c], dst.at[pl.ds(c * chunk, chunk), cols(z)], local_sems.at[4 + i * n_ty + c]))
    for copy in own:
        copy.start()
    enter([core_dev, y_dev, x_dev] + z_dev[1:])

    weights = ((wu_in, wu_v), (wa_in, wa_v), (wd_in, wd_v))
    w_slot = [[links.slot() for _ in range(2 * n_tx)] for _ in weights]
    x_slot = [[links.slot() for _ in range(n_tx)] for _ in weights]

    def w_send(w, hops, src):
        s_left, s_right = z - hops, z + hops
        links.send(w_slot[w][hops + 1], src(s_left), weights[w][1].at[w_rows(s_left, g), :], right, (s_left >= 0) & (z < n_tx - 1))
        links.send(w_slot[w][n_tx + hops + 1], src(s_right), weights[w][1].at[w_rows(s_right, g), :], left, (s_right < n_tx) & (z > 0))

    def w_start(w):
        mine = weights[w][0].at[block(g, half), :]
        w_send(w, 0, lambda s: mine)

    def w_sides(hops):
        return (hops, hops, z - hops, z - hops >= 0), (n_tx + hops, n_tx - hops, z + hops, z + hops < n_tx)

    def w_pass(w, hops):
        out = weights[w][1]
        for slot, x_at, s, ok in w_sides(hops):
            place = out.at[w_rows(s, g), :]
            links.arrive(w_slot[w][slot], place, right, ok)
            links.send(x_slot[w][x_at], place, place, x_dev, ok)
        if hops < n_tx - 1:
            w_send(w, hops, lambda s: out.at[w_rows(s, g), :])

    def w_finish(w):
        for hops in OTHERS:
            for slot, x_at, s, ok in w_sides(hops):
                links.arrive(x_slot[w][x_at], weights[w][1].at[w_rows(s, 1 - g), :], x_dev, ok)

    arrays = ((x_in, x_v), (c_in, c_v))
    z_slot = [[links.slot() for _ in range(n_tx)] for _ in arrays]
    y_slot = [[links.slot() for _ in range(n_tx)] for _ in arrays]
    c_slot = [[[links.slot() for _ in BOTH] for _ in range(n_tx)] for _ in arrays]
    v_slot = [links.slot() for _ in range(n_tx)]

    def src_cols(k):
        return cols((z + n_tx - k) % n_tx)

    def t_start(a):
        for k in OTHERS:
            links.send(z_slot[a][k], arrays[a][0].at[(z + k) % n_tx, t], arrays[a][1].at[rows(t), cols(z)], z_dev[k])

    def t_pass(a, k):
        place = arrays[a][1].at[rows(t), src_cols(k)]
        links.arrive(z_slot[a][k], place, y_dev)
        links.send(y_slot[a][k], place, place, y_dev)
        links.send(c_slot[a][k][0], place, place, core_dev)

    def t_pass_y(a, k):
        place = arrays[a][1].at[rows(t_y), src_cols(k)]
        links.arrive(y_slot[a][k], place, y_dev)
        links.send(c_slot[a][k][1], place, place, core_dev)

    def t_finish(a):
        for k in OTHERS:
            for j, c in enumerate((t_core, t_diag)):
                links.arrive(c_slot[a][k][j], arrays[a][1].at[rows(c), src_cols(k)], core_dev)

    w_start(0)
    w_start(1)
    for k in OTHERS:
        links.send(v_slot[k], v_in, v_out.at[:, cols(z)], z_dev[k])
    t_start(0)
    w_pass(0, 1)
    w_pass(1, 1)
    for k in OTHERS:
        t_pass(0, k)
    w_pass(0, 2)
    w_pass(1, 2)
    w_start(2)
    t_start(1)
    for k in OTHERS:
        t_pass_y(0, k)
    w_pass(0, 3)
    w_pass(1, 3)
    w_finish(0)
    w_finish(1)
    t_finish(0)
    for k in OTHERS:
        links.arrive(v_slot[k], v_out.at[:, src_cols(k)], y_dev)
    for copy in own:
        copy.wait()

    outputs = []

    def write(src, dst):
        copy = pltpu.make_async_copy(src, dst, out_sems.at[len(outputs)])
        copy.start()
        outputs.append(copy)

    write(x_v, x_out)
    write(wu_v, wu_out)
    write(wa_v, wa_out)
    late_steps = {
        0: lambda: w_pass(2, 1),
        2: lambda: [t_pass(1, k) for k in OTHERS],
        3: lambda: w_pass(2, 2),
        4: lambda: [t_pass_y(1, k) for k in OTHERS],
        6: lambda: w_pass(2, 3),
    }
    vec = v_out[...].astype(F32)

    def forward(i, carry):
        at = block(i, blk)
        xf = x_v[at, :].astype(F32)
        xh, _ = normalise(xf)
        h1 = (xh * vec[0:1] + vec[1:2]).astype(BF16)
        h2 = (xh * vec[2:3] + vec[3:4]).astype(BF16)
        h1_v[at, :] = h1
        h2_v[at, :] = h2
        qkv_v[at, :] = (dot_nn(h1, wa_v[:, :3 * width]) + b_qkv[0:1, :]).astype(BF16)
        pre = (dot_nn(h2, wu_v[...]) + b_up[0:1, :]).astype(BF16).astype(F32)
        cdf = 0.5 * (1.0 + lax.erf(pre * (0.5 ** 0.5)))
        u_v[at, :] = (pre * cdf).astype(BF16)
        gp_v[at, :] = cdf + pre * (jnp.exp(-0.5 * pre * pre) * (1.0 / (2.0 * jnp.pi) ** 0.5))
        for when, what in late_steps.items():
            pl.when(i == when)(lambda: (what(), None)[1])
        return carry

    lax.fori_loop(0, tok // blk, forward, 0)
    write(h1_v, h1_out)
    write(qkv_v, qkv_out)
    write(u_v, u_out)
    w_finish(2)
    t_finish(1)
    write(c_v, c_out)
    write(wd_v, wd_out)
    dbup_out[...] = jnp.zeros_like(dbup_out)

    def backward(i, carry):
        at = block(i, blk)
        cot = c_v[at, :]
        d_gelu = dot_nn(cot, wd_v[...]).astype(BF16).astype(F32)
        d_pre = (d_gelu * gp_v[at, :]).astype(BF16)
        dpre_v[at, :] = d_pre
        dbup_out[...] += fold(d_pre.astype(F32))
        dctx_v[at, :] = dot_nn(cot, wa_v[:, 3 * width:]).astype(BF16)
        return carry

    lax.fori_loop(0, tok // blk, backward, 0)
    write(dpre_v, dpre_out)
    write(dctx_v, dctx_out)
    for i, (lhs, rhs, out) in enumerate(((c_v, u_v, dwd_out), (h2_v, dpre_v, dwu_out))):
        def weight(r, carry):
            dw_v[i, cols(r), :] = dot_tn(lhs[:, cols(r)], rhs[...]).astype(BF16)
            return carry
        lax.fori_loop(0, n_tx, weight, 0)
        write(dw_v.at[i], out)
    piece = x_v.at[pl.ds(0, chunk), pl.ds(0, d_loc)]
    for a in BOTH:
        for k in OTHERS:
            for slot in (z_slot[a][k], y_slot[a][k], *c_slot[a][k]):
                links.sent(slot, piece)
    for w in range(len(weights)):
        shard = weights[w][1].at[pl.ds(0, half), :]
        for hops in range(n_tx):
            if hops:
                for _, x_at, _, ok in w_sides(hops):
                    links.sent(x_slot[w][x_at], shard, ok)
            if hops < n_tx - 1:
                links.sent(w_slot[w][hops + 1], shard, (z - hops >= 0) & (z < n_tx - 1))
                links.sent(w_slot[w][n_tx + hops + 1], shard, (z + hops < n_tx) & (z > 0))
    for k in OTHERS:
        links.sent(v_slot[k], v_in)
    for copy in outputs:
        copy.wait()


def layer_front(x_act, cot_out, w_up, w_dt, w_a, vecs, b_qkv, b_up, n_tx, n_ty):
    batch, seq, d_loc = x_act.shape
    tok = batch * seq // n_tx
    d_model, ff, width, blk = d_loc * n_tx, w_up.shape[1], b_qkv.shape[1] // 3, 256
    any_spec, vmem = pl.BlockSpec(memory_space=pl.ANY), pl.BlockSpec(memory_space=pltpu.VMEM)
    arr = lambda *shape: jax.ShapeDtypeStruct(shape, BF16)
    buf = lambda *shape: pltpu.VMEM(shape, BF16)
    slots = 3 * 3 * n_tx + 2 * 4 * n_tx + n_tx
    split = lambda a: a.reshape(n_tx, n_ty, tok // n_ty, d_loc)
    return pl.pallas_call(
        functools.partial(front_kernel, n_tx=n_tx, n_ty=n_ty, blk=blk),
        in_specs=[any_spec] * 6 + [vmem] * 2,
        out_specs=[any_spec] * 5 + [vmem] + [any_spec] * 7 + [vmem],
        out_shape=[
            arr(tok, d_model), arr(tok, d_model), arr(d_model, ff), arr(d_model, ff), arr(d_model, 4 * width), arr(vecs.shape[0], d_model),
            arr(tok, d_model), arr(tok, 3 * width), arr(tok, ff), arr(tok, ff), arr(tok, width), arr(d_model, ff), arr(d_model, ff),
            jax.ShapeDtypeStruct((8, ff), F32),
        ],
        scratch_shapes=[
            buf(tok, d_model), buf(tok, d_model), buf(d_model, ff), buf(d_model, ff), buf(d_model, 4 * width),
            buf(tok, d_model), buf(tok, d_model), buf(tok, ff), pltpu.VMEM((tok, ff), F32), buf(tok, 3 * width), buf(tok, ff), buf(tok, width),
            buf(2, d_model, ff),
            pltpu.SemaphoreType.DMA((slots,)),
            pltpu.SemaphoreType.DMA((slots,)),
            pltpu.SemaphoreType.DMA((4 + 2 * n_ty,)),
            pltpu.SemaphoreType.DMA((12,)),
        ],
        compiler_params=pltpu.CompilerParams(collective_id=0, has_side_effects=True, vmem_limit_bytes=67_000_000),
        cost_estimate=pl.CostEstimate(flops=60_000_000_000, bytes_accessed=60_000_000, transcendentals=0),
        name="layer_front",
    )(split(x_act), split(cot_out), w_up, w_dt, w_a, vecs, b_qkv, b_up)


def tail_kernel(
    qkv, d_ctx, u, d_pre, h1, x, cot, w_d, w_a, w_u, vecs, small, cos_tab, sin_tab, turn_tab,
    y_out, dx_out, small_out, dw_out,
    qkv_b, dctx_b, u_b, dpre_b, h1_b, x_b, cot_b, q_s, k_s, dq_s, ctx_s, dqkv_s, acc, dbq, ln_acc, pw, dw_buf,
    part, rc, sy, ry, fin, x_own, c_own, sm_buf, send_sems, recv_sems, local_sems, *, n_tx, blk,
):
    g, z, t, core, y, t_core, t_y, t_diag = neighbours()
    core_dev, y_dev = (g, z, t_core), (g, z, t_y)
    z_dev = [(g, (z + k) % n_tx, t) for k in range(n_tx)]
    n_seq, seq, d_model = x.shape
    width = d_ctx.shape[-1]
    d_loc = d_model // n_tx
    heads, steps = width // HEAD, seq // blk
    sub = seq // 4
    links = Links(send_sems, recv_sems)
    outs = (y_out, dx_out)
    late = ((u, u_b), (d_pre, dpre_b), (h1, h1_b), (x, x_b), (cot, cot_b))

    def load_early(s):
        slot = s % 2
        return [
            pltpu.make_async_copy(qkv.at[s], qkv_b.at[slot], local_sems.at[slot]),
            pltpu.make_async_copy(d_ctx.at[s], dctx_b.at[slot], local_sems.at[2 + slot]),
        ]

    def load_late(s):
        return [pltpu.make_async_copy(src.at[s], dst, local_sems.at[4 + i]) for i, (src, dst) in enumerate(late)]

    for copy in load_early(0):
        copy.start()
    acc[...] = jnp.zeros_like(acc)
    dbq[...] = jnp.zeros_like(dbq)
    ln_acc[...] = jnp.zeros_like(ln_acc)
    enter([core_dev, y_dev] + z_dev[1:])

    def cols(s):
        return block(s, d_loc)

    def rows(c):
        return block(c, sub)

    core_slot = [[links.slot(n_seq) for _ in BOTH] for _ in BOTH]
    y_slot = [links.slot(n_seq) for _ in BOTH]
    z_slot = [[links.slot(n_seq) for _ in range(n_tx)] for _ in BOTH]
    ag_y = [[links.slot(n_seq) for _ in range(n_tx)] for _ in BOTH]
    ag_c = [[[links.slot(n_seq) for _ in BOTH] for _ in range(n_tx)] for _ in BOTH]
    sm_slot = [links.slot() for _ in range(5)]
    rs_slot = [links.slot() for _ in range(n_tx)]

    turn = turn_tab[...]

    def rotate(v, sign):
        return (v.astype(F32) * cos_tab[...] + sign * (dot_nn(v, turn) * sin_tab[...])).astype(BF16)

    def attend(s):
        slot = s % 2
        q_s[...] = rotate(qkv_b[slot, :, 0:width], 1.0) * BF16(HEAD ** -0.5)
        k_s[...] = rotate(qkv_b[slot, :, width:2 * width], 1.0)
        row = lax.broadcasted_iota(jnp.int32, (blk, blk), 0)
        col = lax.broadcasted_iota(jnp.int32, (blk, blk), 1)
        causal = row >= col
        dk_heads, dv_heads = [], []
        for h in range(heads):
            hs = slice(h * HEAD, (h + 1) * HEAD)
            k_h = k_s[:, hs]
            v_h = qkv_b[slot, :, 2 * width + h * HEAD:2 * width + (h + 1) * HEAD]
            dk = [None] * steps
            dv = [None] * steps
            for i in range(steps):
                at = slice(i * blk, (i + 1) * blk)
                n = (i + 1) * blk
                q_i = q_s[at, hs]
                do_i = dctx_b[slot, at, hs]
                sc = dot_nt(q_i, k_h[:n])
                s_diag = jnp.where(causal, sc[:, n - blk:], -1e30)
                sc = s_diag if i == 0 else jnp.concatenate([sc[:, :n - blk], s_diag], axis=1)
                p = jnp.exp(sc - jnp.max(sc, axis=1, keepdims=True))
                p = p * (1.0 / jnp.sum(p, axis=1, keepdims=True))
                p_b = p.astype(BF16)
                ctx_s[at, hs] = dot_nn(p_b, v_h[:n]).astype(BF16)
                dp = dot_nt(do_i, v_h[:n]).astype(BF16).astype(F32)
                ds = (p * (dp - jnp.sum(p * dp, axis=1, keepdims=True))).astype(BF16)
                dq_s[at, hs] = (dot_nn(ds, k_h[:n]) * HEAD ** -0.5).astype(BF16)
                dk_i = dot_tn(ds, q_i)
                dv_i = dot_tn(p_b, do_i)
                for j in range(i + 1):
                    part_k, part_v = dk_i[j * blk:(j + 1) * blk], dv_i[j * blk:(j + 1) * blk]
                    dk[j] = part_k if dk[j] is None else dk[j] + part_k
                    dv[j] = part_v if dv[j] is None else dv[j] + part_v
            dk_heads.append(jnp.concatenate(dk, axis=0).astype(BF16))
            dv_heads.append(jnp.concatenate(dv, axis=0).astype(BF16))
        pieces = (rotate(dq_s[...], -1.0), rotate(jnp.concatenate(dk_heads, axis=1), -1.0), jnp.concatenate(dv_heads, axis=1))
        for pos, piece in enumerate(pieces):
            at = slice(pos * width, (pos + 1) * width)
            dqkv_s[:, at] = piece
            dbq[:, at] += fold(piece.astype(F32))

    def forward_part(s):
        def body(r, carry):
            at = block(r, blk)
            total = dot_nt(u_b[at, :], w_d[...]) + dot_nt(ctx_s[at, :], w_a[:, 3 * width:])
            part[0, s, at, :] = total.astype(BF16)
            return carry
        lax.fori_loop(0, steps, body, 0)

    def backward_part(s):
        def body(r, carry):
            at = block(r, blk)
            d_h1 = dot_nt(dqkv_s[at, :], w_a[:, :3 * width]).astype(BF16).astype(F32)
            d_h2 = dot_nt(dpre_b[at, :], w_u[...]).astype(BF16).astype(F32)
            xf = x_b[at, :].astype(F32)
            xh, _ = normalise(xf)
            part[1, s, at, :] = (d_h1 * vecs[0:1, :] + d_h2 * vecs[1:2, :]).astype(BF16)
            for i, v in enumerate((d_h1 * xh, d_h1, d_h2 * xh, d_h2)):
                ln_acc[i] += fold(v)
            return carry
        lax.fori_loop(0, steps, body, 0)

    def weight_part():
        def body(r, carry):
            at = block(r, d_loc)
            acc[at, :3 * width] += dot_tn(h1_b[:, at], dqkv_s[...])
            acc[at, 3 * width:] += dot_tn(cot_b[:, at], ctx_s[...])
            return carry
        lax.fori_loop(0, n_tx, body, 0)

    def share(a, s):
        for j, yy in enumerate((1 - y, y)):
            links.send(core_slot[a][j] + s, part.at[a, s, rows(yy * 2 + 1 - core)], rc.at[a, s, yy], core_dev)

    step = 32

    def give(s):
        for a in BOTH:
            links.arrive(core_slot[a][0] + s, rc.at[a, s, 1 - y], core_dev)

            def body(r, carry):
                at = block(r, step)
                mine = part[a, s, pl.ds(pl.multiple_of(t_y * sub + r * step, step), step), :]
                sy[a, s, at, :] = (mine.astype(F32) + rc[a, s, 1 - y, at, :].astype(F32)).astype(BF16)
                return carry
            lax.fori_loop(0, sub // step, body, 0)
            links.send(y_slot[a] + s, sy.at[a, s], ry.at[a, s], y_dev)

    def finish(s):
        for a in BOTH:
            links.arrive(core_slot[a][1] + s, rc.at[a, s, y], core_dev)
            links.arrive(y_slot[a] + s, ry.at[a, s], y_dev)

            def body(r, carry):
                at = block(r, step)
                whole = pl.ds(pl.multiple_of(t * sub + r * step, step), step)
                total = part[a, s, whole, :].astype(F32) + rc[a, s, y, at, :].astype(F32) + ry[a, s, at, :].astype(F32)
                xf = x_own[s, at, :].astype(F32)
                if a == 0:
                    out = xf + total + vecs[2:3, :]
                else:
                    xh, inv = normalise(xf)
                    out = c_own[s, at, :].astype(F32) + inv * (total - row_mean(total) - xh * row_mean(total * xh))
                fin[a, s, at, :] = out.astype(BF16)
                return carry
            lax.fori_loop(0, sub // step, body, 0)
            place = outs[a].at[z * n_seq + s, rows(t)]
            for k in OTHERS:
                links.send(z_slot[a][k] + s, fin.at[a, s, :, cols((z + k) % n_tx)], place, z_dev[k])
            mine = fin.at[a, s, :, cols(z)]
            pltpu.make_async_copy(mine, place, local_sems.at[9 + a * n_seq + s]).start()
            links.send(ag_y[a][0] + s, mine, place, y_dev)
            links.send(ag_c[a][0][0] + s, mine, place, core_dev)

    def src(k):
        return (z + n_tx - k) % n_tx

    def forward(s):
        for a in BOTH:
            for k in OTHERS:
                place = outs[a].at[src(k) * n_seq + s, rows(t)]
                links.arrive(z_slot[a][k] + s, place, y_dev)
                links.send(ag_y[a][k] + s, place, place, y_dev)
                links.send(ag_c[a][k][0] + s, place, place, core_dev)

    def forward_y(s):
        for a in BOTH:
            for k in (0, *OTHERS):
                place = outs[a].at[src(k) * n_seq + s, rows(t_y)]
                links.arrive(ag_y[a][k] + s, place, y_dev)
                links.send(ag_c[a][k][1] + s, place, place, core_dev)

    def settle(s):
        for a in BOTH:
            for k in range(n_tx):
                for j, who in enumerate((t_core, t_diag)):
                    links.arrive(ag_c[a][k][j] + s, outs[a].at[src(k) * n_seq + s, rows(who)], core_dev)
            pltpu.make_async_copy(fin.at[a, s, :, cols(z)], outs[a].at[z * n_seq + s, rows(t)], local_sems.at[9 + a * n_seq + s]).wait()
        done(s)

    def done(s):
        for a in BOTH:
            for j, yy in enumerate((1 - y, y)):
                links.make(core_slot[a][j] + s, part.at[a, s, rows(yy * 2 + 1 - core)], rc.at[a, s, yy], core_dev).wait_send()
            links.make(y_slot[a] + s, sy.at[a, s], ry.at[a, s], y_dev).wait_send()
            for k in range(n_tx):
                mine = fin.at[a, s, :, cols((z + k) % n_tx)]
                place = outs[a].at[src(k) * n_seq + s, rows(t)]
                if k:
                    links.make(z_slot[a][k] + s, mine, place, z_dev[k]).wait_send()
                links.make(ag_y[a][k] + s, place, place, y_dev).wait_send()
                for j in BOTH:
                    links.make(ag_c[a][k][j] + s, place, place, core_dev).wait_send()

    own_in = [
        pltpu.make_async_copy(x.at[:, rows(t), :], x_own, local_sems.at[9 + 2 * n_seq]),
        pltpu.make_async_copy(cot.at[:, rows(t), :], c_own, local_sems.at[10 + 2 * n_seq]),
    ]
    for copy in own_in:
        copy.start()
    for copy in own_in:
        copy.wait()

    def one(s, carry):
        for copy in load_early(s):
            copy.wait()

        @pl.when(s < n_seq - 1)
        def _():
            for copy in load_early(s + 1):
                copy.start()

        for copy in load_late(s):
            copy.start()
        attend(s)
        for copy in load_late(s):
            copy.wait()
        forward_part(s)
        share(0, s)
        backward_part(s)
        share(1, s)
        weight_part()
        give(s)

        @pl.when(s > 0)
        def _():
            finish(s - 1)

        return carry

    lax.fori_loop(0, n_seq, one, 0)
    last = n_seq - 1
    pw[...] = acc[...].astype(BF16)
    for k in OTHERS:
        links.send(rs_slot[k], pw.at[cols((z + k) % n_tx)], dw_buf.at[k - 1], z_dev[k])
    for i in range(4):
        sm_buf[0, i:i + 1, :] = ln_acc[i].sum(0, keepdims=True)
    sm_buf[0, 4:5, :] = small[4:5, :]
    sm_buf[0, 5:6, 0:3 * width] = dbq[...].sum(0, keepdims=True)
    sm_buf[0, 5:6, 3 * width:] = jnp.zeros((1, d_model - 3 * width), F32)
    sm_buf[0, 6:8, :] = jnp.zeros((2, d_model), F32)
    links.send(sm_slot[0], sm_buf.at[0], sm_buf.at[1], core_dev)
    row = lax.broadcasted_iota(jnp.int32, (8, d_model), 0)
    forward(0)
    finish(last)
    links.arrive(sm_slot[0], sm_buf.at[1], core_dev)
    sm_buf[2] = sm_buf[0] + jnp.where(row < 4, sm_buf[1], 0.0)
    links.send(sm_slot[1], sm_buf.at[2], sm_buf.at[3], y_dev)
    forward(1)
    forward_y(0)
    links.arrive(sm_slot[1], sm_buf.at[3], y_dev)
    sm_buf[4] = sm_buf[2] + jnp.where(row < 4, sm_buf[3], 0.0)
    for k in OTHERS:
        links.send(sm_slot[1 + k], sm_buf.at[4], sm_buf.at[4 + k], z_dev[k])
    forward(last)
    forward_y(1)
    forward_y(last)
    for k in OTHERS:
        links.arrive(rs_slot[k], dw_buf.at[k - 1], y_dev)
    dw_out[...] = acc[cols(z), :]
    for k in OTHERS:
        dw_out[...] += dw_buf[k - 1].astype(F32)
    for k in OTHERS:
        links.arrive(sm_slot[1 + k], sm_buf.at[4 + k], y_dev)
    small_out[...] = sm_buf[4] + sm_buf[5] + sm_buf[6] + sm_buf[7]
    for s in range(n_seq):
        settle(s)
    for k in OTHERS:
        links.make(rs_slot[k], pw.at[cols((z + k) % n_tx)], dw_buf.at[k - 1], z_dev[k]).wait_send()
        links.make(sm_slot[1 + k], sm_buf.at[4], sm_buf.at[4 + k], z_dev[k]).wait_send()
    links.make(sm_slot[0], sm_buf.at[0], sm_buf.at[1], core_dev).wait_send()
    links.make(sm_slot[1], sm_buf.at[2], sm_buf.at[3], y_dev).wait_send()


def layer_tail(qkv, d_ctx, u, d_pre, h1, x, cot, w_d, w_a, w_u, vecs, small, n_tx, n_ty):
    n_seq, seq, d_model = x.shape
    width, d_loc, blk, sub = d_ctx.shape[-1], d_model // n_tx, 256, seq // n_ty
    any_spec, vmem = pl.BlockSpec(memory_space=pl.ANY), pl.BlockSpec(memory_space=pltpu.VMEM)
    out = jax.ShapeDtypeStruct((n_seq * n_tx, seq, d_loc), BF16)
    cos_tab, sin_tab = rope_tables(seq, width)
    slots = n_seq * 2 * (3 + 4 * n_tx) + 5 + n_tx
    wide = lambda *lead: pltpu.VMEM(lead + (seq, d_model), BF16)
    piece = lambda *lead: pltpu.VMEM(lead + (sub, d_model), BF16)
    return pl.pallas_call(
        functools.partial(tail_kernel, n_tx=n_tx, blk=blk),
        in_specs=[any_spec] * 7 + [vmem] * 8,
        out_specs=[any_spec, any_spec, vmem, vmem],
        out_shape=[out, out, jax.ShapeDtypeStruct((8, d_model), F32), jax.ShapeDtypeStruct((d_loc, d_model), F32)],
        scratch_shapes=[
            pltpu.VMEM((2, seq, 3 * width), BF16),
            pltpu.VMEM((2, seq, width), BF16),
            wide(), wide(), wide(), wide(), wide(),
            pltpu.VMEM((seq, width), BF16),
            pltpu.VMEM((seq, width), BF16),
            pltpu.VMEM((seq, width), BF16),
            pltpu.VMEM((seq, width), BF16),
            pltpu.VMEM((seq, 3 * width), BF16),
            pltpu.VMEM((d_model, d_model), F32),
            pltpu.VMEM((8, 3 * width), F32),
            pltpu.VMEM((4, 8, d_model), F32),
            pltpu.VMEM((d_model, d_model), BF16),
            pltpu.VMEM((n_tx - 1, d_loc, d_model), BF16),
            wide(2, n_seq),
            piece(2, n_seq, 2),
            piece(2, n_seq),
            piece(2, n_seq),
            piece(2, n_seq),
            piece(n_seq),
            piece(n_seq),
            pltpu.VMEM((8, 8, d_model), F32),
            pltpu.SemaphoreType.DMA((slots,)),
            pltpu.SemaphoreType.DMA((slots,)),
            pltpu.SemaphoreType.DMA((11 + 2 * n_seq,)),
        ],
        compiler_params=pltpu.CompilerParams(collective_id=1, has_side_effects=True, vmem_limit_bytes=67_000_000),
        cost_estimate=pl.CostEstimate(flops=60_000_000_000, bytes_accessed=60_000_000, transcendentals=0),
        name="layer_tail",
    )(qkv, d_ctx, u, d_pre, h1, x, cot, w_d, w_a, w_u, vecs, small, cos_tab, sin_tab, rope_turn(width))


def solution(mesh):
    n_tx, n_ty = mesh.shape['tx'], mesh.shape['ty']
    act_spec = P('dp', None, 'tx')
    width_spec = P('tx')
    in_specs = (act_spec, act_spec, width_spec, width_spec, width_spec, width_spec, P('tx', 'ty', None), P('ty', None), P('ty', 'tx'), width_spec, P('tx', 'ty'), P('ty'), P('ty', 'tx'), width_spec)
    width_out = P(('dp', 'tx'))
    out_specs = (act_spec, act_spec, width_out, width_out, width_out, width_out, P(('dp', 'tx'), 'ty', None), P(('dp', 'ty'), None), P(('dp', 'ty'), 'tx'), width_out, P(('dp', 'tx'), 'ty'), P(('dp', 'ty')), P(('dp', 'ty'), 'tx'), width_out)
    def body(x_act, cot_out, ln1_gain, ln1_bias, ln2_gain, ln2_bias, w_qkv, b_qkv, w_dense, b_dense, w_up, b_up, w_down, b_down):
        batch, seq, d_loc = x_act.shape
        d_model = d_loc * n_tx
        heads = w_qkv.shape[1]
        hw = heads * HEAD
        n_b = batch // n_tx
        tok = n_b * seq
        z, g = lax.axis_index('tx'), lax.axis_index('dp')

        wq_loc = w_qkv.reshape(d_loc, heads, 3, HEAD).transpose(0, 2, 1, 3).reshape(d_loc, 3 * hw)
        vec_loc = jnp.stack([ln1_gain, ln1_bias, ln2_gain, ln2_bias, b_dense, b_down], axis=0)
        vec_loc = jnp.pad(vec_loc, ((0, 10), (0, 0)))
        bq = b_qkv.astype(F32).reshape(heads, 3, HEAD).transpose(1, 0, 2).reshape(1, 3 * hw)
        row8 = lambda a: jnp.pad(a, ((0, 7), (0, 0)))
        x, cot, w_u, w_dt, w_a, vecs, h1, qkv, u, d_pre, d_ctx, part_down, part_up, d_bup = layer_front(
            x_act, cot_out, w_up, w_down.T, jnp.concatenate([wq_loc, w_dense.T], axis=1), vec_loc, row8(bq), row8(b_up.astype(F32)[None]), n_tx, n_ty)
        g1, g2, b_o, b_d = [vecs[i].astype(F32) for i in (0, 2, 4, 5)]

        def scatter_grad(part):
            return lax.psum_scatter(part, 'tx', scatter_dimension=0, tiled=True)

        sum_down, sum_up = scatter_grad(part_down), scatter_grad(part_up)
        d_w_down, d_w_up = sum_down.astype(F32).T, sum_up.astype(F32)
        d_b_up = d_bup.sum(0)
        small = jnp.pad(d_b_up[None], ((4, 3), (0, d_model - d_b_up.shape[0])))
        rows = jnp.pad(jnp.stack([g1, g2, b_o + b_d], axis=0), ((0, 5), (0, 0)))
        by_seq = lambda a: a.reshape(n_b, seq, a.shape[-1])
        y_out, dx_act, total, d_w_a = layer_tail(by_seq(qkv), by_seq(d_ctx), by_seq(u), by_seq(d_pre), by_seq(h1), by_seq(x), by_seq(cot), w_dt, w_a, w_u, rows, small, n_tx, n_ty)
        d_w_qkv = d_w_a[:, :3 * hw].reshape(d_loc, 3, heads, HEAD).transpose(0, 2, 1, 3).reshape(d_loc, heads, 3 * HEAD)
        d_w_dense = d_w_a[:, 3 * hw:].T
        ln_sum = lax.dynamic_slice(total, (0, z * d_loc), (4, d_loc))
        d_b_up = total[4, :d_b_up.shape[0]]
        d_b_qkv = total[5, :3 * hw].reshape(3, heads, HEAD).transpose(1, 0, 2).reshape(heads, 3 * HEAD)
        d_b_out = cot_out.astype(F32).sum((0, 1))
        return (y_out, dx_act, ln_sum[0], ln_sum[1], ln_sum[2], ln_sum[3], d_w_qkv, d_b_qkv, d_w_dense, d_b_out, d_w_up, d_b_up, d_w_down, d_b_out)

    return jax.shard_map(body, mesh=mesh, in_specs=in_specs, out_specs=out_specs, check_vma=False)
```

```python
import functools
import jax
import jax.numpy as jnp
from jax import lax
from jax.experimental import pallas as pl
from jax.experimental.pallas import tpu as pltpu
from jax.sharding import PartitionSpec as P

LN_EPS = 1e-5
ROPE_BASE = 10000.0
HEAD = 64
ROT = 16
F32 = jnp.float32
BF16 = jnp.bfloat16

def rope_tables(seq_len, width):
    inv_freq = ROPE_BASE ** (-jnp.arange(0, ROT, 2, dtype=F32) / ROT)
    angles = jnp.arange(seq_len, dtype=F32)[:, None] * inv_freq[None, :]
    angles = jnp.concatenate([angles, angles], axis=-1)
    pad = ((0, 0), (0, HEAD - ROT))
    cos_head = jnp.pad(jnp.cos(angles), pad, constant_values=1.0)
    sin_head = jnp.pad(jnp.sin(angles), pad)
    return jnp.tile(cos_head, (1, width // HEAD)), jnp.tile(sin_head, (1, width // HEAD))


def rope_turn(width):
    row = lax.broadcasted_iota(jnp.int32, (width, width), 0)
    col = lax.broadcasted_iota(jnp.int32, (width, width), 1)
    lane = col % HEAD
    minus = (row == col + ROT // 2) & (lane < ROT // 2)
    plus = (row == col - ROT // 2) & (lane >= ROT // 2) & (lane < ROT)
    return (plus.astype(F32) - minus.astype(F32)).astype(BF16)


def dot_nn(a, b):
    return lax.dot_general(a, b, (((1,), (0,)), ((), ())), preferred_element_type=F32)


def dot_nt(a, b):
    return lax.dot_general(a, b, (((1,), (1,)), ((), ())), preferred_element_type=F32)


def dot_tn(a, b):
    return lax.dot_general(a, b, (((0,), (0,)), ((), ())), preferred_element_type=F32)


MESH = pl.DeviceIdType.MESH
BOTH = range(2)
OTHERS = (1, 3, 2)


def block(i, size):
    return pl.ds(pl.multiple_of(i * size, size), size)


def row_mean(v):
    return jnp.mean(v, axis=-1, keepdims=True)


def normalise(v):
    mean = row_mean(v)
    inv_std = lax.rsqrt(row_mean(v * v) - mean * mean + LN_EPS)
    return (v - mean) * inv_std, inv_std


def row_sum(v):
    return jnp.sum(v, axis=-1, keepdims=True)


def loop(count, body):
    lax.fori_loop(0, count, lambda i, carry: (body(i), carry)[1], 0)


def fold(v):
    return v.reshape(v.shape[0] // 8, 8, v.shape[1]).sum(0)


class Links:
    def __init__(self, send_sems, recv_sems):
        self.send_sems, self.recv_sems, self.count = send_sems, recv_sems, 0

    def slot(self, count=1):
        self.count += count
        return self.count - count

    def make(self, slot, src, dst, dev):
        return pltpu.make_async_remote_copy(src_ref=src, dst_ref=dst, send_sem=self.send_sems.at[slot], recv_sem=self.recv_sems.at[slot], device_id=dev, device_id_type=MESH)

    def send(self, slot, src, dst, dev, cond=None):
        def go():
            self.make(slot, src, dst, dev).start()
        go() if cond is None else pl.when(cond)(go)

    def arrive(self, slot, dst, dev, cond=None):
        def go():
            self.make(slot, dst, dst, dev).wait_recv()
        go() if cond is None else pl.when(cond)(go)

    def sent(self, slot, like, cond=None):
        def go():
            self.make(slot, like, like, (0, 0, 0)).wait_send()
        go() if cond is None else pl.when(cond)(go)


def neighbours():
    g, z, t = lax.axis_index('dp'), lax.axis_index('tx'), lax.axis_index('ty')
    core, y = t % 2, t // 2
    t_core, t_y, t_diag = y * 2 + 1 - core, (1 - y) * 2 + core, (1 - y) * 2 + 1 - core
    return g, z, t, core, y, t_core, t_y, t_diag


def enter(devices):
    barrier = pltpu.get_barrier_semaphore()
    for dev in devices:
        pl.semaphore_signal(barrier, inc=1, device_id=dev, device_id_type=MESH)
    pl.semaphore_wait(barrier, len(devices))


def front_kernel(
    x_in, c_in, wu_in, wd_in, wa_in, v_in, b_qkv, b_up,
    x_out, c_out, wu_out, wd_out, wa_out, v_out, h1_out, qkv_out, u_out, dpre_out, dctx_out, dwd_out, dwu_out, dbup_out,
    x_v, c_v, wu_v, wd_v, wa_v, h1_v, h2_v, u_v, gp_v, qkv_v, dpre_v, dctx_v, dwd_v, dwu_v,
    send_sems, recv_sems, local_sems, out_sems, *, n_tx, n_ty, blk,
):
    g, z, t, core, y, t_core, t_y, t_diag = neighbours()
    core_dev, y_dev, x_dev = (g, z, t_core), (g, z, t_y), (1 - g, z, t)
    z_dev = [(g, (z + k) % n_tx, t) for k in range(n_tx)]
    left, right = (g, z - 1, t), (g, z + 1, t)
    end = n_tx - 1
    d_loc = x_in.shape[-1]
    half = d_loc // 2
    tok = x_v.shape[0]
    chunk = tok // n_ty
    width = dctx_v.shape[-1]
    links = Links(send_sems, recv_sems)

    def cols(s):
        return block(s, d_loc)

    def rows(c):
        return block(c, chunk)

    def w_rows(s, group):
        return pl.ds(pl.multiple_of(s * d_loc + group * half, half), half)

    own = [pltpu.make_async_copy(v_in, v_out.at[:, cols(z)], local_sems.at[0])]
    for i, (src, dst) in enumerate(((wu_in, wu_v), (wa_in, wa_v), (wd_in, wd_v))):
        own.append(pltpu.make_async_copy(src, dst.at[cols(z), :], local_sems.at[1 + i]))
    for i, (src, dst) in enumerate(((x_in, x_v), (c_in, c_v))):
        for c in range(n_ty):
            own.append(pltpu.make_async_copy(src.at[z, c], dst.at[pl.ds(c * chunk, chunk), cols(z)], local_sems.at[4 + i * n_ty + c]))
    for copy in own:
        copy.start()
    enter([core_dev, y_dev, x_dev] + z_dev[1:])

    weights = ((wu_in, wu_v), (wa_in, wa_v), (wd_in, wd_v))
    w_slot = [[links.slot() for _ in range(2 * n_tx)] for _ in weights]
    x_slot = [[links.slot() for _ in range(n_tx)] for _ in weights]

    def w_send(w, hops, src):
        s_left, s_right = z - hops, z + hops
        links.send(w_slot[w][hops + 1], src(s_left), weights[w][1].at[w_rows(s_left, g), :], right, (s_left >= 0) & (z < end))
        links.send(w_slot[w][n_tx + hops + 1], src(s_right), weights[w][1].at[w_rows(s_right, g), :], left, (s_right < n_tx) & (z > 0))

    def w_start(w):
        mine = weights[w][0].at[block(g, half), :]
        w_send(w, 0, lambda s: mine)

    def w_sides(hops):
        return (hops, hops, z - hops, z - hops >= 0), (n_tx + hops, n_tx - hops, z + hops, z + hops < n_tx)

    def w_pass(w, hops):
        out = weights[w][1]
        for slot, x_at, s, ok in w_sides(hops):
            place = out.at[w_rows(s, g), :]
            links.arrive(w_slot[w][slot], place, right, ok)
            links.send(x_slot[w][x_at], place, place, x_dev, ok)
        if hops < end:
            w_send(w, hops, lambda s: out.at[w_rows(s, g), :])

    def w_finish(w):
        for hops in OTHERS:
            for slot, x_at, s, ok in w_sides(hops):
                links.arrive(x_slot[w][x_at], weights[w][1].at[w_rows(s, 1 - g), :], x_dev, ok)

    arrays = ((x_in, x_v), (c_in, c_v))
    z_slot = [[links.slot() for _ in range(n_tx)] for _ in arrays]
    y_slot = [[links.slot() for _ in range(n_tx)] for _ in arrays]
    c_slot = [[[links.slot() for _ in BOTH] for _ in range(n_tx)] for _ in arrays]
    v_slot = [links.slot() for _ in range(n_tx)]

    def src_cols(k):
        return cols((z + n_tx - k) % n_tx)

    def t_start(a):
        for k in OTHERS:
            links.send(z_slot[a][k], arrays[a][0].at[(z + k) % n_tx, t], arrays[a][1].at[rows(t), cols(z)], z_dev[k])

    def t_pass(a, k):
        place = arrays[a][1].at[rows(t), src_cols(k)]
        links.arrive(z_slot[a][k], place, y_dev)
        links.send(y_slot[a][k], place, place, y_dev)
        links.send(c_slot[a][k][0], place, place, core_dev)

    def t_pass_y(a, k):
        place = arrays[a][1].at[rows(t_y), src_cols(k)]
        links.arrive(y_slot[a][k], place, y_dev)
        links.send(c_slot[a][k][1], place, place, core_dev)

    def t_finish(a):
        for k in OTHERS:
            for j, c in enumerate((t_core, t_diag)):
                links.arrive(c_slot[a][k][j], arrays[a][1].at[rows(c), src_cols(k)], core_dev)

    for w in BOTH:
        w_start(w)
    for k in OTHERS:
        links.send(v_slot[k], v_in, v_out.at[:, cols(z)], z_dev[k])
    t_start(0)
    for w in BOTH:
        w_pass(w, 1)
    for k in OTHERS:
        t_pass(0, k)
    for w in BOTH:
        w_pass(w, 2)
    w_start(2)
    t_start(1)
    for k in OTHERS:
        t_pass_y(0, k)
    for w in BOTH:
        w_pass(w, 3)
        w_finish(w)
    t_finish(0)
    for k in OTHERS:
        links.arrive(v_slot[k], v_out.at[:, src_cols(k)], y_dev)
    for copy in own:
        copy.wait()

    outputs = []

    def write(src, dst):
        copy = pltpu.make_async_copy(src, dst, out_sems.at[len(outputs)])
        copy.start()
        outputs.append(copy)

    write(x_v, x_out)
    write(wu_v, wu_out)
    write(wa_v, wa_out)

    def tokens(step):
        for k in OTHERS:
            step(1, k)

    late_steps = tuple(enumerate((lambda: w_pass(2, 1), None, lambda: tokens(t_pass), lambda: w_pass(2, 2), lambda: tokens(t_pass_y), None, lambda: w_pass(2, 3))))
    vec = v_out[...].astype(F32)
    g1, be1, g2, be2 = [vec[i:i + 1] for i in range(4)]

    def forward(i):
        at = block(i, blk)
        xf = x_v[at, :].astype(F32)
        xh, _ = normalise(xf)
        h1 = (xh * g1 + be1).astype(BF16)
        h2 = (xh * g2 + be2).astype(BF16)
        h1_v[at, :] = h1
        h2_v[at, :] = h2
        qkv_v[at, :] = (dot_nn(h1, wa_v[:, :3 * width]) + b_qkv[...]).astype(BF16)
        pre = (dot_nn(h2, wu_v[...]) + b_up[...]).astype(BF16).astype(F32)
        cdf = 0.5 * (1.0 + lax.erf(pre * (0.5 ** 0.5)))
        u_v[at, :] = (pre * cdf).astype(BF16)
        gp_v[at, :] = cdf + pre * (jnp.exp(-0.5 * pre * pre) * (1.0 / (2.0 * jnp.pi) ** 0.5))
        for when, what in late_steps:
            if what:
                pl.when(i == when)(what)

    loop(tok // blk, forward)
    write(h1_v, h1_out)
    write(qkv_v, qkv_out)
    write(u_v, u_out)
    w_finish(2)
    t_finish(1)
    write(c_v, c_out)
    write(wd_v, wd_out)
    dbup_out[...] = jnp.zeros_like(dbup_out)

    def backward(i):
        at = block(i, blk)
        cot = c_v[at, :]
        d_gelu = dot_nn(cot, wd_v[...]).astype(BF16).astype(F32)
        d_pre = (d_gelu * gp_v[at, :]).astype(BF16)
        dpre_v[at, :] = d_pre
        dbup_out[...] += fold(d_pre.astype(F32))
        dctx_v[at, :] = dot_nn(cot, wa_v[:, 3 * width:]).astype(BF16)

    loop(tok // blk, backward)
    write(dpre_v, dpre_out)
    write(dctx_v, dctx_out)

    def down(r):
        dwd_v[r] = dot_tn(u_v[...], c_v[:, cols(r)]).astype(BF16)

    def up(r):
        dwu_v[r] = dot_tn(h2_v[:, cols(r)], dpre_v[...]).astype(BF16)

    loop(n_tx, down)
    write(dwd_v, dwd_out)
    loop(n_tx, up)
    write(dwu_v, dwu_out)
    piece = x_v.at[pl.ds(0, chunk), pl.ds(0, d_loc)]
    for a in BOTH:
        for k in OTHERS:
            for slot in (z_slot[a][k], y_slot[a][k], *c_slot[a][k]):
                links.sent(slot, piece)
    for w in range(len(weights)):
        shard = weights[w][1].at[pl.ds(0, half), :]
        for hops in range(n_tx):
            if hops:
                for _, x_at, _, ok in w_sides(hops):
                    links.sent(x_slot[w][x_at], shard, ok)
            if hops < end:
                links.sent(w_slot[w][hops + 1], shard, (z - hops >= 0) & (z < end))
                links.sent(w_slot[w][n_tx + hops + 1], shard, (z + hops < n_tx) & (z > 0))
    for k in OTHERS:
        links.sent(v_slot[k], v_in)
    for copy in outputs:
        copy.wait()


def layer_front(x_act, cot_out, w_up, w_dt, w_a, vecs, b_qkv, b_up, n_tx, n_ty):
    batch, seq, d_loc = x_act.shape
    tok = batch * seq // n_tx
    d_model, ff, width, blk = d_loc * n_tx, w_up.shape[1], b_qkv.shape[1] // 3, 256
    any_spec, vmem = pl.BlockSpec(memory_space=pl.ANY), pl.BlockSpec(memory_space=pltpu.VMEM)
    arr = lambda *shape: jax.ShapeDtypeStruct(shape, BF16)
    buf = lambda *shape: pltpu.VMEM(shape, BF16)
    slots = 3 * 3 * n_tx + 2 * 4 * n_tx + n_tx
    split = lambda a: a.reshape(n_tx, n_ty, tok // n_ty, d_loc)
    return pl.pallas_call(
        functools.partial(front_kernel, n_tx=n_tx, n_ty=n_ty, blk=blk),
        in_specs=[any_spec] * 6 + [vmem] * 2,
        out_specs=[any_spec] * 5 + [vmem] + [any_spec] * 7 + [vmem],
        out_shape=[
            arr(tok, d_model), arr(tok, d_model), arr(d_model, ff), arr(d_model, ff), arr(d_model, 4 * width), arr(vecs.shape[0], d_model),
            arr(tok, d_model), arr(tok, 3 * width), arr(tok, ff), arr(tok, ff), arr(tok, width), arr(n_tx, ff, d_loc), arr(n_tx, d_loc, ff),
            jax.ShapeDtypeStruct((8, ff), F32),
        ],
        scratch_shapes=[
            buf(tok, d_model), buf(tok, d_model), buf(d_model, ff), buf(d_model, ff), buf(d_model, 4 * width),
            buf(tok, d_model), buf(tok, d_model), buf(tok, ff), pltpu.VMEM((tok, ff), F32), buf(tok, 3 * width), buf(tok, ff), buf(tok, width),
            buf(n_tx, ff, d_loc),
            buf(n_tx, d_loc, ff),
            pltpu.SemaphoreType.DMA((slots,)),
            pltpu.SemaphoreType.DMA((slots,)),
            pltpu.SemaphoreType.DMA((4 + 2 * n_ty,)),
            pltpu.SemaphoreType.DMA((12,)),
        ],
        compiler_params=pltpu.CompilerParams(collective_id=0, has_side_effects=True, vmem_limit_bytes=67_000_000),
        cost_estimate=pl.CostEstimate(flops=60_000_000_000, bytes_accessed=60_000_000, transcendentals=0),
        name="layer_front",
    )(split(x_act), split(cot_out), w_up, w_dt, w_a, vecs, b_qkv, b_up)


def tail_kernel(
    qkv, d_ctx, u, d_pre, h1, x, cot, w_d, w_a, w_u, p_down, p_up, vecs, small, cos_tab, sin_tab, turn_tab,
    y_out, dx_out, small_out, d_down, d_up, d_a,
    qkv_b, dctx_b, u_b, dpre_b, h1_b, x_b, cot_b, q_s, k_s, dq_s, ctx_s, dqkv_s, acc, dbq, ln_acc, arr_down, arr_up, arr_a, own_down, own_up,
    part, rc, sy, ry, x_own, c_own, sm_buf, send_sems, recv_sems, local_sems, rs_sems, *, n_tx, blk,
):
    g, z, t, core, y, t_core, t_y, t_diag = neighbours()
    core_dev, y_dev = (g, z, t_core), (g, z, t_y)
    z_dev = [(g, (z + k) % n_tx, t) for k in range(n_tx)]
    n_seq, seq, d_model = x.shape
    end = n_tx - 1
    width = d_ctx.shape[-1]
    d_loc = d_model // n_tx
    heads, steps = width // HEAD, seq // blk
    sub = seq // 4
    links = Links(send_sems, recv_sems)
    outs = (y_out, dx_out)
    late = ((u, u_b), (d_pre, dpre_b), (h1, h1_b), (x, x_b), (cot, cot_b))

    def load_early(s):
        slot = s % 2
        return [
            pltpu.make_async_copy(qkv.at[s], qkv_b.at[slot], local_sems.at[slot]),
            pltpu.make_async_copy(d_ctx.at[s], dctx_b.at[slot], local_sems.at[2 + slot]),
        ]

    def load_late(s):
        return [pltpu.make_async_copy(src.at[s], dst, local_sems.at[4 + i]) for i, (src, dst) in enumerate(late)]

    for copy in load_early(0):
        copy.start()
    acc[...] = jnp.zeros_like(acc)
    dbq[...] = jnp.zeros_like(dbq)
    ln_acc[...] = jnp.zeros_like(ln_acc)
    enter([core_dev, y_dev] + z_dev[1:])

    def cols(s):
        return block(s, d_loc)

    def rows(c):
        return block(c, sub)

    core_slot = [[links.slot(n_seq) for _ in BOTH] for _ in BOTH]
    y_slot = [links.slot(n_seq) for _ in BOTH]
    z_slot = [[links.slot(n_seq) for _ in range(n_tx)] for _ in BOTH]
    ag_y = [[links.slot(n_seq) for _ in range(n_tx)] for _ in BOTH]
    ag_c = [[[links.slot(n_seq) for _ in BOTH] for _ in range(n_tx)] for _ in BOTH]
    sm_slot = [links.slot() for _ in range(8)]

    arrivals, owners, results = (arr_down, arr_up, arr_a), ((p_down, own_down), (p_up, own_up)), (d_down, d_up, d_a)
    rs_slot = [[links.slot() for _ in range(5)] for _ in arrivals]
    right, left = (g, z + 1, t), (g, z - 1, t)
    first, last_z = z == 0, z == end
    middle = (z > 0) & (z < end)
    lower = z < n_tx // 2
    R0, L0, R1, L1, FAR = range(5)

    def rs_load(w, slot, d):
        return pltpu.make_async_copy(owners[w][0].at[d], owners[w][1].at[slot], rs_sems.at[w, slot])

    def rs_send(w, name, dev, cond, src=None):
        place = arrivals[w].at[name]
        links.send(rs_slot[w][name], place if src is None else src, place, dev, cond)

    def rs_add(w, name, slot, d, move_from, cond):
        place = arrivals[w].at[move_from]

        @pl.when(cond)
        def _():
            links.arrive(rs_slot[w][move_from], place, right)
            size = place.shape[0] // 4

            def body(r):
                at = block(r, size)
                mine = acc[pl.ds(pl.multiple_of(d * d_loc + r * size, size), size), :] if w >= len(owners) else owners[w][1][slot, at, :].astype(F32)
                arrivals[w][move_from, at, :] = (arrivals[w][move_from, at, :].astype(F32) + mine).astype(BF16)
            loop(4, body)

    def rs_start(w):
        for way, near, cond, to in ((1, (R0, R1, FAR), first, right), (-1, (L0, L1, FAR), last_z, left)):
            for hop in (2, 1, 0):
                d, name = z + way * (hop + 1), near[hop]
                if w >= len(owners):
                    @pl.when(cond)
                    def _():
                        arrivals[w][name] = acc[cols(d), :].astype(BF16)
                    rs_send(w, name, to, cond)
                else:
                    rs_send(w, name, to, cond, owners[w][0].at[d])

    def rs_far(w):
        if w < len(owners):
            rs_load(w, 0, 0).wait()
        rs_add(w, R1, 0, (end) * (2 - z), FAR, middle)
        links.send(rs_slot[w][R1], arrivals[w].at[FAR], arrivals[w].at[R1], right, middle & lower)
        links.send(rs_slot[w][L1], arrivals[w].at[FAR], arrivals[w].at[L1], left, middle & (~lower))
        if w < len(owners):
            rs_load(w, 0, (z + end) % n_tx).start()

    def rs_near(w):
        for slot, name, source, to, d in ((1, R0, R1, right, z + 1), (0, L0, L1, left, z - 1)):
            if w < len(owners):
                rs_load(w, slot, 0).wait()
            rs_add(w, name, slot, d, source, middle)
            links.send(rs_slot[w][name], arrivals[w].at[source], arrivals[w].at[name], to, middle)
            if w < len(owners) and slot:
                rs_load(w, slot, z).start()

    def rs_end(w):
        if w < len(owners):
            rs_load(w, 1, 0).wait()
            results[w][...] = owners[w][1][1].astype(F32)
        else:
            results[w][...] = acc[cols(z), :]
        for name, cond in ((R0, z > 0), (L0, z < end)):
            @pl.when(cond)
            def _():
                links.arrive(rs_slot[w][name], arrivals[w].at[name], right)
                results[w][...] += arrivals[w][name].astype(F32)

    for w in BOTH:
        rs_load(w, 0, (end) * (1 - z // 2)).start()
        rs_load(w, 1, (z + 1) % n_tx).start()

    gain1, gain2, bias = [vecs[i:i + 1, :] for i in range(3)]
    turn = turn_tab[...]

    def rotate(v, sign):
        return (v.astype(F32) * cos_tab[...] + sign * (dot_nn(v, turn) * sin_tab[...])).astype(BF16)

    def attend(s):
        slot = s % 2
        q_s[...] = rotate(qkv_b[slot, :, 0:width], 1.0) * BF16(HEAD ** -0.5)
        k_s[...] = rotate(qkv_b[slot, :, width:2 * width], 1.0)
        row = lax.broadcasted_iota(jnp.int32, (blk, blk), 0)
        col = lax.broadcasted_iota(jnp.int32, (blk, blk), 1)
        causal = row >= col
        dk_heads, dv_heads = [], []
        for h in range(heads):
            hs = slice(h * HEAD, (h + 1) * HEAD)
            k_h = k_s[:, hs]
            v_h = qkv_b[slot, :, 2 * width + h * HEAD:2 * width + (h + 1) * HEAD]
            dk = [None] * steps
            dv = [None] * steps
            for i in range(steps):
                at = slice(i * blk, (i + 1) * blk)
                n = (i + 1) * blk
                q_i = q_s[at, hs]
                do_i = dctx_b[slot, at, hs]
                sc = dot_nt(q_i, k_h[:n])
                s_diag = jnp.where(causal, sc[:, n - blk:], -1e30)
                sc = s_diag if i == 0 else jnp.concatenate([sc[:, :n - blk], s_diag], axis=1)
                p = jnp.exp(sc - jnp.max(sc, axis=-1, keepdims=True))
                p = p * (1.0 / row_sum(p))
                p_b = p.astype(BF16)
                ctx_s[at, hs] = dot_nn(p_b, v_h[:n]).astype(BF16)
                dp = dot_nt(do_i, v_h[:n]).astype(BF16).astype(F32)
                ds = (p * (dp - row_sum(p * dp))).astype(BF16)
                dq_s[at, hs] = (dot_nn(ds, k_h[:n]) * HEAD ** -0.5).astype(BF16)
                dk_i = dot_tn(ds, q_i)
                dv_i = dot_tn(p_b, do_i)
                for j in range(i + 1):
                    part_k, part_v = dk_i[j * blk:(j + 1) * blk], dv_i[j * blk:(j + 1) * blk]
                    dk[j] = part_k if dk[j] is None else dk[j] + part_k
                    dv[j] = part_v if dv[j] is None else dv[j] + part_v
            dk_heads.append(jnp.concatenate(dk, axis=0).astype(BF16))
            dv_heads.append(jnp.concatenate(dv, axis=0).astype(BF16))
        pieces = (rotate(dq_s[...], -1.0), rotate(jnp.concatenate(dk_heads, axis=1), -1.0), jnp.concatenate(dv_heads, axis=1))
        for pos, piece in enumerate(pieces):
            at = slice(pos * width, (pos + 1) * width)
            dqkv_s[:, at] = piece
            dbq[:, at] += fold(piece.astype(F32))

    def forward_part(s):
        def body(r):
            at = block(r, blk)
            total = dot_nt(u_b[at, :], w_d[...]) + dot_nt(ctx_s[at, :], w_a[:, 3 * width:])
            part[0, s % 2, at, :] = total.astype(BF16)
        loop(steps, body)

    def backward_part(s):
        def body(r):
            at = block(r, blk)
            d_h1 = dot_nt(dqkv_s[at, :], w_a[:, :3 * width]).astype(BF16).astype(F32)
            d_h2 = dot_nt(dpre_b[at, :], w_u[...]).astype(BF16).astype(F32)
            xf = x_b[at, :].astype(F32)
            xh, _ = normalise(xf)
            part[1, s % 2, at, :] = (d_h1 * gain1 + d_h2 * gain2).astype(BF16)
            for i, v in enumerate((d_h1 * xh, d_h1, d_h2 * xh, d_h2)):
                ln_acc[i] += fold(v)
        loop(steps, body)

    def weight_part():
        def body(r):
            at = block(r, d_loc)
            acc[at, :3 * width] += dot_tn(h1_b[:, at], dqkv_s[...])
            acc[at, 3 * width:] += dot_tn(cot_b[:, at], ctx_s[...])
        loop(n_tx, body)

    def share(a, s):
        for j, yy in enumerate((1 - y, y)):
            links.send(core_slot[a][j] + s, part.at[a, s % 2, rows(yy * 2 + 1 - core)], rc.at[a, s, yy], core_dev)

    step = 32

    def give(s):
        for a in BOTH:
            links.arrive(core_slot[a][0] + s, rc.at[a, s, 1 - y], core_dev)

            def body(r):
                at = block(r, step)
                mine = part[a, s % 2, pl.ds(pl.multiple_of(t_y * sub + r * step, step), step), :]
                sy[a, s, at, :] = (mine.astype(F32) + rc[a, s, 1 - y, at, :].astype(F32)).astype(BF16)
            loop(sub // step, body)
            links.send(y_slot[a] + s, sy.at[a, s], ry.at[a, s], y_dev)

    def finish(s):
        for a in BOTH:
            links.arrive(core_slot[a][1] + s, rc.at[a, s, y], core_dev)
            links.arrive(y_slot[a] + s, ry.at[a, s], y_dev)
            links.sent(y_slot[a] + s, sy.at[a, s])

            def body(r):
                at = block(r, step)
                whole = pl.ds(pl.multiple_of(t * sub + r * step, step), step)
                total = part[a, s % 2, whole, :].astype(F32) + rc[a, s, y, at, :].astype(F32) + ry[a, s, at, :].astype(F32)
                xf = x_own[s % 2, at, :].astype(F32)
                if a == 0:
                    out = xf + total + bias
                else:
                    xh, inv = normalise(xf)
                    out = c_own[s % 2, at, :].astype(F32) + inv * (total - row_mean(total) - xh * row_mean(total * xh))
                sy[a, s, at, :] = out.astype(BF16)
            loop(sub // step, body)
            place = outs[a].at[z * n_seq + s, rows(t)]
            for k in OTHERS:
                links.send(z_slot[a][k] + s, sy.at[a, s, :, cols((z + k) % n_tx)], place, z_dev[k])
            mine = sy.at[a, s, :, cols(z)]
            pltpu.make_async_copy(mine, place, local_sems.at[9 + a * n_seq + s]).start()
            links.send(ag_y[a][0] + s, mine, place, y_dev)
            links.send(ag_c[a][0][0] + s, mine, place, core_dev)

    def src(k):
        return (z + n_tx - k) % n_tx

    def forward(s):
        for a in BOTH:
            for k in OTHERS:
                place = outs[a].at[src(k) * n_seq + s, rows(t)]
                links.arrive(z_slot[a][k] + s, place, y_dev)
                links.send(ag_y[a][k] + s, place, place, y_dev)
                links.send(ag_c[a][k][0] + s, place, place, core_dev)

    def forward_y(s):
        for a in BOTH:
            for k in (0, *OTHERS):
                place = outs[a].at[src(k) * n_seq + s, rows(t_y)]
                links.arrive(ag_y[a][k] + s, place, y_dev)
                links.send(ag_c[a][k][1] + s, place, place, core_dev)

    def core_done(s):
        for a in BOTH:
            for j in BOTH:
                links.sent(core_slot[a][j] + s, sy.at[a, s])

    def settle(s):
        for a in BOTH:
            for k in range(n_tx):
                piece = outs[a].at[src(k) * n_seq + s, rows(t)]
                for j, who in enumerate((t_core, t_diag)):
                    links.arrive(ag_c[a][k][j] + s, outs[a].at[src(k) * n_seq + s, rows(who)], core_dev)
                    links.sent(ag_c[a][k][j] + s, piece)
                links.sent(ag_y[a][k] + s, piece)
                if k:
                    links.sent(z_slot[a][k] + s, piece)
            pltpu.make_async_copy(sy.at[a, s, :, cols(z)], outs[a].at[z * n_seq + s, rows(t)], local_sems.at[9 + a * n_seq + s]).wait()

    def one(s):
        for copy in load_early(s):
            copy.wait()

        @pl.when(s < n_seq - 1)
        def _():
            for copy in load_early(s + 1):
                copy.start()

        for copy in load_late(s):
            copy.start()
        attend(s)
        pl.when(s == 0)(lambda: rs_far(0))
        pl.when(s == 2)(lambda: rs_far(1))
        for copy in load_late(s):
            copy.wait()

        @pl.when(s == 2)
        def _():
            core_done(0)

        x_own[s % 2] = x_b[rows(t), :]
        c_own[s % 2] = cot_b[rows(t), :]
        forward_part(s)
        share(0, s)
        backward_part(s)
        share(1, s)
        weight_part()
        give(s)

        @pl.when(s == 0)
        def _():
            rs_start(1)
            rs_near(0)

        @pl.when(s > 0)
        def _():
            finish(s - 1)

        pl.when(s == 1)(lambda: rs_end(0))

    rs_start(0)
    loop(n_seq, one)
    rs_start(2)
    forward(0)
    rs_near(1)
    last = n_seq - 1
    MINE, CORE, PAIR, FROM_Y, QUAD = range(5)
    sm_buf[MINE] = small[...]
    for i in range(4):
        sm_buf[MINE, i:i + 1, :] = jnp.sum(ln_acc[i], axis=0, keepdims=True)
    sm_buf[MINE, 5:6, :3 * width] = jnp.sum(dbq[...], axis=0, keepdims=True)
    links.send(sm_slot[0], sm_buf.at[MINE], sm_buf.at[CORE], core_dev)
    over_ty = (lax.broadcasted_iota(jnp.int32, small.shape, 0) < 4).astype(F32)
    finish(last)
    links.arrive(sm_slot[0], sm_buf.at[CORE], core_dev)
    sm_buf[PAIR] = sm_buf[MINE] + over_ty * sm_buf[CORE]
    links.send(sm_slot[PAIR], sm_buf.at[PAIR], sm_buf.at[FROM_Y], y_dev)
    forward(1)
    forward_y(0)
    links.arrive(sm_slot[PAIR], sm_buf.at[FROM_Y], y_dev)
    sm_buf[QUAD] = sm_buf[PAIR] + over_ty * sm_buf[FROM_Y]
    for k in OTHERS:
        links.send(sm_slot[QUAD + k], sm_buf.at[QUAD], sm_buf.at[QUAD + k], z_dev[k])
    rs_far(2)
    rs_end(1)
    forward(last)
    forward_y(1)
    rs_near(2)
    forward_y(last)
    rs_end(2)
    for k in OTHERS:
        links.arrive(sm_slot[QUAD + k], sm_buf.at[QUAD + k], y_dev)
    small_out[...] = jnp.sum(sm_buf[QUAD:], axis=0)
    for s in range(n_seq):
        settle(s)
        if s:
            core_done(s)
    for w, slots in enumerate(rs_slot):
        for name, cond in ((R0, z < end), (L0, z > 0), (R1, lower), (L1, ~lower), (FAR, first | last_z)):
            links.sent(slots[name], arrivals[w].at[name], cond)
    for i in (MINE, PAIR, *[QUAD + k for k in OTHERS]):
        links.sent(sm_slot[i], sm_buf.at[MINE])


def layer_tail(qkv, d_ctx, u, d_pre, h1, x, cot, w_d, w_a, w_u, p_down, p_up, vecs, small, n_tx, n_ty):
    n_seq, seq, d_model = x.shape
    end = n_tx - 1
    width, d_loc, blk, sub = d_ctx.shape[-1], d_model // n_tx, 256, seq // n_ty
    any_spec, vmem = pl.BlockSpec(memory_space=pl.ANY), pl.BlockSpec(memory_space=pltpu.VMEM)
    out = jax.ShapeDtypeStruct((n_seq * n_tx, seq, d_loc), BF16)
    cos_tab, sin_tab = rope_tables(seq, width)
    shapes = (p_down.shape[1:], p_up.shape[1:], (d_loc, d_model))
    slots = n_seq * 2 * (3 + 4 * n_tx) + 5 * 5
    wide = lambda *lead: pltpu.VMEM(lead + (seq, d_model), BF16)
    piece = lambda *lead: pltpu.VMEM(lead + (sub, d_model), BF16)
    return pl.pallas_call(
        functools.partial(tail_kernel, n_tx=n_tx, blk=blk),
        in_specs=[any_spec] * 7 + [vmem] * 3 + [any_spec] * 2 + [vmem] * 5,
        out_specs=[any_spec] * 2 + [vmem] * 4,
        out_shape=[out, out, *[jax.ShapeDtypeStruct(shape, F32) for shape in (small.shape, *shapes)]],
        scratch_shapes=[
            pltpu.VMEM((2, seq, 3 * width), BF16),
            pltpu.VMEM((2, seq, width), BF16),
            wide(), wide(), wide(), wide(), wide(),
            pltpu.VMEM((seq, width), BF16),
            pltpu.VMEM((seq, width), BF16),
            pltpu.VMEM((seq, width), BF16),
            pltpu.VMEM((seq, width), BF16),
            pltpu.VMEM((seq, 3 * width), BF16),
            pltpu.VMEM((d_model, d_model), F32),
            pltpu.VMEM((8, 3 * width), F32),
            pltpu.VMEM((4, 8, d_model), F32),
            *[pltpu.VMEM((n,) + shape, BF16) for n, shape in zip((5, 5, 5, 2, 2), shapes + shapes)],
            wide(2, 2),
            piece(2, n_seq, 2),
            piece(2, n_seq),
            piece(2, n_seq),
            piece(2),
            piece(2),
            pltpu.VMEM((8, 8, d_model), F32),
            pltpu.SemaphoreType.DMA((slots,)),
            pltpu.SemaphoreType.DMA((slots,)),
            pltpu.SemaphoreType.DMA((9 + 2 * n_seq,)),
            pltpu.SemaphoreType.DMA((2, 2)),
        ],
        compiler_params=pltpu.CompilerParams(collective_id=1, has_side_effects=True, vmem_limit_bytes=67_000_000),
        cost_estimate=pl.CostEstimate(flops=60_000_000_000, bytes_accessed=60_000_000, transcendentals=0),
        name="layer_tail",
    )(qkv, d_ctx, u, d_pre, h1, x, cot, w_d, w_a, w_u, p_down, p_up, vecs, small, cos_tab, sin_tab, rope_turn(width))


def solution(mesh):
    n_tx, n_ty = mesh.shape['tx'], mesh.shape['ty']
    act_spec = P('dp', None, 'tx')
    width_spec = P('tx')
    in_specs = (act_spec, act_spec, width_spec, width_spec, width_spec, width_spec, P('tx', 'ty', None), P('ty', None), P('ty', 'tx'), width_spec, P('tx', 'ty'), P('ty'), P('ty', 'tx'), width_spec)
    width_out = P(('dp', 'tx'))
    out_specs = (act_spec, act_spec, width_out, width_out, width_out, width_out, P(('dp', 'tx'), 'ty', None), P(('dp', 'ty'), None), P(('dp', 'ty'), 'tx'), width_out, P(('dp', 'tx'), 'ty'), P(('dp', 'ty')), P(('dp', 'ty'), 'tx'), width_out)
    def body(x_act, cot_out, ln1_gain, ln1_bias, ln2_gain, ln2_bias, w_qkv, b_qkv, w_dense, b_dense, w_up, b_up, w_down, b_down):
        batch, seq, d_loc = x_act.shape
        d_model = d_loc * n_tx
        heads = w_qkv.shape[1]
        hw = heads * HEAD
        n_b = batch // n_tx
        tok = n_b * seq
        z, g = lax.axis_index('tx'), lax.axis_index('dp')

        wq_loc = w_qkv.reshape(d_loc, heads, 3, HEAD).transpose(0, 2, 1, 3).reshape(d_loc, 3 * hw)
        vec_loc = jnp.stack([ln1_gain, ln1_bias, ln2_gain, ln2_bias, b_dense, b_down], axis=0)
        vec_loc = jnp.pad(vec_loc, ((0, 10), (0, 0)))
        bq = b_qkv.astype(F32).reshape(heads, 3, HEAD).transpose(1, 0, 2).reshape(1, 3 * hw)
        x, cot, w_u, w_dt, w_a, vecs, h1, qkv, u, d_pre, d_ctx, part_down, part_up, d_bup = layer_front(
            x_act, cot_out, w_up, w_down.T, jnp.concatenate([wq_loc, w_dense.T], axis=1), vec_loc, bq, b_up.astype(F32)[None], n_tx, n_ty)
        g1, g2, b_o, b_d = [vecs[i].astype(F32) for i in (0, 2, 4, 5)]

        d_b_up = d_bup.sum(0)
        small = jnp.pad(d_b_up[None], ((4, 3), (0, d_model - d_b_up.shape[0])))
        rows = jnp.pad(jnp.stack([g1, g2, b_o + b_d], axis=0), ((0, 5), (0, 0)))
        by_seq = lambda a: a.reshape(n_b, seq, a.shape[-1])
        y_out, dx_act, total, d_w_down, d_w_up, d_w_a = layer_tail(by_seq(qkv), by_seq(d_ctx), by_seq(u), by_seq(d_pre), by_seq(h1), by_seq(x), by_seq(cot), w_dt, w_a, w_u, part_down, part_up, rows, small, n_tx, n_ty)
        d_w_qkv = d_w_a[:, :3 * hw].reshape(d_loc, 3, heads, HEAD).transpose(0, 2, 1, 3).reshape(d_loc, heads, 3 * HEAD)
        d_w_dense = d_w_a[:, 3 * hw:].T
        ln_sum = lax.dynamic_slice(total, (0, z * d_loc), (4, d_loc))
        d_b_up, d_b_qkv = total[4, :d_b_up.shape[0]], total[5, :3 * hw].reshape(3, heads, HEAD).transpose(1, 0, 2).reshape(heads, 3 * HEAD)
        d_b_out = cot_out.astype(F32).sum((0, 1))
        return (y_out, dx_act, *ln_sum, d_w_qkv, d_b_qkv, d_w_dense, d_b_out, d_w_up, d_b_up, d_w_down, d_b_out)

    return jax.shard_map(body, mesh=mesh, in_specs=in_specs, out_specs=out_specs, check_vma=False)
```

```python
import functools
import jax
import jax.numpy as jnp
import numpy as np
from jax import lax
from jax.experimental import pallas as pl
from jax.experimental.pallas import tpu as pltpu
from jax.sharding import PartitionSpec as P

LN_EPS = 1e-5
ROPE_BASE = 10000.0
HEAD = 64
ROT = 16
F32 = jnp.float32
BF16 = jnp.bfloat16

def rope_tables(seq_len, width):
    inv_freq = (ROPE_BASE ** (-np.arange(0, ROT, 2, dtype=np.float32) / ROT)).astype(np.float32)
    angles = np.arange(seq_len, dtype=np.float32)[:, None] * inv_freq[None]
    angles = np.concatenate([angles, angles, np.zeros((seq_len, HEAD - ROT), np.float32)], axis=1)
    angles = np.tile(angles, (1, width // HEAD)).astype(np.float64)
    return np.cos(angles).astype(np.float32), np.sin(angles).astype(np.float32)


def rope_turn(width):
    turn = np.zeros((width, width), np.float32)
    for lane in range(width):
        place = lane % HEAD
        if place < ROT:
            lower = place < ROT // 2
            turn[lane + ROT // 2 if lower else lane - ROT // 2, lane] = -1.0 if lower else 1.0
    return turn.astype(BF16)


def dot_nn(a, b):
    return lax.dot_general(a, b, (((1,), (0,)), ((), ())), preferred_element_type=F32)


def dot_nt(a, b):
    return lax.dot_general(a, b, (((1,), (1,)), ((), ())), preferred_element_type=F32)


def dot_tn(a, b):
    return lax.dot_general(a, b, (((0,), (0,)), ((), ())), preferred_element_type=F32)


MESH = pl.DeviceIdType.MESH
BOTH = range(2)
OTHERS = (1, 3, 2)


def block(i, size):
    return pl.ds(pl.multiple_of(i * size, size), size)


def row_mean(v):
    return jnp.mean(v, axis=-1, keepdims=True)


def normalise(v):
    mean = row_mean(v)
    inv_std = lax.rsqrt(row_mean(v * v) - mean * mean + LN_EPS)
    return (v - mean) * inv_std, inv_std


def row_sum(v):
    return jnp.sum(v, axis=-1, keepdims=True)


def loop(count, body):
    lax.fori_loop(0, count, lambda i, carry: (body(i), carry)[1], 0)


def fold(v):
    return v.reshape(v.shape[0] // 8, 8, v.shape[1]).sum(0)


class Links:
    def __init__(self, send_sems, recv_sems):
        self.send_sems, self.recv_sems, self.count = send_sems, recv_sems, 0

    def slot(self, count=1):
        self.count += count
        return self.count - count

    def make(self, slot, src, dst, dev):
        return pltpu.make_async_remote_copy(src_ref=src, dst_ref=dst, send_sem=self.send_sems.at[slot], recv_sem=self.recv_sems.at[slot], device_id=dev, device_id_type=MESH)

    def send(self, slot, src, dst, dev, cond=None):
        def go():
            self.make(slot, src, dst, dev).start()
        go() if cond is None else pl.when(cond)(go)

    def arrive(self, slot, dst, dev, cond=None):
        def go():
            self.make(slot, dst, dst, dev).wait_recv()
        go() if cond is None else pl.when(cond)(go)

    def sent(self, slot, like, cond=None):
        def go():
            self.make(slot, like, like, (0, 0, 0)).wait_send()
        go() if cond is None else pl.when(cond)(go)


def neighbours():
    g, z, t = lax.axis_index('dp'), lax.axis_index('tx'), lax.axis_index('ty')
    core, y = t % 2, t // 2
    t_core, t_y, t_diag = y * 2 + 1 - core, (1 - y) * 2 + core, (1 - y) * 2 + 1 - core
    return g, z, t, core, y, t_core, t_y, t_diag


def enter(devices):
    barrier = pltpu.get_barrier_semaphore()
    for dev in devices:
        pl.semaphore_signal(barrier, inc=1, device_id=dev, device_id_type=MESH)
    pl.semaphore_wait(barrier, len(devices))


def front_kernel(
    x_in, c_in, wu_in, wd_in, wa_in, v0, v1, v2, v3, v4, v5, b_qkv, b_up,
    x_out, c_out, wu_out, wd_out, wa_out, v_out, h1_out, qkv_out, u_out, dpre_out, dctx_out, dwd_out, dwu_out, sums_out,
    v_in, x_v, c_v, wu_v, wd_v, wa_v, h1_v, h2_v, u_v, gp_v, qkv_v, dpre_v, dctx_v, dwd_v, dwu_v,
    send_sems, recv_sems, local_sems, out_sems, *, n_tx, n_ty, blk,
):
    g, z, t, core, y, t_core, t_y, t_diag = neighbours()
    core_dev, y_dev, x_dev = (g, z, t_core), (g, z, t_y), (1 - g, z, t)
    z_dev = [(g, (z + k) % n_tx, t) for k in range(n_tx)]
    left, right = (g, z - 1, t), (g, z + 1, t)
    end = n_tx - 1
    d_loc = x_in.shape[-1]
    half = d_loc // 2
    tok = x_v.shape[0]
    chunk = tok // n_ty
    width = dctx_v.shape[-1]
    links = Links(send_sems, recv_sems)

    def cols(s):
        return block(s, d_loc)

    def rows(c):
        return block(c, chunk)

    def w_rows(s, group):
        return pl.ds(pl.multiple_of(s * d_loc + group * half, half), half)

    v_in[...] = jnp.zeros_like(v_in)
    for i, v in enumerate((v0, v1, v2, v3, v4, v5)):
        v_in[i:i + 1, :] = v[...].astype(F32).reshape(1, d_loc)
    v_out[:, cols(z)] = v_in[...]
    own = []
    for i, (src, dst) in enumerate(((wu_in, wu_v.at[cols(z), :]), (wd_in, wd_v.at[:, cols(z)]), (wa_in, wa_v.at[cols(z), :]))):
        own.append(pltpu.make_async_copy(src, dst, local_sems.at[1 + i]))
    for i, (src, dst) in enumerate(((x_in, x_v), (c_in, c_v))):
        for c in range(n_ty):
            own.append(pltpu.make_async_copy(src.at[z, c], dst.at[pl.ds(c * chunk, chunk), cols(z)], local_sems.at[4 + i * n_ty + c]))
    for copy in own:
        copy.start()
    enter([core_dev, y_dev, x_dev] + z_dev[1:])

    mine = block(g, half)
    weights = (
        (wu_in.at[mine, :], lambda s, group: wu_v.at[w_rows(s, group), :]),
        (wd_in.at[:, mine], lambda s, group: wd_v.at[:, w_rows(s, group)]),
        (wa_in.at[mine, :], lambda s, group: wa_v.at[w_rows(s, group), :]),
    )
    UP, DOWN, ATTN = range(len(weights))
    w_slot = [[links.slot() for _ in range(2 * n_tx)] for _ in weights]
    x_slot = [[links.slot() for _ in range(n_tx)] for _ in weights]

    def w_send(w, hops):
        own_half, place = weights[w]
        for slot, s, to, ok in ((hops, z - hops, right, (z >= hops) & (z < end)), (n_tx + hops, z + hops, left, (z + hops < n_tx) & (z > 0))):
            links.send(w_slot[w][slot + 1], place(s, g) if hops else own_half, place(s, g), to, ok)

    def w_sides(hops):
        return (hops, hops, z - hops, z >= hops), (n_tx + hops, n_tx - hops, z + hops, z + hops < n_tx)

    def w_pass(w, hops):
        for slot, x_at, s, ok in w_sides(hops):
            place = weights[w][1](s, g)
            links.arrive(w_slot[w][slot], place, right, ok)
            links.send(x_slot[w][x_at], place, place, x_dev, ok)
        if hops < end:
            w_send(w, hops)

    def w_finish(w):
        for hops in range(1, n_tx):
            for slot, x_at, s, ok in w_sides(hops):
                links.arrive(x_slot[w][x_at], weights[w][1](s, 1 - g), x_dev, ok)

    arrays = ((x_in, x_v), (c_in, c_v))
    z_slot = [[links.slot() for _ in range(n_tx)] for _ in arrays]
    y_slot = [[links.slot() for _ in range(n_tx)] for _ in arrays]
    c_slot = [[[links.slot() for _ in BOTH] for _ in range(n_tx)] for _ in arrays]
    v_slot = [links.slot() for _ in range(n_tx)]

    def src_cols(k):
        return cols((z + n_tx - k) % n_tx)

    def t_send(a, *which):
        for k in which:
            links.send(z_slot[a][k], arrays[a][0].at[(z + k) % n_tx, t], arrays[a][1].at[rows(t), cols(z)], z_dev[k])

    def t_pass(a, k):
        place = arrays[a][1].at[rows(t), src_cols(k)]
        links.arrive(z_slot[a][k], place, y_dev)
        links.send(y_slot[a][k], place, place, y_dev)
        links.send(c_slot[a][k][0], place, place, core_dev)

    def t_pass_y(a, k):
        place = arrays[a][1].at[rows(t_y), src_cols(k)]
        links.arrive(y_slot[a][k], place, y_dev)
        links.send(c_slot[a][k][1], place, place, core_dev)

    def t_finish(a):
        for k in OTHERS:
            for j, c in enumerate((t_core, t_diag)):
                links.arrive(c_slot[a][k][j], arrays[a][1].at[rows(c), src_cols(k)], core_dev)

    X, COT = BOTH
    w_send(UP, 0)
    for k in OTHERS:
        links.send(v_slot[k], v_in, v_out.at[:, cols(z)], z_dev[k])
    t_send(X, *OTHERS)
    w_pass(UP, 1)
    for k in OTHERS:
        t_pass(X, k)
    w_pass(UP, 2)
    w_send(DOWN, 0)
    t_send(COT, 2)
    for k in OTHERS:
        t_pass_y(X, k)
    w_pass(UP, 3)
    w_finish(UP)
    t_finish(X)
    for k in OTHERS:
        links.arrive(v_slot[k], v_out.at[:, src_cols(k)], y_dev)
    for copy in own:
        copy.wait()

    outputs = []

    def write(src, dst):
        copy = pltpu.make_async_copy(src, dst, out_sems.at[len(outputs)])
        copy.start()
        outputs.append(copy)

    write(x_v, x_out)
    write(wu_v, wu_out)

    def early():
        w_pass(DOWN, 1)
        t_send(COT, 1)
        w_send(ATTN, 0)
        t_send(COT, 3)

    vec = v_out[...]
    g1, be1, g2, be2 = [vec[i:i + 1] for i in range(4)]

    def forward(i):
        at = block(i, blk)
        xf = x_v[at, :].astype(F32)
        xh, _ = normalise(xf)
        h1 = (xh * g1 + be1).astype(BF16)
        h2 = (xh * g2 + be2).astype(BF16)
        h1_v[at, :] = h1
        h2_v[at, :] = h2
        pre = (dot_nn(h2, wu_v[...]) + b_up[...].astype(F32).reshape(1, -1)).astype(BF16).astype(F32)
        cdf = 0.5 * (1.0 + lax.erf(pre * (0.5 ** 0.5)))
        u_v[at, :] = (pre * cdf).astype(BF16)
        gp_v[at, :] = cdf + pre * (jnp.exp(-0.5 * pre * pre) * (1.0 / (2.0 * jnp.pi) ** 0.5))
        pl.when(i == 0)(early)
        pl.when(i == 4)(lambda: w_pass(DOWN, 2))

    loop(tok // blk, forward)
    write(h1_v, h1_out)
    write(u_v, u_out)
    t_pass(COT, 2)
    t_pass(COT, 1)
    w_pass(ATTN, 1)
    t_pass(COT, 3)
    w_pass(DOWN, 3)
    for k in (2, 1, 3):
        t_pass_y(COT, k)
    w_finish(DOWN)
    t_finish(COT)
    write(c_v, c_out)
    write(wd_v, wd_out)
    sums_out[...] = jnp.zeros_like(sums_out)

    def backward(i):
        at = block(i, blk)
        cot = c_v[at, :]
        d_gelu = dot_nt(cot, wd_v[...]).astype(BF16).astype(F32)
        d_pre = (d_gelu * gp_v[at, :]).astype(BF16)
        dpre_v[at, :] = d_pre
        sums_out[0] += fold(d_pre.astype(F32))
        sums_out[1] += fold(cot.astype(F32))
        pl.when(i == 4)(lambda: w_pass(ATTN, 2))

    loop(tok // blk, backward)
    write(dpre_v, dpre_out)

    def down(r):
        dwd_v[r] = dot_tn(u_v[...], c_v[:, cols(r)]).astype(BF16)

    def up(r):
        dwu_v[r] = dot_tn(h2_v[:, cols(r)], dpre_v[...]).astype(BF16)

    def attn(i):
        at = block(i, blk)
        qkv_v[at, :] = (dot_nn(h1_v[at, :], wa_v[:, :3 * width]) + b_qkv[...]).astype(BF16)
        dctx_v[at, :] = dot_nn(c_v[at, :], wa_v[:, 3 * width:]).astype(BF16)

    loop(n_tx, down)
    write(dwd_v, dwd_out)
    w_pass(ATTN, 3)
    loop(n_tx, up)
    write(dwu_v, dwu_out)
    w_finish(ATTN)
    write(wa_v, wa_out)
    loop(tok // blk, attn)
    write(qkv_v, qkv_out)
    write(dctx_v, dctx_out)
    piece = x_v.at[pl.ds(0, chunk), pl.ds(0, d_loc)]
    for a in BOTH:
        for k in OTHERS:
            for slot in (z_slot[a][k], y_slot[a][k], *c_slot[a][k]):
                links.sent(slot, piece)
    for w in range(len(weights)):
        shard = weights[w][0]
        for hops in range(n_tx):
            if hops:
                for _, x_at, _, ok in w_sides(hops):
                    links.sent(x_slot[w][x_at], shard, ok)
            if hops < end:
                links.sent(w_slot[w][hops + 1], shard, (z >= hops) & (z < end))
                links.sent(w_slot[w][n_tx + hops + 1], shard, (z + hops < n_tx) & (z > 0))
    for k in OTHERS:
        links.sent(v_slot[k], v_in)
    for copy in outputs:
        copy.wait()


def layer_front(x_act, cot_out, w_up, w_down, w_a, vecs, b_qkv, b_up, n_tx, n_ty):
    batch, seq, d_loc = x_act.shape
    tok = batch * seq // n_tx
    d_model, ff, width, blk = d_loc * n_tx, w_up.shape[1], b_qkv.shape[1] // 3, 256
    any_spec, vmem = pl.BlockSpec(memory_space=pl.ANY), pl.BlockSpec(memory_space=pltpu.VMEM)
    arr = lambda *shape: jax.ShapeDtypeStruct(shape, BF16)
    buf = lambda *shape: pltpu.VMEM(shape, BF16)
    slots = 3 * 3 * n_tx + 2 * 4 * n_tx + n_tx
    split = lambda a: a.reshape(n_tx, n_ty, tok // n_ty, d_loc)
    return pl.pallas_call(
        functools.partial(front_kernel, n_tx=n_tx, n_ty=n_ty, blk=blk),
        in_specs=[any_spec] * 5 + [vmem] * 8,
        out_specs=[any_spec] * 5 + [vmem] + [any_spec] * 7 + [vmem],
        out_shape=[
            arr(tok, d_model), arr(tok, d_model), arr(d_model, ff), arr(ff, d_model), arr(d_model, 4 * width), jax.ShapeDtypeStruct((8, d_model), F32),
            arr(tok, d_model), arr(tok, 3 * width), arr(tok, ff), arr(tok, ff), arr(tok, width), arr(n_tx, ff, d_loc), arr(n_tx, d_loc, ff),
            jax.ShapeDtypeStruct((2, 8, ff), F32),
        ],
        scratch_shapes=[
            pltpu.VMEM((8, d_loc), F32),
            buf(tok, d_model), buf(tok, d_model), buf(d_model, ff), buf(ff, d_model), buf(d_model, 4 * width),
            buf(tok, d_model), buf(tok, d_model), buf(tok, ff), pltpu.VMEM((tok, ff), F32), buf(tok, 3 * width), buf(tok, ff), buf(tok, width),
            buf(n_tx, ff, d_loc),
            buf(n_tx, d_loc, ff),
            pltpu.SemaphoreType.DMA((slots,)),
            pltpu.SemaphoreType.DMA((slots,)),
            pltpu.SemaphoreType.DMA((4 + 2 * n_ty,)),
            pltpu.SemaphoreType.DMA((12,)),
        ],
        compiler_params=pltpu.CompilerParams(collective_id=0, has_side_effects=True, vmem_limit_bytes=67_000_000),
        cost_estimate=pl.CostEstimate(flops=60_000_000_000, bytes_accessed=60_000_000, transcendentals=0),
        name="layer_front",
    )(split(x_act), split(cot_out), w_up, w_down, w_a, *vecs, b_qkv, b_up)


def tail_kernel(
    qkv, d_ctx, u, d_pre, h1, x, cot, w_d, w_a, w_u, p_down, p_up, vecs, sums, cos_tab, sin_tab, turn_tab,
    y_out, dx_out, small_out, d_down, d_up, d_a,
    qkv_b, dctx_b, u_b, dpre_b, h1_b, x_b, cot_b, q_s, k_s, dq_s, ctx_s, dqkv_s, acc, dbq, ln_acc, arr_down, arr_up, arr_a, own_down, own_up,
    part, rc, sy, ry, x_own, c_own, sm_buf, send_sems, recv_sems, local_sems, rs_sems, *, n_tx, blk,
):
    g, z, t, core, y, t_core, t_y, t_diag = neighbours()
    core_dev, y_dev = (g, z, t_core), (g, z, t_y)
    z_dev = [(g, (z + k) % n_tx, t) for k in range(n_tx)]
    n_seq, seq, d_model = x.shape
    end = n_tx - 1
    width = d_ctx.shape[-1]
    d_loc = d_model // n_tx
    heads, steps = width // HEAD, seq // blk
    sub = seq // 4
    links = Links(send_sems, recv_sems)
    outs = (y_out, dx_out)
    late = ((u, u_b), (d_pre, dpre_b), (h1, h1_b), (x, x_b), (cot, cot_b))

    def load_early(s):
        slot = s % 2
        return [
            pltpu.make_async_copy(qkv.at[s], qkv_b.at[slot], local_sems.at[slot]),
            pltpu.make_async_copy(d_ctx.at[s], dctx_b.at[slot], local_sems.at[2 + slot]),
        ]

    def load_late(s):
        return [pltpu.make_async_copy(src.at[s], dst, local_sems.at[4 + i]) for i, (src, dst) in enumerate(late)]

    for copy in load_early(0):
        copy.start()
    acc[...] = jnp.zeros_like(acc)
    dbq[...] = jnp.zeros_like(dbq)
    ln_acc[...] = jnp.zeros_like(ln_acc)
    enter([core_dev, y_dev] + z_dev[1:])

    def cols(s):
        return block(s, d_loc)

    def rows(c):
        return block(c, sub)

    core_slot = [[links.slot(n_seq) for _ in BOTH] for _ in BOTH]
    y_slot = [links.slot(n_seq) for _ in BOTH]
    z_slot = [[links.slot(n_seq) for _ in range(n_tx)] for _ in BOTH]
    ag_y = [[links.slot(n_seq) for _ in range(n_tx)] for _ in BOTH]
    ag_c = [[[links.slot(n_seq) for _ in BOTH] for _ in range(n_tx)] for _ in BOTH]
    sm_slot = [links.slot() for _ in range(8)]

    arrivals, owners, results = (arr_down, arr_up, arr_a), ((p_down, own_down), (p_up, own_up)), (d_down, d_up, d_a)
    rs_slot = [[links.slot() for _ in range(5)] for _ in arrivals]
    right, left = (g, z + 1, t), (g, z - 1, t)
    first, last_z = z == 0, z == end
    middle = (z > 0) & (z < end)
    lower = z < n_tx // 2
    R0, L0, R1, L1, FAR = range(5)

    def rs_load(w, slot, d):
        return pltpu.make_async_copy(owners[w][0].at[d], owners[w][1].at[slot], rs_sems.at[w, slot])

    def rs_send(w, name, dev, cond, src=None):
        place = arrivals[w].at[name]
        links.send(rs_slot[w][name], place if src is None else src, place, dev, cond)

    def rs_add(w, name, slot, d, move_from, cond):
        place = arrivals[w].at[move_from]

        @pl.when(cond)
        def _():
            links.arrive(rs_slot[w][move_from], place, right)
            size = place.shape[0] // 4

            def body(r):
                at = block(r, size)
                mine = acc[pl.ds(pl.multiple_of(d * d_loc + r * size, size), size), :] if w >= len(owners) else owners[w][1][slot, at, :].astype(F32)
                arrivals[w][move_from, at, :] = (arrivals[w][move_from, at, :].astype(F32) + mine).astype(BF16)
            loop(4, body)

    def rs_start(w, *hops):
        for way, near, cond, to in ((1, (R0, R1, FAR), first, right), (-1, (L0, L1, FAR), last_z, left)):
            for hop in hops:
                d, name = z + way * (hop + 1), near[hop]
                if w >= len(owners):
                    @pl.when(cond)
                    def _():
                        arrivals[w][name] = acc[cols(d), :].astype(BF16)
                    rs_send(w, name, to, cond)
                else:
                    rs_send(w, name, to, cond, owners[w][0].at[d])

    def rs_far(w):
        if w < len(owners):
            rs_load(w, 0, 0).wait()
        rs_add(w, R1, 0, (end) * (2 - z), FAR, middle)
        links.send(rs_slot[w][R1], arrivals[w].at[FAR], arrivals[w].at[R1], right, middle & lower)
        links.send(rs_slot[w][L1], arrivals[w].at[FAR], arrivals[w].at[L1], left, middle & (~lower))
        if w < len(owners):
            rs_load(w, 0, (z + end) % n_tx).start()

    def rs_near(w):
        for slot, name, source, to, d in ((1, R0, R1, right, z + 1), (0, L0, L1, left, z - 1)):
            if w < len(owners):
                rs_load(w, slot, 0).wait()
            rs_add(w, name, slot, d, source, middle)
            links.send(rs_slot[w][name], arrivals[w].at[source], arrivals[w].at[name], to, middle)
            if w < len(owners) and slot:
                rs_load(w, slot, z).start()

    def rs_end(w):
        if w < len(owners):
            rs_load(w, 1, 0).wait()
            results[w][...] = owners[w][1][1].astype(F32)
        else:
            results[w][...] = acc[cols(z), :]
        for name, cond in ((R0, z > 0), (L0, z < end)):
            @pl.when(cond)
            def _():
                links.arrive(rs_slot[w][name], arrivals[w].at[name], right)
                results[w][...] += arrivals[w][name].astype(F32)

    for w in BOTH:
        rs_load(w, 0, (end) * (1 - z // 2)).start()
        rs_load(w, 1, (z + 1) % n_tx).start()

    gain1, _, gain2, _, bias_o, bias_d = [vecs[i:i + 1, :] for i in range(6)]
    bias = bias_o + bias_d
    turn = turn_tab[...]

    def rotate(v, sign):
        cos, sin = [jnp.concatenate([tab[...]] * (heads // 2), axis=1) for tab in (cos_tab, sin_tab)]
        return (v.astype(F32) * cos + sign * (dot_nn(v, turn) * sin)).astype(BF16)

    def attend(s):
        slot = s % 2
        q_s[...] = rotate(qkv_b[slot, :, 0:width], 1.0) * BF16(HEAD ** -0.5)
        k_s[...] = rotate(qkv_b[slot, :, width:2 * width], 1.0)
        row = lax.broadcasted_iota(jnp.int32, (blk, blk), 0)
        col = lax.broadcasted_iota(jnp.int32, (blk, blk), 1)
        causal = row >= col
        dk_heads, dv_heads = [], []
        for h in range(heads):
            hs = slice(h * HEAD, (h + 1) * HEAD)
            k_h = k_s[:, hs]
            v_h = qkv_b[slot, :, 2 * width + h * HEAD:2 * width + (h + 1) * HEAD]
            dk = [None] * steps
            dv = [None] * steps
            for i in range(steps):
                at = slice(i * blk, (i + 1) * blk)
                n = (i + 1) * blk
                q_i = q_s[at, hs]
                do_i = dctx_b[slot, at, hs]
                sc = dot_nt(q_i, k_h[:n])
                s_diag = jnp.where(causal, sc[:, n - blk:], -1e30)
                sc = s_diag if i == 0 else jnp.concatenate([sc[:, :n - blk], s_diag], axis=1)
                p = jnp.exp(sc - jnp.max(sc, axis=-1, keepdims=True))
                p = p * (1.0 / row_sum(p))
                p_b = p.astype(BF16)
                ctx_s[at, hs] = dot_nn(p_b, v_h[:n]).astype(BF16)
                dp = dot_nt(do_i, v_h[:n]).astype(BF16).astype(F32)
                ds = (p * (dp - row_sum(p * dp))).astype(BF16)
                dq_s[at, hs] = (dot_nn(ds, k_h[:n]) * HEAD ** -0.5).astype(BF16)
                dk_i = dot_tn(ds, q_i)
                dv_i = dot_tn(p_b, do_i)
                for j in range(i + 1):
                    part_k, part_v = dk_i[j * blk:(j + 1) * blk], dv_i[j * blk:(j + 1) * blk]
                    dk[j] = part_k if dk[j] is None else dk[j] + part_k
                    dv[j] = part_v if dv[j] is None else dv[j] + part_v
            dk_heads.append(jnp.concatenate(dk, axis=0).astype(BF16))
            dv_heads.append(jnp.concatenate(dv, axis=0).astype(BF16))
        pieces = (rotate(dq_s[...], -1.0), rotate(jnp.concatenate(dk_heads, axis=1), -1.0), jnp.concatenate(dv_heads, axis=1))
        for pos, piece in enumerate(pieces):
            at = slice(pos * width, (pos + 1) * width)
            dqkv_s[:, at] = piece
            dbq[:, at] += fold(piece.astype(F32))

    def forward_part(s):
        def body(r):
            at = block(r, blk)
            total = dot_nn(u_b[at, :], w_d[...]) + dot_nt(ctx_s[at, :], w_a[:, 3 * width:])
            part[0, s % 2, at, :] = total.astype(BF16)
        loop(steps, body)

    def backward_part(s):
        def body(r):
            at = block(r, blk)
            d_h1 = dot_nt(dqkv_s[at, :], w_a[:, :3 * width]).astype(BF16).astype(F32)
            d_h2 = dot_nt(dpre_b[at, :], w_u[...]).astype(BF16).astype(F32)
            xf = x_b[at, :].astype(F32)
            xh, _ = normalise(xf)
            part[1, s % 2, at, :] = (d_h1 * gain1 + d_h2 * gain2).astype(BF16)
            for i, v in enumerate((d_h1 * xh, d_h1, d_h2 * xh, d_h2)):
                ln_acc[i] += fold(v)
        loop(steps, body)

    def weight_part():
        def body(r):
            at = block(r, d_loc)
            acc[at, :3 * width] += dot_tn(h1_b[:, at], dqkv_s[...])
            acc[at, 3 * width:] += dot_tn(cot_b[:, at], ctx_s[...])
        loop(n_tx, body)

    def share(a, s):
        for j, yy in enumerate((1 - y, y)):
            links.send(core_slot[a][j] + s, part.at[a, s % 2, rows(yy * 2 + 1 - core)], rc.at[a, s, yy], core_dev)

    step = 32

    def give(s):
        for a in BOTH:
            links.arrive(core_slot[a][0] + s, rc.at[a, s, 1 - y], core_dev)

            def body(r):
                at = block(r, step)
                mine = part[a, s % 2, pl.ds(pl.multiple_of(t_y * sub + r * step, step), step), :]
                sy[a, s, at, :] = (mine.astype(F32) + rc[a, s, 1 - y, at, :].astype(F32)).astype(BF16)
            loop(sub // step, body)
            links.send(y_slot[a] + s, sy.at[a, s], ry.at[a, s], y_dev)

    def finish(s):
        for a in BOTH:
            links.arrive(core_slot[a][1] + s, rc.at[a, s, y], core_dev)
            links.arrive(y_slot[a] + s, ry.at[a, s], y_dev)
            links.sent(y_slot[a] + s, sy.at[a, s])

            def body(r):
                at = block(r, step)
                whole = pl.ds(pl.multiple_of(t * sub + r * step, step), step)
                total = part[a, s % 2, whole, :].astype(F32) + rc[a, s, y, at, :].astype(F32) + ry[a, s, at, :].astype(F32)
                xf = x_own[s % 2, at, :].astype(F32)
                if a == 0:
                    out = xf + total + bias
                else:
                    xh, inv = normalise(xf)
                    out = c_own[s % 2, at, :].astype(F32) + inv * (total - row_mean(total) - xh * row_mean(total * xh))
                sy[a, s, at, :] = out.astype(BF16)
            loop(sub // step, body)
            place = outs[a].at[z * n_seq + s, rows(t)]
            for k in OTHERS:
                links.send(z_slot[a][k] + s, sy.at[a, s, :, cols((z + k) % n_tx)], place, z_dev[k])
            mine = sy.at[a, s, :, cols(z)]
            pltpu.make_async_copy(mine, place, local_sems.at[9 + a * n_seq + s]).start()
            links.send(ag_y[a][0] + s, mine, place, y_dev)
            links.send(ag_c[a][0][0] + s, mine, place, core_dev)

    def src(k):
        return (z + n_tx - k) % n_tx

    def forward(s):
        for a in BOTH:
            for k in OTHERS:
                place = outs[a].at[src(k) * n_seq + s, rows(t)]
                links.arrive(z_slot[a][k] + s, place, y_dev)
                links.send(ag_y[a][k] + s, place, place, y_dev)
                links.send(ag_c[a][k][0] + s, place, place, core_dev)

    def forward_y(s):
        for a in BOTH:
            for k in (0, *OTHERS):
                place = outs[a].at[src(k) * n_seq + s, rows(t_y)]
                links.arrive(ag_y[a][k] + s, place, y_dev)
                links.send(ag_c[a][k][1] + s, place, place, core_dev)

    def core_done(s):
        for a in BOTH:
            for j in BOTH:
                links.sent(core_slot[a][j] + s, sy.at[a, s])

    def settle(s):
        for a in BOTH:
            for k in range(n_tx):
                piece = outs[a].at[src(k) * n_seq + s, rows(t)]
                for j, who in enumerate((t_core, t_diag)):
                    links.arrive(ag_c[a][k][j] + s, outs[a].at[src(k) * n_seq + s, rows(who)], core_dev)
                    links.sent(ag_c[a][k][j] + s, piece)
                links.sent(ag_y[a][k] + s, piece)
                if k:
                    links.sent(z_slot[a][k] + s, piece)
            pltpu.make_async_copy(sy.at[a, s, :, cols(z)], outs[a].at[z * n_seq + s, rows(t)], local_sems.at[9 + a * n_seq + s]).wait()

    def one(s):
        for copy in load_early(s):
            copy.wait()

        @pl.when(s < n_seq - 1)
        def _():
            for copy in load_early(s + 1):
                copy.start()

        for copy in load_late(s):
            copy.start()
        attend(s)
        pl.when(s == 1)(lambda: rs_near(0))
        pl.when(s == 2)(lambda: rs_near(1))
        for copy in load_late(s):
            copy.wait()
        pl.when(s == 2)(lambda: core_done(0))
        x_own[s % 2] = x_b[rows(t), :]
        c_own[s % 2] = cot_b[rows(t), :]
        forward_part(s)
        share(0, s)
        backward_part(s)
        share(1, s)
        pl.when(s == 0)(lambda: rs_far(0))
        weight_part()
        give(s)
        pl.when(s > 0)(lambda: finish(s - 1))

        @pl.when(s == 1)
        def _():
            rs_far(1)
            rs_start(0, 0)

        pl.when(s == 2)(lambda: rs_start(2, 2, 1))

    for w in BOTH:
        rs_start(w, 2, 1)
    loop(n_seq, one)
    forward(0)
    last = n_seq - 1
    MINE, CORE, PAIR, FROM_Y, QUAD = range(5)
    sm_buf[MINE] = jnp.zeros_like(small_out)
    sm_buf[MINE, 4:5, :], sm_buf[MINE, 6:7, :] = [jnp.sum(sums[i], axis=0, keepdims=True) for i in BOTH]
    for i in range(4):
        sm_buf[MINE, i:i + 1, :] = jnp.sum(ln_acc[i], axis=0, keepdims=True)
    sm_buf[MINE, 5:6, :3 * width] = jnp.sum(dbq[...], axis=0, keepdims=True)
    links.send(sm_slot[0], sm_buf.at[MINE], sm_buf.at[CORE], core_dev)
    over_ty = (lax.broadcasted_iota(jnp.int32, small_out.shape, 0) < 4).astype(F32)
    finish(last)
    rs_start(1, 0)
    rs_start(2, 0)
    links.arrive(sm_slot[0], sm_buf.at[CORE], core_dev)
    sm_buf[PAIR] = sm_buf[MINE] + over_ty * sm_buf[CORE]
    links.send(sm_slot[PAIR], sm_buf.at[PAIR], sm_buf.at[FROM_Y], y_dev)
    rs_end(0)
    forward(1)
    forward_y(0)
    rs_far(2)
    links.arrive(sm_slot[PAIR], sm_buf.at[FROM_Y], y_dev)
    sm_buf[QUAD] = sm_buf[PAIR] + over_ty * sm_buf[FROM_Y]
    for k in OTHERS:
        links.send(sm_slot[QUAD + k], sm_buf.at[QUAD], sm_buf.at[QUAD + k], z_dev[k])
    forward(last)
    rs_near(2)
    forward_y(1)
    rs_end(1)
    forward_y(last)
    rs_end(2)
    for k in OTHERS:
        links.arrive(sm_slot[QUAD + k], sm_buf.at[QUAD + k], y_dev)
    small_out[...] = jnp.sum(sm_buf[QUAD:], axis=0)
    for s in range(n_seq):
        settle(s)
        if s:
            core_done(s)
    for w, slots in enumerate(rs_slot):
        for name, cond in ((R0, z < end), (L0, z > 0), (R1, lower), (L1, ~lower), (FAR, first | last_z)):
            links.sent(slots[name], arrivals[w].at[name], cond)
    for i in (MINE, PAIR, *[QUAD + k for k in OTHERS]):
        links.sent(sm_slot[i], sm_buf.at[MINE])


def layer_tail(qkv, d_ctx, u, d_pre, h1, x, cot, w_d, w_a, w_u, p_down, p_up, vecs, sums, n_tx, n_ty):
    n_seq, seq, d_model = x.shape
    end = n_tx - 1
    width, d_loc, blk, sub = d_ctx.shape[-1], d_model // n_tx, 256, seq // n_ty
    any_spec, vmem = pl.BlockSpec(memory_space=pl.ANY), pl.BlockSpec(memory_space=pltpu.VMEM)
    out = jax.ShapeDtypeStruct((n_seq * n_tx, seq, d_loc), BF16)
    cos_tab, sin_tab = rope_tables(seq, 2 * HEAD)
    shapes = (p_down.shape[1:], p_up.shape[1:], (d_loc, d_model))
    slots = n_seq * 2 * (3 + 4 * n_tx) + 5 * 5
    wide = lambda *lead: pltpu.VMEM(lead + (seq, d_model), BF16)
    piece = lambda *lead: pltpu.VMEM(lead + (sub, d_model), BF16)
    return pl.pallas_call(
        functools.partial(tail_kernel, n_tx=n_tx, blk=blk),
        in_specs=[any_spec] * 7 + [vmem] * 3 + [any_spec] * 2 + [vmem] * 5,
        out_specs=[any_spec] * 2 + [vmem] * 4,
        out_shape=[out, out, *[jax.ShapeDtypeStruct(shape, F32) for shape in (vecs.shape, *shapes)]],
        scratch_shapes=[
            pltpu.VMEM((2, seq, 3 * width), BF16),
            pltpu.VMEM((2, seq, width), BF16),
            wide(), wide(), wide(), wide(), wide(),
            pltpu.VMEM((seq, width), BF16),
            pltpu.VMEM((seq, width), BF16),
            pltpu.VMEM((seq, width), BF16),
            pltpu.VMEM((seq, width), BF16),
            pltpu.VMEM((seq, 3 * width), BF16),
            pltpu.VMEM((d_model, d_model), F32),
            pltpu.VMEM((8, 3 * width), F32),
            pltpu.VMEM((4, 8, d_model), F32),
            *[pltpu.VMEM((n,) + shape, BF16) for n, shape in zip((5, 5, 5, 2, 2), shapes + shapes)],
            wide(2, 2),
            piece(2, n_seq, 2),
            piece(2, n_seq),
            piece(2, n_seq),
            piece(2),
            piece(2),
            pltpu.VMEM((8, 8, d_model), F32),
            pltpu.SemaphoreType.DMA((slots,)),
            pltpu.SemaphoreType.DMA((slots,)),
            pltpu.SemaphoreType.DMA((9 + 2 * n_seq,)),
            pltpu.SemaphoreType.DMA((2, 2)),
        ],
        compiler_params=pltpu.CompilerParams(collective_id=1, has_side_effects=True, vmem_limit_bytes=67_000_000),
        cost_estimate=pl.CostEstimate(flops=60_000_000_000, bytes_accessed=60_000_000, transcendentals=0),
        name="layer_tail",
    )(qkv, d_ctx, u, d_pre, h1, x, cot, w_d, w_a, w_u, p_down, p_up, vecs, sums, cos_tab, sin_tab, rope_turn(width))


def solution(mesh):
    n_tx, n_ty = mesh.shape['tx'], mesh.shape['ty']
    act_spec = P('dp', None, 'tx')
    width_spec = P('tx')
    in_specs = (act_spec, act_spec, width_spec, width_spec, width_spec, width_spec, P('tx', 'ty', None), P('ty', None), P('ty', 'tx'), width_spec, P('tx', 'ty'), P('ty'), P('ty', 'tx'), width_spec)
    width_out = P(('dp', 'tx'))
    out_specs = (act_spec, act_spec, width_out, width_out, width_out, width_out, P(('dp', 'tx'), 'ty', None), P(('dp', 'ty'), None), P(('dp', 'ty'), 'tx'), width_out, P(('dp', 'tx'), 'ty'), P(('dp', 'ty')), P(('dp', 'ty'), 'tx'), width_out)
    def body(x_act, cot_out, ln1_gain, ln1_bias, ln2_gain, ln2_bias, w_qkv, b_qkv, w_dense, b_dense, w_up, b_up, w_down, b_down):
        batch, seq, d_loc = x_act.shape
        d_model = d_loc * n_tx
        heads = w_qkv.shape[1]
        hw = heads * HEAD
        n_b = batch // n_tx
        tok = n_b * seq
        z, g = lax.axis_index('tx'), lax.axis_index('dp')

        wq_loc = w_qkv.reshape(d_loc, heads, 3, HEAD).transpose(0, 2, 1, 3).reshape(d_loc, 3 * hw)
        bq = b_qkv.astype(F32).reshape(heads, 3, HEAD).transpose(1, 0, 2).reshape(1, 3 * hw)
        x, cot, w_u, w_d, w_a, vecs, h1, qkv, u, d_pre, d_ctx, part_down, part_up, sums = layer_front(
            x_act, cot_out, w_up, w_down, jnp.concatenate([wq_loc, w_dense.T], axis=1), (ln1_gain, ln1_bias, ln2_gain, ln2_bias, b_dense, b_down), bq, b_up, n_tx, n_ty)
        by_seq = lambda a: a.reshape(n_b, seq, a.shape[-1])
        y_out, dx_act, total, d_w_down, d_w_up, d_w_a = layer_tail(by_seq(qkv), by_seq(d_ctx), by_seq(u), by_seq(d_pre), by_seq(h1), by_seq(x), by_seq(cot), w_d, w_a, w_u, part_down, part_up, vecs, sums, n_tx, n_ty)
        d_w_qkv = d_w_a[:, :3 * hw].reshape(d_loc, 3, heads, HEAD).transpose(0, 2, 1, 3).reshape(d_loc, heads, 3 * HEAD)
        d_w_dense = d_w_a[:, 3 * hw:].T
        by_width = lax.dynamic_slice(total, (0, z * d_loc), (8, d_loc))
        d_b_up, d_b_qkv = total[4, :b_up.shape[0]], total[5, :3 * hw].reshape(3, heads, HEAD).transpose(1, 0, 2).reshape(heads, 3 * HEAD)
        d_b_out = by_width[6]
        return (y_out, dx_act, *by_width[:4], d_w_qkv, d_b_qkv, d_w_dense, d_b_out, d_w_up, d_b_up, d_w_down, d_b_out)

    return jax.shard_map(body, mesh=mesh, in_specs=in_specs, out_specs=out_specs, check_vma=False)
```
